32 devices in a mesh: dp: 4 (over y, x), frame: 2 (over core), tensor: 4 (over z).
Axes of the slice: x: 2, y: 2, z: 4, core: 2. Of those that a mesh axis runs over, the one named last changes fastest.
Arguments:
- tokens: bfloat16 [8, 8, 256, 1024], P('dp', ('frame', 'tensor')), may hold values from -6 to 6
- out_grad: bfloat16 [8, 8, 256, 1024], P('dp', ('frame', 'tensor')), may hold values from -6 to 6
- noise_index: int32 [8, 8], P('dp', 'frame'), may hold values from 0 to 999, as said below
- qkv_weight: bfloat16 [1024, 3, 1024], P(('dp', 'frame'), None, 'tensor'), may hold values from -0.1875 to 0.1875
- out_weight: bfloat16 [1024, 1024], P(('dp', 'frame'), 'tensor'), may hold values from -0.75 to 0.75
- up_weight: bfloat16 [1024, 4096], P(('dp', 'frame'), 'tensor'), may hold values from -0.1875 to 0.1875
- down_weight: bfloat16 [1024, 4096], P(('dp', 'frame'), 'tensor'), may hold values from -0.09375 to 0.09375
- ada_weight: bfloat16 [1024, 6, 1024], P(('dp', 'frame'), None, 'tensor'), may hold values from -0.25 to 0.25
Outputs:
- result: bfloat16 [8, 8, 256, 1024], P('dp', ('frame', 'tensor'))
- input_grad: bfloat16 [8, 8, 256, 1024], P('dp', ('frame', 'tensor'))
- qkv_grad: float32 [1024, 3, 1024], P(('dp', 'frame'), None, 'tensor')
- out_weight_grad: float32 [1024, 1024], P(('dp', 'frame'), 'tensor')
- up_grad: float32 [1024, 4096], P(('dp', 'frame'), 'tensor')
- down_grad: float32 [1024, 4096], P(('dp', 'frame'), 'tensor')
- ada_grad: float32 [1024, 6, 1024], P(('dp', 'frame'), None, 'tensor')
The draws below stay inside these ranges and needn't reach their ends.
Inputs may be any that keep to these rules, and one draw needn't show every extreme that they name: `noise_index`: each frame's noise level, most often near 1000 - 1.
All inputs are finite; a program needn't handle non-finite values.
Results may differ from the reference program's by a relative error of at most 0.018.
Values may be sent and summed in bfloat16 or wider, within the bound.
A program may use at most 192 MiB of HBM per device.

```python
import math
import jax
import jax.numpy as jnp
from jax import lax

D = 1024
HEADS = 16
HEAD_DIM = 64
FF = 4096
PATCHES = 256
LEVELS = 1000
FRAMES = 8
CLIPS = 8


def draw_noise_index(key, part):
    first_key, second_key = jax.random.split(jax.random.fold_in(key, 11))
    left = jax.random.randint(first_key, (CLIPS, FRAMES), 0, LEVELS)
    right = jax.random.randint(second_key, (CLIPS, FRAMES), 0, LEVELS)
    levels = LEVELS - 1 - left * right // LEVELS
    levels = levels.at[0, 0].set(LEVELS - 1).at[0, 1].set(0)
    return levels.astype(jnp.int32)


def shard_levels(stream_key, shape, shards, low, top_value):
    level = 1.0
    for axis_at, shards_of in shards:
        steps = jax.random.uniform(jax.random.fold_in(jax.random.fold_in(stream_key, 6), axis_at), (shards_of,), jnp.float32, low / len(shards), top_value / len(shards))
        level = level * jnp.repeat(jnp.exp(steps), shape[axis_at] // shards_of).reshape((-1,) + (1,) * (len(shape) - 1 - axis_at))
    return level


def bell_draw(stream_key, shape, width, bound, cuts=(), held_as=jnp.bfloat16):
    values = width * jax.random.normal(stream_key, shape, jnp.float32)
    if cuts:
        values = values * shard_levels(stream_key, shape, cuts, -0.22, 0.18)
    return jnp.clip(values, -bound, bound).astype(held_as)


def setup_inputs(seed: int = 0) -> dict:
    splits = jax.random.split(jax.random.key(seed), 9)
    tokens = bell_draw(splits[0], (CLIPS, FRAMES, PATCHES, D), 1.0, 6.0, ((0, 4), (1, 8)))
    out_grad = bell_draw(splits[1], (CLIPS, FRAMES, PATCHES, D), 1.0, 6.0, ((0, 4), (1, 8)))
    noise_index = draw_noise_index(jax.random.fold_in(splits[8], 71), 0)
    qkv_weight = bell_draw(splits[3], (D, 3, D), D ** -0.5, 0.1875, ((0, 8), (2, 4)))
    out_weight = bell_draw(splits[4], (D, D), (D // 16) ** -0.5, 0.75, ((0, 8), (1, 4)))
    up_weight = bell_draw(splits[5], (D, FF), D ** -0.5, 0.1875, ((0, 8), (1, 4)))
    down_weight = bell_draw(splits[6], (D, FF), FF ** -0.5, 0.09375, ((0, 8), (1, 4)))
    ada_weight = bell_draw(splits[7], (D, 6, D), (D // 2) ** -0.5, 0.25, ((0, 8), (2, 4)))
    return {"tokens": tokens, "out_grad": out_grad, "noise_index": noise_index, "qkv_weight": qkv_weight, "out_weight": out_weight, "up_weight": up_weight, "down_weight": down_weight, "ada_weight": ada_weight}


epsilon = 1e-06
highest = lax.Precision.HIGHEST

@jax.custom_vjp
def low(v):
    return lax.optimization_barrier(v.astype(jnp.bfloat16)).astype(jnp.float32)

@jax.custom_vjp
def low_back(v):
    return v

def low_keep(v):
    return (low(v), None)

def low_pass(kept, grad):
    return (grad,)

def back_keep(v):
    return (v, None)

def back_low(kept, grad):
    return (low(grad),)
low.defvjp(low_keep, low_pass)
low_back.defvjp(back_keep, back_low)

def layer_normed(values):
    center = values - lax.optimization_barrier(jnp.mean(values, axis=-1, keepdims=True))
    spread = lax.optimization_barrier(jnp.mean(center * center, axis=-1, keepdims=True))
    return center * lax.rsqrt(spread + epsilon)

def level_embedding(levels, model_width):
    halfway = model_width // 2
    frequency = jnp.exp(-math.log(10000.0) * jnp.arange(halfway, dtype=jnp.float32) / halfway)
    angles = levels.astype(jnp.float32)[..., None] * frequency
    return jnp.concatenate([jnp.cos(angles), jnp.sin(angles)], axis=-1)

def clip_forward(clip_tokens, condition, qkv_weight, out_weight, up_weight, down_weight, ada_weight):
    modulation = jnp.einsum('fd,dkc->fkc', condition, ada_weight, precision=highest)[:, :, None, :]
    token_count = FRAMES * PATCHES
    entering_one = low(layer_normed(clip_tokens) * (1.0 + modulation[:, 1]) + modulation[:, 0]).reshape(token_count, D)
    projected = low(low_back(jnp.einsum('rd,dkc->rkc', entering_one, qkv_weight, precision=highest)))
    queries = projected[:, 0].reshape(token_count, HEADS, HEAD_DIM)
    keys_all = projected[:, 1].reshape(token_count, HEADS, HEAD_DIM)
    values_all = projected[:, 2].reshape(token_count, HEADS, HEAD_DIM)
    block_rows = min(512, token_count)
    query_blocks = queries.reshape(token_count // block_rows, block_rows, HEADS, HEAD_DIM)

    def attend(query_block):
        scores = low_back(HEAD_DIM ** (-0.5) * jnp.einsum('qhe,khe->hqk', query_block, keys_all, precision=highest))
        probs = jax.nn.softmax(scores, axis=-1)
        return low(low_back(jnp.einsum('hqk,khe->qhe', low(probs), values_all, precision=highest)))
    attended = lax.map(jax.checkpoint(attend), query_blocks).reshape(token_count, D)
    branch_one = low_back(jnp.dot(attended, out_weight.T, precision=highest)).reshape(FRAMES, PATCHES, D)
    middle = clip_tokens + modulation[:, 2] * branch_one
    entering_two = low(layer_normed(middle) * (1.0 + modulation[:, 4]) + modulation[:, 3]).reshape(token_count, D)
    up_values = low_back(jnp.dot(entering_two, up_weight, precision=highest))
    hidden = low(jax.nn.gelu(up_values, approximate=True))
    branch_two = low_back(jnp.dot(hidden, down_weight.T, precision=highest)).reshape(FRAMES, PATCHES, D)
    return middle + modulation[:, 5] * branch_two

def reference(tokens, out_grad, noise_index, qkv_weight, out_weight, up_weight, down_weight, ada_weight):
    params = tuple((weight.astype(jnp.float32) for weight in (qkv_weight, out_weight, up_weight, down_weight, ada_weight)))
    condition = low(jax.nn.silu(level_embedding(noise_index, D)))

    def one_clip(totals, inputs):
        clip_tokens, clip_cotangent, clip_condition = inputs

        def forward(values, *weights):
            return clip_forward(values, clip_condition, *weights)
        output, pullback = jax.vjp(forward, clip_tokens.astype(jnp.float32), *params)
        gradients = pullback(clip_cotangent.astype(jnp.float32))
        totals = tuple((total + single for total, single in zip(totals, gradients[1:])))
        return (totals, (output.astype(jnp.bfloat16), gradients[0].astype(jnp.bfloat16)))
    initial = tuple((jnp.zeros_like(weight) for weight in params))
    totals, (result, input_grad) = lax.scan(one_clip, initial, (tokens, out_grad, condition))
    return (result, input_grad, totals[0], totals[1], totals[2], totals[3], totals[4])
```

```python
import math

import jax
import jax.numpy as jnp
from jax import lax
from jax.sharding import PartitionSpec as P

HEAD_DIM = 64


epsilon = 1e-06
highest = lax.Precision.HIGHEST


def normalize(values):
    center = values - jnp.mean(values, axis=-1, keepdims=True)
    spread = jnp.mean(center * center, axis=-1, keepdims=True)
    inverse = lax.rsqrt(spread + epsilon)
    return (center * inverse, inverse)


def norm_back(upstream, normed, inverse):
    upstream_mean = jnp.mean(upstream, axis=-1, keepdims=True)
    product_mean = jnp.mean(upstream * normed, axis=-1, keepdims=True)
    return inverse * (upstream - upstream_mean - normed * product_mean)


def level_embedding(levels, model_width):
    halfway = model_width // 2
    frequency = jnp.exp(-math.log(10000.0) * jnp.arange(halfway, dtype=jnp.float32) / halfway)
    angles = levels.astype(jnp.float32)[..., None] * frequency
    return jnp.concatenate([jnp.cos(angles), jnp.sin(angles)], axis=-1)


def gelu_tanh(values):
    return jax.nn.gelu(values, approximate=True)


def on_device(
    tokens, out_grad, noise_index, qkv_weight, out_weight, up_weight, down_weight, ada_weight
):
    clips = tokens.shape[0]
    patches = tokens.shape[2]
    model_width = tokens.shape[-1]
    local_width = qkv_weight.shape[2]
    rows_here = qkv_weight.shape[0]
    heads_here = local_width // HEAD_DIM
    scaling = HEAD_DIM ** (-0.5)
    groups = lax.axis_size("tensor")
    halves = lax.axis_size("frame")
    replicas = lax.axis_size("dp")

    with jax.named_scope("modulation"):
        levels_all = lax.all_gather(noise_index, ("dp", "frame"), axis=0, tiled=True)
        levels_all = levels_all.reshape(replicas * halves, clips, groups)
        condition_all = jax.nn.silu(level_embedding(levels_all, model_width)).astype(jnp.bfloat16)
        row_block = lax.axis_index("dp") * halves + lax.axis_index("frame")
        my_condition = lax.dynamic_slice_in_dim(
            condition_all, row_block * rows_here, rows_here, axis=3
        )
        partial_mod = jnp.einsum(
            "acgd,dkw->acgkw", my_condition, ada_weight, preferred_element_type=jnp.float32
        )
        summed_mod = lax.psum_scatter(
            partial_mod, ("dp", "frame"), scatter_dimension=0, tiled=True
        )[0]
        modulation = lax.all_to_all(summed_mod, "tensor", 1, 3, tiled=True)
        modulation = modulation.reshape(clips, 6, 1, model_width)

    with jax.named_scope("weights"):
        joint_weight, mixer_weight, upward_weight, downward_weight = (
            lax.all_gather(w, ("dp", "frame"), axis=0, tiled=True)
            for w in (qkv_weight, out_weight, up_weight, down_weight)
        )

    residual = tokens[:, 0].astype(jnp.float32)
    upstream = out_grad[:, 0].astype(jnp.float32)
    shift1, scale1, gate1 = modulation[:, 0], modulation[:, 1], modulation[:, 2]
    shift2, scale2, gate2 = modulation[:, 3], modulation[:, 4], modulation[:, 5]

    def gather_tokens(values):
        return lax.all_gather(values, "tensor", axis=1, tiled=True)

    def scatter_tokens(values):
        return lax.psum_scatter(
            values.astype(jnp.bfloat16), "tensor", scatter_dimension=1, tiled=True
        ).astype(jnp.float32)

    with jax.named_scope("forward"):
        normed_one, inverse_one = normalize(residual)
        entering_one = (normed_one * (1.0 + scale1) + shift1).astype(jnp.bfloat16)
        flat_one = gather_tokens(entering_one)
        token_count = flat_one.shape[1]
        projected = jnp.einsum(
            "crd,dkh->crkh", flat_one, joint_weight, preferred_element_type=jnp.float32
        ).astype(jnp.bfloat16)
        queries = projected[:, :, 0]
        keys_all = lax.all_gather(projected[:, :, 1], "frame", axis=1, tiled=True)
        values_all = lax.all_gather(projected[:, :, 2], "frame", axis=1, tiled=True)
        key_heads = keys_all.reshape(clips, -1, heads_here, HEAD_DIM)
        value_heads = values_all.reshape(clips, -1, heads_here, HEAD_DIM)
        block_rows = min(512, token_count)
        block_count = token_count // block_rows
        query_blocks = jnp.moveaxis(
            queries.reshape(clips, block_count, block_rows, heads_here, HEAD_DIM), 1, 0
        )

        def attend(query_block):
            scores = (
                jnp.einsum(
                    "cqhe,ckhe->chqk", query_block, key_heads, preferred_element_type=jnp.float32
                )
                * scaling
            )
            largest = jnp.max(scores, axis=-1, keepdims=True)
            raised = jnp.exp(scores - largest)
            totals_row = jnp.sum(raised, axis=-1, keepdims=True)
            probs_low = (raised / totals_row).astype(jnp.bfloat16)
            outputs = jnp.einsum(
                "chqk,ckhe->cqhe", probs_low, value_heads, preferred_element_type=jnp.float32
            )
            return (outputs.astype(jnp.bfloat16), (largest + jnp.log(totals_row))[..., 0])

        attended_blocks, log_totals = lax.map(attend, query_blocks)
        attended = jnp.moveaxis(attended_blocks, 0, 1).reshape(clips, token_count, local_width)
        partial_one = jnp.einsum(
            "crh,oh->cro", attended, mixer_weight, preferred_element_type=jnp.float32
        )
        branch_one = scatter_tokens(partial_one)
        middle = residual + gate1 * branch_one
        normed_two, inverse_two = normalize(middle)
        entering_two = (normed_two * (1.0 + scale2) + shift2).astype(jnp.bfloat16)
        flat_two = gather_tokens(entering_two)
        up_values = jnp.einsum(
            "crd,df->crf", flat_two, upward_weight, preferred_element_type=jnp.float32
        )
        hidden = gelu_tanh(up_values).astype(jnp.bfloat16)
        partial_two = jnp.einsum(
            "crf,of->cro", hidden, downward_weight, preferred_element_type=jnp.float32
        )
        branch_two = scatter_tokens(partial_two)
        output = (middle + gate2 * branch_two).astype(jnp.bfloat16)

    with jax.named_scope("backward_ffn"):
        grad_gate_two = jnp.sum(upstream * branch_two, axis=1)
        grad_branch_two = (gate2 * upstream).astype(jnp.bfloat16)
        grad_two_all = gather_tokens(grad_branch_two)
        grad_hidden = jnp.einsum(
            "cro,of->crf", grad_two_all, downward_weight, preferred_element_type=jnp.float32
        )
        down_total = jnp.einsum(
            "cro,crf->of", grad_two_all, hidden, preferred_element_type=jnp.float32
        )
        _, gelu_pullback = jax.vjp(gelu_tanh, up_values)
        grad_up = gelu_pullback(grad_hidden)[0].astype(jnp.bfloat16)
        up_total = jnp.einsum(
            "crd,crf->df", flat_two, grad_up, preferred_element_type=jnp.float32
        )
        partial_back_two = jnp.einsum(
            "crf,df->crd", grad_up, upward_weight, preferred_element_type=jnp.float32
        )
        grad_entering_two = scatter_tokens(partial_back_two)
        grad_shift_two = jnp.sum(grad_entering_two, axis=1)
        grad_scale_two = jnp.sum(grad_entering_two * normed_two, axis=1)
        grad_middle = upstream + norm_back(
            grad_entering_two * (1.0 + scale2), normed_two, inverse_two
        )
        grad_gate_one = jnp.sum(grad_middle * branch_one, axis=1)

    with jax.named_scope("backward_attention"):
        grad_branch_one = (gate1 * grad_middle).astype(jnp.bfloat16)
        grad_one_all = gather_tokens(grad_branch_one)
        grad_attended = jnp.einsum(
            "cro,oh->crh", grad_one_all, mixer_weight, preferred_element_type=jnp.float32
        ).astype(jnp.bfloat16)
        mixer_total = jnp.einsum(
            "cro,crh->oh", grad_one_all, attended, preferred_element_type=jnp.float32
        )
        grad_blocks = jnp.moveaxis(
            grad_attended.reshape(clips, block_count, block_rows, heads_here, HEAD_DIM), 1, 0
        )

        def attend_back(carried, pieces):
            key_sum, value_sum = carried
            query_block, grad_block, log_block = pieces
            scores = (
                jnp.einsum(
                    "cqhe,ckhe->chqk", query_block, key_heads, preferred_element_type=jnp.float32
                )
                * scaling
            )
            probs = jnp.exp(scores - log_block[..., None])
            grad_probs = jnp.einsum(
                "cqhe,ckhe->chqk", grad_block, value_heads, preferred_element_type=jnp.float32
            )
            value_sum = value_sum + jnp.einsum(
                "chqk,cqhe->ckhe",
                probs.astype(jnp.bfloat16),
                grad_block,
                preferred_element_type=jnp.float32,
            )
            row_terms = jnp.sum(probs * grad_probs, axis=-1, keepdims=True)
            grad_scores = (probs * (grad_probs - row_terms)).astype(jnp.bfloat16)
            grad_queries = (
                jnp.einsum(
                    "chqk,ckhe->cqhe", grad_scores, key_heads, preferred_element_type=jnp.float32
                )
                * scaling
            )
            key_sum = (
                key_sum
                + jnp.einsum(
                    "chqk,cqhe->ckhe", grad_scores, query_block, preferred_element_type=jnp.float32
                )
                * scaling
            )
            return ((key_sum, value_sum), grad_queries)

        zeros_keys = jnp.zeros(key_heads.shape, jnp.float32)
        (key_grads, value_grads), query_grads = lax.scan(
            attend_back, (zeros_keys, zeros_keys), (query_blocks, grad_blocks, log_totals)
        )
        query_grads = jnp.moveaxis(query_grads, 0, 1).reshape(clips, token_count, local_width)
        key_own, value_own = (
            lax.psum_scatter(
                grads.reshape(clips, -1, local_width).astype(jnp.bfloat16),
                "frame",
                scatter_dimension=1,
                tiled=True,
            ).astype(jnp.float32)
            for grads in (key_grads, value_grads)
        )
        grad_projected = jnp.stack([query_grads, key_own, value_own], axis=2).astype(
            jnp.bfloat16
        )
        joint_total = jnp.einsum(
            "crd,crkh->dkh", flat_one, grad_projected, preferred_element_type=jnp.float32
        )
        partial_back_one = jnp.einsum(
            "crkh,dkh->crd", grad_projected, joint_weight, preferred_element_type=jnp.float32
        )
        grad_entering_one = scatter_tokens(partial_back_one)
        grad_shift_one = jnp.sum(grad_entering_one, axis=1)
        grad_scale_one = jnp.sum(grad_entering_one * normed_one, axis=1)
        grad_input = grad_middle + norm_back(
            grad_entering_one * (1.0 + scale1), normed_one, inverse_one
        )

    with jax.named_scope("ada_grad"):
        grad_modulation = jnp.stack(
            [
                grad_shift_one,
                grad_scale_one,
                grad_gate_one,
                grad_shift_two,
                grad_scale_two,
                grad_gate_two,
            ],
            axis=1,
        )
        grad_columns = lax.all_to_all(
            grad_modulation.reshape(clips, 1, 6, model_width), "tensor", 3, 1, tiled=True
        )
        grad_all = lax.all_gather(grad_columns, ("dp", "frame"), axis=0, tiled=True)
        grad_all = grad_all.reshape(replicas * halves, clips, groups, 6, local_width)
        adaptive_total = jnp.einsum(
            "acgd,acgkw->dkw",
            my_condition.astype(jnp.float32),
            grad_all,
            precision=highest,
        )

    with jax.named_scope("weight_grads"):
        summed = tuple(
            lax.psum_scatter(
                total.astype(jnp.bfloat16), ("dp", "frame"), scatter_dimension=0, tiled=True
            ).astype(jnp.float32)
            for total in (joint_total, mixer_total, up_total, down_total)
        )
    result = output[:, None]
    input_grad = grad_input.astype(jnp.bfloat16)[:, None]
    return (result, input_grad, summed[0], summed[1], summed[2], summed[3], adaptive_total)


def solution(mesh):
    return jax.shard_map(
        on_device,
        mesh=mesh,
        in_specs=(
            P("dp", ("frame", "tensor"), None, None),
            P("dp", ("frame", "tensor"), None, None),
            P("dp", "frame"),
            P(("dp", "frame"), None, "tensor"),
            P(("dp", "frame"), "tensor"),
            P(("dp", "frame"), "tensor"),
            P(("dp", "frame"), "tensor"),
            P(("dp", "frame"), None, "tensor"),
        ),
        out_specs=(
            P("dp", ("frame", "tensor"), None, None),
            P("dp", ("frame", "tensor"), None, None),
            P(("dp", "frame"), None, "tensor"),
            P(("dp", "frame"), "tensor"),
            P(("dp", "frame"), "tensor"),
            P(("dp", "frame"), "tensor"),
            P(("dp", "frame"), None, "tensor"),
        ),
        check_vma=False,
    )
```

```python
import math

import jax
import jax.numpy as jnp
from jax import lax
from jax.sharding import PartitionSpec as P

HEAD_DIM = 64


epsilon = 1e-06
highest = lax.Precision.HIGHEST


def normalize(values):
    center = values - jnp.mean(values, axis=-1, keepdims=True)
    spread = jnp.mean(center * center, axis=-1, keepdims=True)
    inverse = lax.rsqrt(spread + epsilon)
    return (center * inverse, inverse)


def norm_back(upstream, normed, inverse):
    upstream_mean = jnp.mean(upstream, axis=-1, keepdims=True)
    product_mean = jnp.mean(upstream * normed, axis=-1, keepdims=True)
    return inverse * (upstream - upstream_mean - normed * product_mean)


def level_embedding(levels, model_width):
    halfway = model_width // 2
    frequency = jnp.exp(-math.log(10000.0) * jnp.arange(halfway, dtype=jnp.float32) / halfway)
    angles = levels.astype(jnp.float32)[..., None] * frequency
    return jnp.concatenate([jnp.cos(angles), jnp.sin(angles)], axis=-1)


def gelu_tanh(values):
    return jax.nn.gelu(values, approximate=True)


def on_device(
    tokens, out_grad, noise_index, qkv_weight, out_weight, up_weight, down_weight, ada_weight
):
    clips = tokens.shape[0]
    patches = tokens.shape[2]
    model_width = tokens.shape[-1]
    local_width = qkv_weight.shape[2]
    rows_here = qkv_weight.shape[0]
    heads_here = local_width // HEAD_DIM
    scaling = HEAD_DIM ** (-0.5)
    groups = lax.axis_size("tensor")
    halves = lax.axis_size("frame")
    replicas = lax.axis_size("dp")

    with jax.named_scope("modulation"):
        levels_all = lax.all_gather(noise_index, ("dp", "frame"), axis=0, tiled=True)
        levels_all = levels_all.reshape(replicas * halves, clips, groups)
        condition_all = jax.nn.silu(level_embedding(levels_all, model_width)).astype(jnp.bfloat16)
        row_block = lax.axis_index("dp") * halves + lax.axis_index("frame")
        my_condition = lax.dynamic_slice_in_dim(
            condition_all, row_block * rows_here, rows_here, axis=3
        )
        partial_mod = jnp.einsum(
            "acgd,dkw->acgkw", my_condition, ada_weight, preferred_element_type=jnp.float32
        )
        summed_mod = lax.psum_scatter(
            partial_mod, ("dp", "frame"), scatter_dimension=0, tiled=True
        )[0]
        modulation = lax.all_to_all(summed_mod, "tensor", 1, 3, tiled=True)
        modulation = modulation.reshape(clips, 6, 1, model_width)

    with jax.named_scope("weights"):
        joint_weight, mixer_weight, upward_weight, downward_weight = (
            lax.all_gather(w, ("dp", "frame"), axis=0, tiled=True)
            for w in (qkv_weight, out_weight, up_weight, down_weight)
        )

    residual = tokens[:, 0].astype(jnp.float32)
    upstream = out_grad[:, 0].astype(jnp.float32)
    def clip_pass(residual, upstream, modulation):
        clips = residual.shape[0]
        shift1, scale1, gate1 = modulation[:, 0], modulation[:, 1], modulation[:, 2]
        shift2, scale2, gate2 = modulation[:, 3], modulation[:, 4], modulation[:, 5]
        def gather_tokens(values):
            return lax.all_gather(values, "tensor", axis=1, tiled=True)

        def scatter_tokens(values):
            return lax.psum_scatter(
                values.astype(jnp.bfloat16), "tensor", scatter_dimension=1, tiled=True
            ).astype(jnp.float32)

        with jax.named_scope("forward"):
            normed_one, inverse_one = normalize(residual)
            entering_one = (normed_one * (1.0 + scale1) + shift1).astype(jnp.bfloat16)
            flat_one = gather_tokens(entering_one)
            token_count = flat_one.shape[1]
            projected = jnp.einsum(
                "crd,dkh->crkh", flat_one, joint_weight, preferred_element_type=jnp.float32
            ).astype(jnp.bfloat16)
            queries = projected[:, :, 0]
            keys_all = lax.all_gather(projected[:, :, 1], "frame", axis=1, tiled=True)
            values_all = lax.all_gather(projected[:, :, 2], "frame", axis=1, tiled=True)
            key_heads = keys_all.reshape(clips, -1, heads_here, HEAD_DIM)
            value_heads = values_all.reshape(clips, -1, heads_here, HEAD_DIM)
            block_rows = min(512, token_count)
            block_count = token_count // block_rows
            query_blocks = jnp.moveaxis(
                queries.reshape(clips, block_count, block_rows, heads_here, HEAD_DIM), 1, 0
            )

            def attend(query_block):
                scores = (
                    jnp.einsum(
                        "cqhe,ckhe->chqk", query_block, key_heads, preferred_element_type=jnp.float32
                    )
                    * scaling
                )
                largest = jnp.max(scores, axis=-1, keepdims=True)
                raised = jnp.exp(scores - largest)
                totals_row = jnp.sum(raised, axis=-1, keepdims=True)
                probs_low = (raised / totals_row).astype(jnp.bfloat16)
                outputs = jnp.einsum(
                    "chqk,ckhe->cqhe", probs_low, value_heads, preferred_element_type=jnp.float32
                )
                return (outputs.astype(jnp.bfloat16), (largest + jnp.log(totals_row))[..., 0])

            attended_blocks, log_totals = lax.map(attend, query_blocks)
            attended = jnp.moveaxis(attended_blocks, 0, 1).reshape(clips, token_count, local_width)
            partial_one = jnp.einsum(
                "crh,oh->cro", attended, mixer_weight, preferred_element_type=jnp.float32
            )
            branch_one = scatter_tokens(partial_one)
            middle = residual + gate1 * branch_one
            normed_two, inverse_two = normalize(middle)
            entering_two = (normed_two * (1.0 + scale2) + shift2).astype(jnp.bfloat16)
            flat_two = gather_tokens(entering_two)
            up_values = jnp.einsum(
                "crd,df->crf", flat_two, upward_weight, preferred_element_type=jnp.float32
            )
            hidden = gelu_tanh(up_values).astype(jnp.bfloat16)
            partial_two = jnp.einsum(
                "crf,of->cro", hidden, downward_weight, preferred_element_type=jnp.float32
            )
            branch_two = scatter_tokens(partial_two)
            output = (middle + gate2 * branch_two).astype(jnp.bfloat16)

        with jax.named_scope("backward_ffn"):
            grad_gate_two = jnp.sum(upstream * branch_two, axis=1)
            grad_branch_two = (gate2 * upstream).astype(jnp.bfloat16)
            grad_two_all = gather_tokens(grad_branch_two)
            grad_hidden = jnp.einsum(
                "cro,of->crf", grad_two_all, downward_weight, preferred_element_type=jnp.float32
            )
            down_total = jnp.einsum(
                "cro,crf->of", grad_two_all, hidden, preferred_element_type=jnp.float32
            )
            _, gelu_pullback = jax.vjp(gelu_tanh, up_values)
            grad_up = gelu_pullback(grad_hidden)[0].astype(jnp.bfloat16)
            up_total = jnp.einsum(
                "crd,crf->df", flat_two, grad_up, preferred_element_type=jnp.float32
            )
            partial_back_two = jnp.einsum(
                "crf,df->crd", grad_up, upward_weight, preferred_element_type=jnp.float32
            )
            grad_entering_two = scatter_tokens(partial_back_two)
            grad_shift_two = jnp.sum(grad_entering_two, axis=1)
            grad_scale_two = jnp.sum(grad_entering_two * normed_two, axis=1)
            grad_middle = upstream + norm_back(
                grad_entering_two * (1.0 + scale2), normed_two, inverse_two
            )
            grad_gate_one = jnp.sum(grad_middle * branch_one, axis=1)

        with jax.named_scope("backward_attention"):
            grad_branch_one = (gate1 * grad_middle).astype(jnp.bfloat16)
            grad_one_all = gather_tokens(grad_branch_one)
            grad_attended = jnp.einsum(
                "cro,oh->crh", grad_one_all, mixer_weight, preferred_element_type=jnp.float32
            ).astype(jnp.bfloat16)
            mixer_total = jnp.einsum(
                "cro,crh->oh", grad_one_all, attended, preferred_element_type=jnp.float32
            )
            grad_blocks = jnp.moveaxis(
                grad_attended.reshape(clips, block_count, block_rows, heads_here, HEAD_DIM), 1, 0
            )

            def attend_back(carried, pieces):
                key_sum, value_sum = carried
                query_block, grad_block, log_block = pieces
                scores = (
                    jnp.einsum(
                        "cqhe,ckhe->chqk", query_block, key_heads, preferred_element_type=jnp.float32
                    )
                    * scaling
                )
                probs = jnp.exp(scores - log_block[..., None])
                grad_probs = jnp.einsum(
                    "cqhe,ckhe->chqk", grad_block, value_heads, preferred_element_type=jnp.float32
                )
                value_sum = value_sum + jnp.einsum(
                    "chqk,cqhe->ckhe",
                    probs.astype(jnp.bfloat16),
                    grad_block,
                    preferred_element_type=jnp.float32,
                )
                row_terms = jnp.sum(probs * grad_probs, axis=-1, keepdims=True)
                grad_scores = (probs * (grad_probs - row_terms)).astype(jnp.bfloat16)
                grad_queries = (
                    jnp.einsum(
                        "chqk,ckhe->cqhe", grad_scores, key_heads, preferred_element_type=jnp.float32
                    )
                    * scaling
                )
                key_sum = (
                    key_sum
                    + jnp.einsum(
                        "chqk,cqhe->ckhe", grad_scores, query_block, preferred_element_type=jnp.float32
                    )
                    * scaling
                )
                return ((key_sum, value_sum), grad_queries)

            zeros_keys = jnp.zeros(key_heads.shape, jnp.float32)
            (key_grads, value_grads), query_grads = lax.scan(
                attend_back, (zeros_keys, zeros_keys), (query_blocks, grad_blocks, log_totals)
            )
            query_grads = jnp.moveaxis(query_grads, 0, 1).reshape(clips, token_count, local_width)
            key_own, value_own = (
                lax.psum_scatter(
                    grads.reshape(clips, -1, local_width).astype(jnp.bfloat16),
                    "frame",
                    scatter_dimension=1,
                    tiled=True,
                ).astype(jnp.float32)
                for grads in (key_grads, value_grads)
            )
            grad_projected = jnp.stack([query_grads, key_own, value_own], axis=2).astype(
                jnp.bfloat16
            )
            joint_total = jnp.einsum(
                "crd,crkh->dkh", flat_one, grad_projected, preferred_element_type=jnp.float32
            )
            partial_back_one = jnp.einsum(
                "crkh,dkh->crd", grad_projected, joint_weight, preferred_element_type=jnp.float32
            )
            grad_entering_one = scatter_tokens(partial_back_one)
            grad_shift_one = jnp.sum(grad_entering_one, axis=1)
            grad_scale_one = jnp.sum(grad_entering_one * normed_one, axis=1)
            grad_input = grad_middle + norm_back(
                grad_entering_one * (1.0 + scale1), normed_one, inverse_one
            )


        grad_modulation = jnp.stack(
            [grad_shift_one, grad_scale_one, grad_gate_one, grad_shift_two, grad_scale_two, grad_gate_two],
            axis=1,
        )
        totals = (joint_total, mixer_total, up_total, down_total)
        return output, grad_input.astype(jnp.bfloat16), grad_modulation, totals

    pieces = [
        clip_pass(residual[i : i + 1], upstream[i : i + 1], modulation[i : i + 1])
        for i in range(clips)
    ]
    output = jnp.concatenate([p[0] for p in pieces], axis=0)
    grad_input_low = jnp.concatenate([p[1] for p in pieces], axis=0)
    grad_modulation = jnp.concatenate([p[2] for p in pieces], axis=0)
    joint_total, mixer_total, up_total, down_total = (
        sum(p[3][k] for p in pieces[1:]) + pieces[0][3][k] for k in range(4)
    )
    with jax.named_scope("ada_grad"):
        grad_columns = lax.all_to_all(
            grad_modulation.reshape(clips, 1, 6, model_width), "tensor", 3, 1, tiled=True
        )
        grad_all = lax.all_gather(grad_columns, ("dp", "frame"), axis=0, tiled=True)
        grad_all = grad_all.reshape(replicas * halves, clips, groups, 6, local_width)
        adaptive_total = jnp.einsum(
            "acgd,acgkw->dkw",
            my_condition.astype(jnp.float32),
            grad_all,
            precision=highest,
        )

    with jax.named_scope("weight_grads"):
        summed = tuple(
            lax.psum_scatter(
                total.astype(jnp.bfloat16), ("dp", "frame"), scatter_dimension=0, tiled=True
            ).astype(jnp.float32)
            for total in (joint_total, mixer_total, up_total, down_total)
        )
    result = output[:, None]
    input_grad = grad_input_low[:, None]
    return (result, input_grad, summed[0], summed[1], summed[2], summed[3], adaptive_total)


def solution(mesh):
    return jax.shard_map(
        on_device,
        mesh=mesh,
        in_specs=(
            P("dp", ("frame", "tensor"), None, None),
            P("dp", ("frame", "tensor"), None, None),
            P("dp", "frame"),
            P(("dp", "frame"), None, "tensor"),
            P(("dp", "frame"), "tensor"),
            P(("dp", "frame"), "tensor"),
            P(("dp", "frame"), "tensor"),
            P(("dp", "frame"), None, "tensor"),
        ),
        out_specs=(
            P("dp", ("frame", "tensor"), None, None),
            P("dp", ("frame", "tensor"), None, None),
            P(("dp", "frame"), None, "tensor"),
            P(("dp", "frame"), "tensor"),
            P(("dp", "frame"), "tensor"),
            P(("dp", "frame"), "tensor"),
            P(("dp", "frame"), None, "tensor"),
        ),
        check_vma=False,
    )
```

```python
import math

import jax
import jax.numpy as jnp
from jax import lax
from jax.sharding import PartitionSpec as P

HEAD_DIM = 64


epsilon = 1e-06
highest = lax.Precision.HIGHEST


def normalize(values):
    center = values - jnp.mean(values, axis=-1, keepdims=True)
    spread = jnp.mean(center * center, axis=-1, keepdims=True)
    inverse = lax.rsqrt(spread + epsilon)
    return (center * inverse, inverse)


def norm_back(upstream, normed, inverse):
    upstream_mean = jnp.mean(upstream, axis=-1, keepdims=True)
    product_mean = jnp.mean(upstream * normed, axis=-1, keepdims=True)
    return inverse * (upstream - upstream_mean - normed * product_mean)


def level_embedding(levels, model_width):
    halfway = model_width // 2
    frequency = jnp.exp(-math.log(10000.0) * jnp.arange(halfway, dtype=jnp.float32) / halfway)
    angles = levels.astype(jnp.float32)[..., None] * frequency
    return jnp.concatenate([jnp.cos(angles), jnp.sin(angles)], axis=-1)


def gelu_tanh(values):
    return jax.nn.gelu(values, approximate=True)


def on_device(
    tokens, out_grad, noise_index, qkv_weight, out_weight, up_weight, down_weight, ada_weight
):
    clips = tokens.shape[0]
    patches = tokens.shape[2]
    model_width = tokens.shape[-1]
    local_width = qkv_weight.shape[2]
    rows_here = qkv_weight.shape[0]
    heads_here = local_width // HEAD_DIM
    scaling = HEAD_DIM ** (-0.5)
    groups = lax.axis_size("tensor")
    halves = lax.axis_size("frame")
    replicas = lax.axis_size("dp")

    with jax.named_scope("modulation"):
        levels_all = lax.all_gather(noise_index, ("dp", "frame"), axis=0, tiled=True)
        levels_all = levels_all.reshape(replicas * halves, clips, groups)
        condition_all = jax.nn.silu(level_embedding(levels_all, model_width)).astype(jnp.bfloat16)
        row_block = lax.axis_index("dp") * halves + lax.axis_index("frame")
        my_condition = lax.dynamic_slice_in_dim(
            condition_all, row_block * rows_here, rows_here, axis=3
        )
        partial_mod = jnp.einsum(
            "acgd,dkw->acgkw", my_condition, ada_weight, preferred_element_type=jnp.float32
        )
        summed_mod = jnp.sum(
            lax.all_to_all(partial_mod, ("dp", "frame"), 0, 0, tiled=True), axis=0
        )
        modulation = lax.all_to_all(summed_mod, "tensor", 1, 3, tiled=True)
        modulation = modulation.reshape(clips, 6, 1, model_width)

    with jax.named_scope("weights"):
        joint_weight, mixer_weight, upward_weight, downward_weight = (
            lax.all_gather(w, ("dp", "frame"), axis=0, tiled=True)
            for w in (qkv_weight, out_weight, up_weight, down_weight)
        )

    residual = tokens[:, 0].astype(jnp.float32)
    upstream = out_grad[:, 0].astype(jnp.float32)
    def gather_halves(values):
        if halves != 2:
            return lax.all_gather(values, "frame", axis=1, tiled=True)
        other = lax.ppermute(values, "frame", [(0, 1), (1, 0)])
        return jnp.concatenate([values, other], axis=1)

    def scatter_halves(values):
        if halves != 2:
            return lax.psum_scatter(
                values.astype(jnp.bfloat16), "frame", scatter_dimension=1, tiled=True
            ).astype(jnp.float32)
        count = values.shape[1] // 2
        mine = values[:, :count]
        other = lax.ppermute(values[:, count:].astype(jnp.bfloat16), "frame", [(0, 1), (1, 0)])
        return mine.astype(jnp.bfloat16).astype(jnp.float32) + other.astype(jnp.float32)

    def clip_pass(residual, upstream, modulation):
        clips = residual.shape[0]
        shift1, scale1, gate1 = modulation[:, 0], modulation[:, 1], modulation[:, 2]
        shift2, scale2, gate2 = modulation[:, 3], modulation[:, 4], modulation[:, 5]
        def gather_tokens(values):
            return lax.all_gather(values, "tensor", axis=1, tiled=True)

        def scatter_tokens(values):
            parts = values.astype(jnp.bfloat16).reshape(
                values.shape[0], groups, -1, values.shape[-1]
            )
            received = lax.all_to_all(parts, "tensor", 1, 1, tiled=True)
            return jnp.sum(received.astype(jnp.float32), axis=1)

        with jax.named_scope("forward"):
            normed_one, inverse_one = normalize(residual)
            entering_one = (normed_one * (1.0 + scale1) + shift1).astype(jnp.bfloat16)
            flat_one = gather_tokens(entering_one)
            token_count = flat_one.shape[1]
            projected = jnp.einsum(
                "crd,dkh->crkh", flat_one, joint_weight, preferred_element_type=jnp.float32
            ).astype(jnp.bfloat16)
            queries = projected[:, :, 0]
            keys_all = gather_halves(projected[:, :, 1])
            values_all = gather_halves(projected[:, :, 2])
            key_heads = keys_all.reshape(clips, -1, heads_here, HEAD_DIM)
            value_heads = values_all.reshape(clips, -1, heads_here, HEAD_DIM)
            block_rows = min(512, token_count)
            block_count = token_count // block_rows
            query_blocks = jnp.moveaxis(
                queries.reshape(clips, block_count, block_rows, heads_here, HEAD_DIM), 1, 0
            )

            def attend(query_block):
                scores = (
                    jnp.einsum(
                        "cqhe,ckhe->chqk", query_block, key_heads, preferred_element_type=jnp.float32
                    )
                    * scaling
                )
                largest = jnp.max(scores, axis=-1, keepdims=True)
                raised = jnp.exp(scores - largest)
                totals_row = jnp.sum(raised, axis=-1, keepdims=True)
                probs_low = (raised / totals_row).astype(jnp.bfloat16)
                outputs = jnp.einsum(
                    "chqk,ckhe->cqhe", probs_low, value_heads, preferred_element_type=jnp.float32
                )
                return (outputs.astype(jnp.bfloat16), (largest + jnp.log(totals_row))[..., 0])

            attended_blocks, log_totals = lax.map(attend, query_blocks)
            attended = jnp.moveaxis(attended_blocks, 0, 1).reshape(clips, token_count, local_width)
            partial_one = jnp.einsum(
                "crh,oh->cro", attended, mixer_weight, preferred_element_type=jnp.float32
            )
            branch_one = scatter_tokens(partial_one)
            middle = residual + gate1 * branch_one
            normed_two, inverse_two = normalize(middle)
            entering_two = (normed_two * (1.0 + scale2) + shift2).astype(jnp.bfloat16)
            flat_two = gather_tokens(entering_two)
            up_values = jnp.einsum(
                "crd,df->crf", flat_two, upward_weight, preferred_element_type=jnp.float32
            )
            hidden = gelu_tanh(up_values).astype(jnp.bfloat16)
            partial_two = jnp.einsum(
                "crf,of->cro", hidden, downward_weight, preferred_element_type=jnp.float32
            )
            branch_two = scatter_tokens(partial_two)
            output = (middle + gate2 * branch_two).astype(jnp.bfloat16)

        with jax.named_scope("backward_ffn"):
            grad_gate_two = jnp.sum(upstream * branch_two, axis=1)
            grad_branch_two = (gate2 * upstream).astype(jnp.bfloat16)
            grad_two_all = gather_tokens(grad_branch_two)
            grad_hidden = jnp.einsum(
                "cro,of->crf", grad_two_all, downward_weight, preferred_element_type=jnp.float32
            )
            down_total = jnp.einsum(
                "cro,crf->of", grad_two_all, hidden, preferred_element_type=jnp.float32
            )
            _, gelu_pullback = jax.vjp(gelu_tanh, up_values)
            grad_up = gelu_pullback(grad_hidden)[0].astype(jnp.bfloat16)
            up_total = jnp.einsum(
                "crd,crf->df", flat_two, grad_up, preferred_element_type=jnp.float32
            )
            partial_back_two = jnp.einsum(
                "crf,df->crd", grad_up, upward_weight, preferred_element_type=jnp.float32
            )
            grad_entering_two = scatter_tokens(partial_back_two)
            grad_shift_two = jnp.sum(grad_entering_two, axis=1)
            grad_scale_two = jnp.sum(grad_entering_two * normed_two, axis=1)
            grad_middle = upstream + norm_back(
                grad_entering_two * (1.0 + scale2), normed_two, inverse_two
            )
            grad_gate_one = jnp.sum(grad_middle * branch_one, axis=1)

        with jax.named_scope("backward_attention"):
            grad_branch_one = (gate1 * grad_middle).astype(jnp.bfloat16)
            grad_one_all = gather_tokens(grad_branch_one)
            grad_attended = jnp.einsum(
                "cro,oh->crh", grad_one_all, mixer_weight, preferred_element_type=jnp.float32
            ).astype(jnp.bfloat16)
            mixer_total = jnp.einsum(
                "cro,crh->oh", grad_one_all, attended, preferred_element_type=jnp.float32
            )
            grad_blocks = jnp.moveaxis(
                grad_attended.reshape(clips, block_count, block_rows, heads_here, HEAD_DIM), 1, 0
            )

            def attend_back(carried, pieces):
                key_sum, value_sum = carried
                query_block, grad_block, log_block = pieces
                scores = (
                    jnp.einsum(
                        "cqhe,ckhe->chqk", query_block, key_heads, preferred_element_type=jnp.float32
                    )
                    * scaling
                )
                probs = jnp.exp(scores - log_block[..., None])
                grad_probs = jnp.einsum(
                    "cqhe,ckhe->chqk", grad_block, value_heads, preferred_element_type=jnp.float32
                )
                value_sum = value_sum + jnp.einsum(
                    "chqk,cqhe->ckhe",
                    probs.astype(jnp.bfloat16),
                    grad_block,
                    preferred_element_type=jnp.float32,
                )
                row_terms = jnp.sum(probs * grad_probs, axis=-1, keepdims=True)
                grad_scores = (probs * (grad_probs - row_terms)).astype(jnp.bfloat16)
                grad_queries = (
                    jnp.einsum(
                        "chqk,ckhe->cqhe", grad_scores, key_heads, preferred_element_type=jnp.float32
                    )
                    * scaling
                )
                key_sum = (
                    key_sum
                    + jnp.einsum(
                        "chqk,cqhe->ckhe", grad_scores, query_block, preferred_element_type=jnp.float32
                    )
                    * scaling
                )
                return ((key_sum, value_sum), grad_queries)

            zeros_keys = jnp.zeros(key_heads.shape, jnp.float32)
            (key_grads, value_grads), query_grads = lax.scan(
                attend_back, (zeros_keys, zeros_keys), (query_blocks, grad_blocks, log_totals)
            )
            query_grads = jnp.moveaxis(query_grads, 0, 1).reshape(clips, token_count, local_width)
            key_own, value_own = (
                scatter_halves(grads.reshape(clips, -1, local_width))
                for grads in (key_grads, value_grads)
            )
            grad_projected = jnp.stack([query_grads, key_own, value_own], axis=2).astype(
                jnp.bfloat16
            )
            joint_total = jnp.einsum(
                "crd,crkh->dkh", flat_one, grad_projected, preferred_element_type=jnp.float32
            )
            partial_back_one = jnp.einsum(
                "crkh,dkh->crd", grad_projected, joint_weight, preferred_element_type=jnp.float32
            )
            grad_entering_one = scatter_tokens(partial_back_one)
            grad_shift_one = jnp.sum(grad_entering_one, axis=1)
            grad_scale_one = jnp.sum(grad_entering_one * normed_one, axis=1)
            grad_input = grad_middle + norm_back(
                grad_entering_one * (1.0 + scale1), normed_one, inverse_one
            )


        grad_modulation = jnp.stack(
            [grad_shift_one, grad_scale_one, grad_gate_one, grad_shift_two, grad_scale_two, grad_gate_two],
            axis=1,
        )
        totals = (joint_total, mixer_total, up_total, down_total)
        return output, grad_input.astype(jnp.bfloat16), grad_modulation, totals

    pieces = [
        clip_pass(residual[i : i + 1], upstream[i : i + 1], modulation[i : i + 1])
        for i in range(clips)
    ]
    output = jnp.concatenate([p[0] for p in pieces], axis=0)
    grad_input_low = jnp.concatenate([p[1] for p in pieces], axis=0)
    grad_modulation = jnp.concatenate([p[2] for p in pieces], axis=0)
    joint_total, mixer_total, up_total, down_total = (
        sum(p[3][k] for p in pieces[1:]) + pieces[0][3][k] for k in range(4)
    )
    with jax.named_scope("ada_grad"):
        grad_columns = lax.all_to_all(
            grad_modulation.reshape(clips, 1, 6, model_width), "tensor", 3, 1, tiled=True
        )
        grad_all = lax.all_gather(grad_columns, ("dp", "frame"), axis=0, tiled=True)
        grad_all = grad_all.reshape(replicas * halves, clips, groups, 6, local_width)
        adaptive_total = jnp.einsum(
            "acgd,acgkw->dkw",
            my_condition.astype(jnp.float32),
            grad_all,
            precision=highest,
        )

    with jax.named_scope("weight_grads"):
        summed = tuple(
            lax.psum_scatter(
                total.astype(jnp.bfloat16), ("dp", "frame"), scatter_dimension=0, tiled=True
            ).astype(jnp.float32)
            for total in (joint_total, mixer_total, up_total, down_total)
        )
    result = output[:, None]
    input_grad = grad_input_low[:, None]
    return (result, input_grad, summed[0], summed[1], summed[2], summed[3], adaptive_total)


def solution(mesh):
    return jax.shard_map(
        on_device,
        mesh=mesh,
        in_specs=(
            P("dp", ("frame", "tensor"), None, None),
            P("dp", ("frame", "tensor"), None, None),
            P("dp", "frame"),
            P(("dp", "frame"), None, "tensor"),
            P(("dp", "frame"), "tensor"),
            P(("dp", "frame"), "tensor"),
            P(("dp", "frame"), "tensor"),
            P(("dp", "frame"), None, "tensor"),
        ),
        out_specs=(
            P("dp", ("frame", "tensor"), None, None),
            P("dp", ("frame", "tensor"), None, None),
            P(("dp", "frame"), None, "tensor"),
            P(("dp", "frame"), "tensor"),
            P(("dp", "frame"), "tensor"),
            P(("dp", "frame"), "tensor"),
            P(("dp", "frame"), None, "tensor"),
        ),
        check_vma=False,
    )
```

```python
import math

import jax
import jax.numpy as jnp
from jax import lax
from jax.sharding import PartitionSpec as P

HEAD_DIM = 64


epsilon = 1e-06
highest = lax.Precision.HIGHEST


def normalize(values):
    center = values - jnp.mean(values, axis=-1, keepdims=True)
    spread = jnp.mean(center * center, axis=-1, keepdims=True)
    inverse = lax.rsqrt(spread + epsilon)
    return (center * inverse, inverse)


def norm_back(upstream, normed, inverse):
    upstream_mean = jnp.mean(upstream, axis=-1, keepdims=True)
    product_mean = jnp.mean(upstream * normed, axis=-1, keepdims=True)
    return inverse * (upstream - upstream_mean - normed * product_mean)


def level_embedding(levels, model_width):
    halfway = model_width // 2
    frequency = jnp.exp(-math.log(10000.0) * jnp.arange(halfway, dtype=jnp.float32) / halfway)
    angles = levels.astype(jnp.float32)[..., None] * frequency
    return jnp.concatenate([jnp.cos(angles), jnp.sin(angles)], axis=-1)


def gelu_tanh(values):
    return jax.nn.gelu(values, approximate=True)


def on_device(
    tokens, out_grad, noise_index, qkv_weight, out_weight, up_weight, down_weight, ada_weight
):
    clips = tokens.shape[0]
    patches = tokens.shape[2]
    model_width = tokens.shape[-1]
    local_width = qkv_weight.shape[2]
    rows_here = qkv_weight.shape[0]
    heads_here = local_width // HEAD_DIM
    scaling = HEAD_DIM ** (-0.5)
    groups = lax.axis_size("tensor")
    halves = lax.axis_size("frame")
    replicas = lax.axis_size("dp")

    with jax.named_scope("modulation"):
        levels_all = lax.all_gather(noise_index, ("dp", "frame"), axis=0, tiled=True)
        levels_all = levels_all.reshape(replicas * halves, clips, groups)
        condition_all = jax.nn.silu(level_embedding(levels_all, model_width)).astype(jnp.bfloat16)
        row_block = lax.axis_index("dp") * halves + lax.axis_index("frame")
        my_condition = lax.dynamic_slice_in_dim(
            condition_all, row_block * rows_here, rows_here, axis=3
        )
        partial_mod = jnp.einsum(
            "acgd,dkw->acgkw", my_condition, ada_weight, preferred_element_type=jnp.float32
        )
        summed_mod = jnp.sum(
            lax.all_to_all(partial_mod, ("dp", "frame"), 0, 0, tiled=True), axis=0
        )
        group_mod = lax.all_gather(summed_mod, "tensor", axis=3, tiled=True)
        group_mod = jnp.swapaxes(group_mod, 1, 2)[:, :, :, None, :]
        group_index = lax.axis_index("tensor")
        modulation = lax.dynamic_index_in_dim(group_mod, group_index, axis=2, keepdims=False)

    with jax.named_scope("weights"):
        joint_weight, mixer_weight, upward_weight, downward_weight = (
            lax.all_gather(w, ("dp", "frame"), axis=0, tiled=True)
            for w in (qkv_weight, out_weight, up_weight, down_weight)
        )

    residual = tokens[:, 0].astype(jnp.float32)
    upstream = out_grad[:, 0].astype(jnp.float32)
    with jax.named_scope("group_inputs"):
        group_tokens = lax.all_gather(tokens[:, 0], "tensor", axis=1, tiled=True)
        group_upstream = lax.all_gather(out_grad[:, 0], "tensor", axis=1, tiled=True)
    def gather_halves(values):
        if halves != 2:
            return lax.all_gather(values, "frame", axis=1, tiled=True)
        other = lax.ppermute(values, "frame", [(0, 1), (1, 0)])
        return jnp.concatenate([values, other], axis=1)

    def scatter_halves(values):
        if halves != 2:
            return lax.psum_scatter(
                values.astype(jnp.bfloat16), "frame", scatter_dimension=1, tiled=True
            ).astype(jnp.float32)
        count = values.shape[1] // 2
        mine = values[:, :count]
        other = lax.ppermute(values[:, count:].astype(jnp.bfloat16), "frame", [(0, 1), (1, 0)])
        return mine.astype(jnp.bfloat16).astype(jnp.float32) + other.astype(jnp.float32)

    def clip_pass(residual, upstream, modulation, group_tokens, group_upstream, group_mod):
        clips = residual.shape[0]
        patches = residual.shape[1]
        shift1, scale1, gate1 = modulation[:, 0], modulation[:, 1], modulation[:, 2]
        shift2, scale2, gate2 = modulation[:, 3], modulation[:, 4], modulation[:, 5]
        def gather_tokens(values):
            return lax.all_gather(values, "tensor", axis=1, tiled=True)

        def scatter_tokens(values):
            parts = values.astype(jnp.bfloat16).reshape(
                values.shape[0], groups, -1, values.shape[-1]
            )
            received = lax.all_to_all(parts, "tensor", 1, 1, tiled=True)
            return jnp.sum(received.astype(jnp.float32), axis=1)

        with jax.named_scope("forward"):
            normed_one, inverse_one = normalize(residual)
            group_normed, _ = normalize(
                group_tokens.astype(jnp.float32).reshape(clips, groups, patches, model_width)
            )
            flat_one = (
                (group_normed * (1.0 + group_mod[:, 1]) + group_mod[:, 0])
                .astype(jnp.bfloat16)
                .reshape(clips, groups * patches, model_width)
            )
            token_count = flat_one.shape[1]
            projected = jnp.einsum(
                "crd,dkh->crkh", flat_one, joint_weight, preferred_element_type=jnp.float32
            ).astype(jnp.bfloat16)
            queries = projected[:, :, 0]
            keys_all = gather_halves(projected[:, :, 1])
            values_all = gather_halves(projected[:, :, 2])
            key_heads = keys_all.reshape(clips, -1, heads_here, HEAD_DIM)
            value_heads = values_all.reshape(clips, -1, heads_here, HEAD_DIM)
            block_rows = min(512, token_count)
            block_count = token_count // block_rows
            query_blocks = jnp.moveaxis(
                queries.reshape(clips, block_count, block_rows, heads_here, HEAD_DIM), 1, 0
            )

            def attend(query_block):
                scores = (
                    jnp.einsum(
                        "cqhe,ckhe->chqk", query_block, key_heads, preferred_element_type=jnp.float32
                    )
                    * scaling
                )
                largest = jnp.max(scores, axis=-1, keepdims=True)
                raised = jnp.exp(scores - largest)
                totals_row = jnp.sum(raised, axis=-1, keepdims=True)
                probs_low = (raised / totals_row).astype(jnp.bfloat16)
                outputs = jnp.einsum(
                    "chqk,ckhe->cqhe", probs_low, value_heads, preferred_element_type=jnp.float32
                )
                return (outputs.astype(jnp.bfloat16), (largest + jnp.log(totals_row))[..., 0])

            attended_blocks, log_totals = lax.map(attend, query_blocks)
            attended = jnp.moveaxis(attended_blocks, 0, 1).reshape(clips, token_count, local_width)
            partial_one = jnp.einsum(
                "crh,oh->cro", attended, mixer_weight, preferred_element_type=jnp.float32
            )
            branch_one = scatter_tokens(partial_one)
            middle = residual + gate1 * branch_one
            normed_two, inverse_two = normalize(middle)
            entering_two = (normed_two * (1.0 + scale2) + shift2).astype(jnp.bfloat16)
            flat_two = gather_tokens(entering_two)
            up_values = jnp.einsum(
                "crd,df->crf", flat_two, upward_weight, preferred_element_type=jnp.float32
            )
            hidden = gelu_tanh(up_values).astype(jnp.bfloat16)
            partial_two = jnp.einsum(
                "crf,of->cro", hidden, downward_weight, preferred_element_type=jnp.float32
            )
            branch_two = scatter_tokens(partial_two)
            output = (middle + gate2 * branch_two).astype(jnp.bfloat16)

        with jax.named_scope("backward_ffn"):
            grad_gate_two = jnp.sum(upstream * branch_two, axis=1)
            grad_two_all = (
                (
                    group_mod[:, 5]
                    * group_upstream.astype(jnp.float32).reshape(clips, groups, patches, model_width)
                )
                .astype(jnp.bfloat16)
                .reshape(clips, groups * patches, model_width)
            )
            grad_hidden = jnp.einsum(
                "cro,of->crf", grad_two_all, downward_weight, preferred_element_type=jnp.float32
            )
            down_total = jnp.einsum(
                "cro,crf->of", grad_two_all, hidden, preferred_element_type=jnp.float32
            )
            _, gelu_pullback = jax.vjp(gelu_tanh, up_values)
            grad_up = gelu_pullback(grad_hidden)[0].astype(jnp.bfloat16)
            up_total = jnp.einsum(
                "crd,crf->df", flat_two, grad_up, preferred_element_type=jnp.float32
            )
            partial_back_two = jnp.einsum(
                "crf,df->crd", grad_up, upward_weight, preferred_element_type=jnp.float32
            )
            grad_entering_two = scatter_tokens(partial_back_two)
            grad_shift_two = jnp.sum(grad_entering_two, axis=1)
            grad_scale_two = jnp.sum(grad_entering_two * normed_two, axis=1)
            grad_middle = upstream + norm_back(
                grad_entering_two * (1.0 + scale2), normed_two, inverse_two
            )
            grad_gate_one = jnp.sum(grad_middle * branch_one, axis=1)

        with jax.named_scope("backward_attention"):
            grad_branch_one = (gate1 * grad_middle).astype(jnp.bfloat16)
            grad_one_all = gather_tokens(grad_branch_one)
            grad_attended = jnp.einsum(
                "cro,oh->crh", grad_one_all, mixer_weight, preferred_element_type=jnp.float32
            ).astype(jnp.bfloat16)
            mixer_total = jnp.einsum(
                "cro,crh->oh", grad_one_all, attended, preferred_element_type=jnp.float32
            )
            grad_blocks = jnp.moveaxis(
                grad_attended.reshape(clips, block_count, block_rows, heads_here, HEAD_DIM), 1, 0
            )

            def attend_back(carried, pieces):
                key_sum, value_sum = carried
                query_block, grad_block, log_block = pieces
                scores = (
                    jnp.einsum(
                        "cqhe,ckhe->chqk", query_block, key_heads, preferred_element_type=jnp.float32
                    )
                    * scaling
                )
                probs = jnp.exp(scores - log_block[..., None])
                grad_probs = jnp.einsum(
                    "cqhe,ckhe->chqk", grad_block, value_heads, preferred_element_type=jnp.float32
                )
                value_sum = value_sum + jnp.einsum(
                    "chqk,cqhe->ckhe",
                    probs.astype(jnp.bfloat16),
                    grad_block,
                    preferred_element_type=jnp.float32,
                )
                row_terms = jnp.sum(probs * grad_probs, axis=-1, keepdims=True)
                grad_scores = (probs * (grad_probs - row_terms)).astype(jnp.bfloat16)
                grad_queries = (
                    jnp.einsum(
                        "chqk,ckhe->cqhe", grad_scores, key_heads, preferred_element_type=jnp.float32
                    )
                    * scaling
                )
                key_sum = (
                    key_sum
                    + jnp.einsum(
                        "chqk,cqhe->ckhe", grad_scores, query_block, preferred_element_type=jnp.float32
                    )
                    * scaling
                )
                return ((key_sum, value_sum), grad_queries)

            zeros_keys = jnp.zeros(key_heads.shape, jnp.float32)
            (key_grads, value_grads), query_grads = lax.scan(
                attend_back, (zeros_keys, zeros_keys), (query_blocks, grad_blocks, log_totals)
            )
            query_grads = jnp.moveaxis(query_grads, 0, 1).reshape(clips, token_count, local_width)
            key_own, value_own = (
                scatter_halves(grads.reshape(clips, -1, local_width))
                for grads in (key_grads, value_grads)
            )
            grad_projected = jnp.stack([query_grads, key_own, value_own], axis=2).astype(
                jnp.bfloat16
            )
            joint_total = jnp.einsum(
                "crd,crkh->dkh", flat_one, grad_projected, preferred_element_type=jnp.float32
            )
            partial_back_one = jnp.einsum(
                "crkh,dkh->crd", grad_projected, joint_weight, preferred_element_type=jnp.float32
            )
            grad_entering_one = scatter_tokens(partial_back_one)
            grad_shift_one = jnp.sum(grad_entering_one, axis=1)
            grad_scale_one = jnp.sum(grad_entering_one * normed_one, axis=1)
            grad_input = grad_middle + norm_back(
                grad_entering_one * (1.0 + scale1), normed_one, inverse_one
            )


        grad_modulation = jnp.stack(
            [grad_shift_one, grad_scale_one, grad_gate_one, grad_shift_two, grad_scale_two, grad_gate_two],
            axis=1,
        )
        totals = (joint_total, mixer_total, up_total, down_total)
        return output, grad_input.astype(jnp.bfloat16), grad_modulation, totals

    pieces = [
        clip_pass(
            residual[i : i + 1],
            upstream[i : i + 1],
            modulation[i : i + 1],
            group_tokens[i : i + 1],
            group_upstream[i : i + 1],
            group_mod[i : i + 1],
        )
        for i in range(clips)
    ]
    output = jnp.concatenate([p[0] for p in pieces], axis=0)
    grad_input_low = jnp.concatenate([p[1] for p in pieces], axis=0)
    grad_modulation = jnp.concatenate([p[2] for p in pieces], axis=0)
    joint_total, mixer_total, up_total, down_total = (
        sum(p[3][k] for p in pieces[1:]) + pieces[0][3][k] for k in range(4)
    )
    with jax.named_scope("ada_grad"):
        grad_columns = lax.all_to_all(
            grad_modulation.reshape(clips, 1, 6, model_width), "tensor", 3, 1, tiled=True
        )
        grad_all = lax.all_gather(grad_columns, ("dp", "frame"), axis=0, tiled=True)
        grad_all = grad_all.reshape(replicas * halves, clips, groups, 6, local_width)
        adaptive_total = jnp.einsum(
            "acgd,acgkw->dkw",
            my_condition.astype(jnp.float32),
            grad_all,
            precision=highest,
        )

    with jax.named_scope("weight_grads"):
        summed = tuple(
            lax.psum_scatter(
                total.astype(jnp.bfloat16), ("dp", "frame"), scatter_dimension=0, tiled=True
            ).astype(jnp.float32)
            for total in (joint_total, mixer_total, up_total, down_total)
        )
    result = output[:, None]
    input_grad = grad_input_low[:, None]
    return (result, input_grad, summed[0], summed[1], summed[2], summed[3], adaptive_total)


def solution(mesh):
    return jax.shard_map(
        on_device,
        mesh=mesh,
        in_specs=(
            P("dp", ("frame", "tensor"), None, None),
            P("dp", ("frame", "tensor"), None, None),
            P("dp", "frame"),
            P(("dp", "frame"), None, "tensor"),
            P(("dp", "frame"), "tensor"),
            P(("dp", "frame"), "tensor"),
            P(("dp", "frame"), "tensor"),
            P(("dp", "frame"), None, "tensor"),
        ),
        out_specs=(
            P("dp", ("frame", "tensor"), None, None),
            P("dp", ("frame", "tensor"), None, None),
            P(("dp", "frame"), None, "tensor"),
            P(("dp", "frame"), "tensor"),
            P(("dp", "frame"), "tensor"),
            P(("dp", "frame"), "tensor"),
            P(("dp", "frame"), None, "tensor"),
        ),
        check_vma=False,
    )
```

```python
import functools
import math

import jax
import jax.numpy as jnp
from jax import lax
from jax.experimental import pallas as pl
from jax.experimental.pallas import tpu as pltpu
from jax.sharding import PartitionSpec as P

HEAD_DIM = 64


epsilon = 1e-06
highest = lax.Precision.HIGHEST


def normalize(values):
    center = values - jnp.mean(values, axis=-1, keepdims=True)
    spread = jnp.mean(center * center, axis=-1, keepdims=True)
    inverse = lax.rsqrt(spread + epsilon)
    return (center * inverse, inverse)


def norm_back(upstream, normed, inverse):
    upstream_mean = jnp.mean(upstream, axis=-1, keepdims=True)
    product_mean = jnp.mean(upstream * normed, axis=-1, keepdims=True)
    return inverse * (upstream - upstream_mean - normed * product_mean)


def level_embedding(levels, model_width):
    halfway = model_width // 2
    frequency = jnp.exp(-math.log(10000.0) * jnp.arange(halfway, dtype=jnp.float32) / halfway)
    angles = levels.astype(jnp.float32)[..., None] * frequency
    return jnp.concatenate([jnp.cos(angles), jnp.sin(angles)], axis=-1)


def _nt(a, b):
    return lax.dot_general(a, b, (((1,), (1,)), ((), ())), preferred_element_type=jnp.float32)


def _tn(a, b):
    return lax.dot_general(a, b, (((0,), (0,)), ((), ())), preferred_element_type=jnp.float32)


def _forward_kernel(heads, scaling, q_ref, k_ref, v_ref, o_ref, lse_ref):
    for h in range(heads):
        cols = slice(h * HEAD_DIM, (h + 1) * HEAD_DIM)
        scores = _nt(q_ref[:, cols], k_ref[:, cols]) * scaling
        largest = jnp.max(scores, axis=1, keepdims=True)
        raised = jnp.exp(scores - largest)
        total = jnp.sum(raised, axis=1, keepdims=True)
        probs_low = (raised / total).astype(jnp.bfloat16)
        out = jnp.dot(probs_low, v_ref[:, cols], preferred_element_type=jnp.float32)
        o_ref[:, cols] = out.astype(o_ref.dtype)
        lse_ref[:, h : h + 1] = largest + jnp.log(total)


def _backward_kernel(heads, scaling, q_ref, k_ref, v_ref, g_ref, lse_ref, dq_ref, dk_ref, dv_ref):
    @pl.when(pl.program_id(0) == 0)
    def _():
        dk_ref[...] = jnp.zeros_like(dk_ref)
        dv_ref[...] = jnp.zeros_like(dv_ref)

    for h in range(heads):
        cols = slice(h * HEAD_DIM, (h + 1) * HEAD_DIM)
        q = q_ref[:, cols]
        g = g_ref[:, cols]
        scores = _nt(q, k_ref[:, cols]) * scaling
        probs = jnp.exp(scores - lse_ref[:, h : h + 1])
        grad_probs = _nt(g, v_ref[:, cols])
        dv_ref[:, cols] += _tn(probs.astype(jnp.bfloat16), g)
        row_terms = jnp.sum(probs * grad_probs, axis=1, keepdims=True)
        grad_scores = (probs * (grad_probs - row_terms)).astype(jnp.bfloat16)
        dq_ref[:, cols] = jnp.dot(grad_scores, k_ref[:, cols], preferred_element_type=jnp.float32) * scaling
        dk_ref[:, cols] += _tn(grad_scores, q) * scaling


def attention_forward(queries, keys, values, block_rows=256):
    rows, width = queries.shape
    length = keys.shape[0]
    heads = width // HEAD_DIM
    block_rows = min(block_rows, rows)
    flops = 4 * rows * length * width
    return pl.pallas_call(
        functools.partial(_forward_kernel, heads, HEAD_DIM ** (-0.5)),
        out_shape=(
            jax.ShapeDtypeStruct((rows, width), jnp.bfloat16),
            jax.ShapeDtypeStruct((rows, heads), jnp.float32),
        ),
        grid=(rows // block_rows,),
        in_specs=[
            pl.BlockSpec((block_rows, width), lambda i: (i, 0)),
            pl.BlockSpec((length, width), lambda i: (0, 0)),
            pl.BlockSpec((length, width), lambda i: (0, 0)),
        ],
        out_specs=[
            pl.BlockSpec((block_rows, width), lambda i: (i, 0)),
            pl.BlockSpec((block_rows, heads), lambda i: (i, 0)),
        ],
        compiler_params=pltpu.CompilerParams(
            dimension_semantics=("arbitrary",), vmem_limit_bytes=56 * 1024 * 1024
        ),
        cost_estimate=pl.CostEstimate(
            flops=flops,
            transcendentals=rows * length * heads,
            bytes_accessed=2 * (2 * rows * width + 2 * length * width),
        ),
    )(queries, keys, values)


def attention_backward(queries, keys, values, grad_out, lse, block_rows=256):
    rows, width = queries.shape
    length = keys.shape[0]
    heads = width // HEAD_DIM
    block_rows = min(block_rows, rows)
    flops = 10 * rows * length * width
    return pl.pallas_call(
        functools.partial(_backward_kernel, heads, HEAD_DIM ** (-0.5)),
        out_shape=(
            jax.ShapeDtypeStruct((rows, width), jnp.float32),
            jax.ShapeDtypeStruct((length, width), jnp.float32),
            jax.ShapeDtypeStruct((length, width), jnp.float32),
        ),
        grid=(rows // block_rows,),
        in_specs=[
            pl.BlockSpec((block_rows, width), lambda i: (i, 0)),
            pl.BlockSpec((length, width), lambda i: (0, 0)),
            pl.BlockSpec((length, width), lambda i: (0, 0)),
            pl.BlockSpec((block_rows, width), lambda i: (i, 0)),
            pl.BlockSpec((block_rows, heads), lambda i: (i, 0)),
        ],
        out_specs=[
            pl.BlockSpec((block_rows, width), lambda i: (i, 0)),
            pl.BlockSpec((length, width), lambda i: (0, 0)),
            pl.BlockSpec((length, width), lambda i: (0, 0)),
        ],
        compiler_params=pltpu.CompilerParams(
            dimension_semantics=("arbitrary",), vmem_limit_bytes=56 * 1024 * 1024
        ),
        cost_estimate=pl.CostEstimate(
            flops=flops,
            transcendentals=rows * length * heads,
            bytes_accessed=2 * (3 * rows * width + 2 * length * width) + 4 * (rows + 2 * length) * width,
        ),
    )(queries, keys, values, grad_out, lse)


def gelu_tanh(values):
    return jax.nn.gelu(values, approximate=True)


def on_device(
    tokens, out_grad, noise_index, qkv_weight, out_weight, up_weight, down_weight, ada_weight
):
    clips = tokens.shape[0]
    patches = tokens.shape[2]
    model_width = tokens.shape[-1]
    local_width = qkv_weight.shape[2]
    rows_here = qkv_weight.shape[0]
    heads_here = local_width // HEAD_DIM
    scaling = HEAD_DIM ** (-0.5)
    groups = lax.axis_size("tensor")
    halves = lax.axis_size("frame")
    replicas = lax.axis_size("dp")

    with jax.named_scope("modulation"):
        levels_all = lax.all_gather(noise_index, ("dp", "frame"), axis=0, tiled=True)
        levels_all = levels_all.reshape(replicas * halves, clips, groups)
        condition_all = jax.nn.silu(level_embedding(levels_all, model_width)).astype(jnp.bfloat16)
        row_block = lax.axis_index("dp") * halves + lax.axis_index("frame")
        my_condition = lax.dynamic_slice_in_dim(
            condition_all, row_block * rows_here, rows_here, axis=3
        )
        partial_mod = jnp.einsum(
            "acgd,dkw->acgkw", my_condition, ada_weight, preferred_element_type=jnp.float32
        )
        summed_mod = jnp.sum(
            lax.all_to_all(partial_mod, ("dp", "frame"), 0, 0, tiled=True), axis=0
        )
        group_mod = lax.all_gather(summed_mod, "tensor", axis=3, tiled=True)
        group_mod = jnp.swapaxes(group_mod, 1, 2)[:, :, :, None, :]
        group_index = lax.axis_index("tensor")
        modulation = lax.dynamic_index_in_dim(group_mod, group_index, axis=2, keepdims=False)

    with jax.named_scope("weights"):
        joint_weight, mixer_weight, upward_weight, downward_weight = (
            lax.all_gather(w, ("dp", "frame"), axis=0, tiled=True)
            for w in (qkv_weight, out_weight, up_weight, down_weight)
        )

    residual = tokens[:, 0].astype(jnp.float32)
    upstream = out_grad[:, 0].astype(jnp.float32)
    with jax.named_scope("group_inputs"):
        group_tokens = lax.all_gather(tokens[:, 0], "tensor", axis=1, tiled=True)
        group_upstream = lax.all_gather(out_grad[:, 0], "tensor", axis=1, tiled=True)
    def gather_halves(values):
        if halves != 2:
            return lax.all_gather(values, "frame", axis=1, tiled=True)
        other = lax.ppermute(values, "frame", [(0, 1), (1, 0)])
        return jnp.concatenate([values, other], axis=1)

    def scatter_halves(values):
        if halves != 2:
            return lax.psum_scatter(
                values.astype(jnp.bfloat16), "frame", scatter_dimension=1, tiled=True
            ).astype(jnp.float32)
        count = values.shape[1] // 2
        mine = values[:, :count]
        other = lax.ppermute(values[:, count:].astype(jnp.bfloat16), "frame", [(0, 1), (1, 0)])
        return mine.astype(jnp.bfloat16).astype(jnp.float32) + other.astype(jnp.float32)

    def clip_pass(residual, upstream, modulation, group_tokens, group_upstream, group_mod):
        clips = residual.shape[0]
        patches = residual.shape[1]
        shift1, scale1, gate1 = modulation[:, 0], modulation[:, 1], modulation[:, 2]
        shift2, scale2, gate2 = modulation[:, 3], modulation[:, 4], modulation[:, 5]
        def gather_tokens(values):
            return lax.all_gather(values, "tensor", axis=1, tiled=True)

        def scatter_tokens(values):
            parts = values.astype(jnp.bfloat16).reshape(
                values.shape[0], groups, -1, values.shape[-1]
            )
            received = lax.all_to_all(parts, "tensor", 1, 1, tiled=True)
            return jnp.sum(received.astype(jnp.float32), axis=1)

        with jax.named_scope("forward"):
            normed_one, inverse_one = normalize(residual)
            group_normed, _ = normalize(
                group_tokens.astype(jnp.float32).reshape(clips, groups, patches, model_width)
            )
            flat_one = (
                (group_normed * (1.0 + group_mod[:, 1]) + group_mod[:, 0])
                .astype(jnp.bfloat16)
                .reshape(clips, groups * patches, model_width)
            )
            token_count = flat_one.shape[1]
            projected = jnp.einsum(
                "crd,dkh->crkh", flat_one, joint_weight, preferred_element_type=jnp.float32
            ).astype(jnp.bfloat16)
            queries = projected[:, :, 0]
            keys_all = gather_halves(projected[:, :, 1])
            values_all = gather_halves(projected[:, :, 2])
            attended, log_totals = attention_forward(queries[0], keys_all[0], values_all[0])
            attended = attended[None]
            partial_one = jnp.einsum(
                "crh,oh->cro", attended, mixer_weight, preferred_element_type=jnp.float32
            )
            branch_one = scatter_tokens(partial_one)
            middle = residual + gate1 * branch_one
            normed_two, inverse_two = normalize(middle)
            entering_two = (normed_two * (1.0 + scale2) + shift2).astype(jnp.bfloat16)
            flat_two = gather_tokens(entering_two)
            up_values = jnp.einsum(
                "crd,df->crf", flat_two, upward_weight, preferred_element_type=jnp.float32
            )
            hidden = gelu_tanh(up_values).astype(jnp.bfloat16)
            partial_two = jnp.einsum(
                "crf,of->cro", hidden, downward_weight, preferred_element_type=jnp.float32
            )
            branch_two = scatter_tokens(partial_two)
            output = (middle + gate2 * branch_two).astype(jnp.bfloat16)

        with jax.named_scope("backward_ffn"):
            grad_gate_two = jnp.sum(upstream * branch_two, axis=1)
            grad_two_all = (
                (
                    group_mod[:, 5]
                    * group_upstream.astype(jnp.float32).reshape(clips, groups, patches, model_width)
                )
                .astype(jnp.bfloat16)
                .reshape(clips, groups * patches, model_width)
            )
            grad_hidden = jnp.einsum(
                "cro,of->crf", grad_two_all, downward_weight, preferred_element_type=jnp.float32
            )
            down_total = jnp.einsum(
                "cro,crf->of", grad_two_all, hidden, preferred_element_type=jnp.float32
            )
            _, gelu_pullback = jax.vjp(gelu_tanh, up_values)
            grad_up = gelu_pullback(grad_hidden)[0].astype(jnp.bfloat16)
            up_total = jnp.einsum(
                "crd,crf->df", flat_two, grad_up, preferred_element_type=jnp.float32
            )
            partial_back_two = jnp.einsum(
                "crf,df->crd", grad_up, upward_weight, preferred_element_type=jnp.float32
            )
            grad_entering_two = scatter_tokens(partial_back_two)
            grad_shift_two = jnp.sum(grad_entering_two, axis=1)
            grad_scale_two = jnp.sum(grad_entering_two * normed_two, axis=1)
            grad_middle = upstream + norm_back(
                grad_entering_two * (1.0 + scale2), normed_two, inverse_two
            )
            grad_gate_one = jnp.sum(grad_middle * branch_one, axis=1)

        with jax.named_scope("backward_attention"):
            grad_branch_one = (gate1 * grad_middle).astype(jnp.bfloat16)
            grad_one_all = gather_tokens(grad_branch_one)
            grad_attended = jnp.einsum(
                "cro,oh->crh", grad_one_all, mixer_weight, preferred_element_type=jnp.float32
            ).astype(jnp.bfloat16)
            mixer_total = jnp.einsum(
                "cro,crh->oh", grad_one_all, attended, preferred_element_type=jnp.float32
            )
            query_grads, key_grads, value_grads = attention_backward(
                queries[0], keys_all[0], values_all[0], grad_attended[0], log_totals
            )
            query_grads = query_grads[None]
            key_grads = key_grads[None]
            value_grads = value_grads[None]
            key_own, value_own = (
                scatter_halves(grads.reshape(clips, -1, local_width))
                for grads in (key_grads, value_grads)
            )
            grad_projected = jnp.stack([query_grads, key_own, value_own], axis=2).astype(
                jnp.bfloat16
            )
            joint_total = jnp.einsum(
                "crd,crkh->dkh", flat_one, grad_projected, preferred_element_type=jnp.float32
            )
            partial_back_one = jnp.einsum(
                "crkh,dkh->crd", grad_projected, joint_weight, preferred_element_type=jnp.float32
            )
            grad_entering_one = scatter_tokens(partial_back_one)
            grad_shift_one = jnp.sum(grad_entering_one, axis=1)
            grad_scale_one = jnp.sum(grad_entering_one * normed_one, axis=1)
            grad_input = grad_middle + norm_back(
                grad_entering_one * (1.0 + scale1), normed_one, inverse_one
            )


        grad_modulation = jnp.stack(
            [grad_shift_one, grad_scale_one, grad_gate_one, grad_shift_two, grad_scale_two, grad_gate_two],
            axis=1,
        )
        totals = (joint_total, mixer_total, up_total, down_total)
        return output, grad_input.astype(jnp.bfloat16), grad_modulation, totals

    pieces = [
        clip_pass(
            residual[i : i + 1],
            upstream[i : i + 1],
            modulation[i : i + 1],
            group_tokens[i : i + 1],
            group_upstream[i : i + 1],
            group_mod[i : i + 1],
        )
        for i in range(clips)
    ]
    output = jnp.concatenate([p[0] for p in pieces], axis=0)
    grad_input_low = jnp.concatenate([p[1] for p in pieces], axis=0)
    grad_modulation = jnp.concatenate([p[2] for p in pieces], axis=0)
    joint_total, mixer_total, up_total, down_total = (
        sum(p[3][k] for p in pieces[1:]) + pieces[0][3][k] for k in range(4)
    )
    with jax.named_scope("ada_grad"):
        grad_columns = lax.all_to_all(
            grad_modulation.reshape(clips, 1, 6, model_width), "tensor", 3, 1, tiled=True
        )
        grad_all = lax.all_gather(grad_columns, ("dp", "frame"), axis=0, tiled=True)
        grad_all = grad_all.reshape(replicas * halves, clips, groups, 6, local_width)
        adaptive_total = jnp.einsum(
            "acgd,acgkw->dkw",
            my_condition.astype(jnp.float32),
            grad_all,
            precision=highest,
        )

    with jax.named_scope("weight_grads"):
        summed = tuple(
            lax.psum_scatter(
                total.astype(jnp.bfloat16), ("dp", "frame"), scatter_dimension=0, tiled=True
            ).astype(jnp.float32)
            for total in (joint_total, mixer_total, up_total, down_total)
        )
    result = output[:, None]
    input_grad = grad_input_low[:, None]
    return (result, input_grad, summed[0], summed[1], summed[2], summed[3], adaptive_total)


def solution(mesh):
    return jax.shard_map(
        on_device,
        mesh=mesh,
        in_specs=(
            P("dp", ("frame", "tensor"), None, None),
            P("dp", ("frame", "tensor"), None, None),
            P("dp", "frame"),
            P(("dp", "frame"), None, "tensor"),
            P(("dp", "frame"), "tensor"),
            P(("dp", "frame"), "tensor"),
            P(("dp", "frame"), "tensor"),
            P(("dp", "frame"), None, "tensor"),
        ),
        out_specs=(
            P("dp", ("frame", "tensor"), None, None),
            P("dp", ("frame", "tensor"), None, None),
            P(("dp", "frame"), None, "tensor"),
            P(("dp", "frame"), "tensor"),
            P(("dp", "frame"), "tensor"),
            P(("dp", "frame"), "tensor"),
            P(("dp", "frame"), None, "tensor"),
        ),
        check_vma=False,
    )
```

```python
import functools
import math

import jax
import jax.numpy as jnp
from jax import lax
from jax.experimental import pallas as pl
from jax.experimental.pallas import tpu as pltpu
from jax.sharding import PartitionSpec as P

HEAD_DIM = 64


epsilon = 1e-06
highest = lax.Precision.HIGHEST


def normalize(values):
    center = values - jnp.mean(values, axis=-1, keepdims=True)
    spread = jnp.mean(center * center, axis=-1, keepdims=True)
    inverse = lax.rsqrt(spread + epsilon)
    return (center * inverse, inverse)


def norm_back(upstream, normed, inverse):
    upstream_mean = jnp.mean(upstream, axis=-1, keepdims=True)
    product_mean = jnp.mean(upstream * normed, axis=-1, keepdims=True)
    return inverse * (upstream - upstream_mean - normed * product_mean)


def level_embedding(levels, model_width):
    halfway = model_width // 2
    frequency = jnp.exp(-math.log(10000.0) * jnp.arange(halfway, dtype=jnp.float32) / halfway)
    angles = levels.astype(jnp.float32)[..., None] * frequency
    return jnp.concatenate([jnp.cos(angles), jnp.sin(angles)], axis=-1)


def _nt(a, b):
    return lax.dot_general(a, b, (((1,), (1,)), ((), ())), preferred_element_type=jnp.float32)


def _tn(a, b):
    return lax.dot_general(a, b, (((0,), (0,)), ((), ())), preferred_element_type=jnp.float32)


def _forward_kernel(heads, scaling, q_ref, k_ref, v_ref, o_ref, lse_ref):
    for h in range(heads):
        cols = slice(h * HEAD_DIM, (h + 1) * HEAD_DIM)
        scores = _nt(q_ref[:, cols], k_ref[:, cols]) * scaling
        largest = jnp.max(scores, axis=1, keepdims=True)
        raised = jnp.exp(scores - largest)
        total = jnp.sum(raised, axis=1, keepdims=True)
        probs_low = (raised / total).astype(jnp.bfloat16)
        out = jnp.dot(probs_low, v_ref[:, cols], preferred_element_type=jnp.float32)
        o_ref[:, cols] = out.astype(o_ref.dtype)
        lse_ref[:, h : h + 1] = largest + jnp.log(total)


def _backward_kernel(heads, scaling, q_ref, k_ref, v_ref, g_ref, lse_ref, dq_ref, dk_ref, dv_ref):
    @pl.when(pl.program_id(0) == 0)
    def _():
        dk_ref[...] = jnp.zeros_like(dk_ref)
        dv_ref[...] = jnp.zeros_like(dv_ref)

    for h in range(heads):
        cols = slice(h * HEAD_DIM, (h + 1) * HEAD_DIM)
        q = q_ref[:, cols]
        g = g_ref[:, cols]
        scores = _nt(q, k_ref[:, cols]) * scaling
        probs = jnp.exp(scores - lse_ref[:, h : h + 1])
        grad_probs = _nt(g, v_ref[:, cols])
        dv_ref[:, cols] += _tn(probs.astype(jnp.bfloat16), g)
        row_terms = jnp.sum(probs * grad_probs, axis=1, keepdims=True)
        grad_scores = (probs * (grad_probs - row_terms)).astype(jnp.bfloat16)
        dq_ref[:, cols] = jnp.dot(grad_scores, k_ref[:, cols], preferred_element_type=jnp.float32) * scaling
        dk_ref[:, cols] += _tn(grad_scores, q) * scaling


def attention_forward(queries, keys, values, block_rows=256):
    rows, width = queries.shape
    length = keys.shape[0]
    heads = width // HEAD_DIM
    block_rows = min(block_rows, rows)
    flops = 4 * rows * length * width
    return pl.pallas_call(
        functools.partial(_forward_kernel, heads, HEAD_DIM ** (-0.5)),
        out_shape=(
            jax.ShapeDtypeStruct((rows, width), jnp.bfloat16),
            jax.ShapeDtypeStruct((rows, heads), jnp.float32),
        ),
        grid=(rows // block_rows,),
        in_specs=[
            pl.BlockSpec((block_rows, width), lambda i: (i, 0)),
            pl.BlockSpec((length, width), lambda i: (0, 0)),
            pl.BlockSpec((length, width), lambda i: (0, 0)),
        ],
        out_specs=[
            pl.BlockSpec((block_rows, width), lambda i: (i, 0)),
            pl.BlockSpec((block_rows, heads), lambda i: (i, 0)),
        ],
        compiler_params=pltpu.CompilerParams(
            dimension_semantics=("arbitrary",), vmem_limit_bytes=56 * 1024 * 1024
        ),
        cost_estimate=pl.CostEstimate(
            flops=flops,
            transcendentals=rows * length * heads,
            bytes_accessed=2 * (2 * rows * width + 2 * length * width),
        ),
    )(queries, keys, values)


def attention_backward(queries, keys, values, grad_out, lse, block_rows=256):
    rows, width = queries.shape
    length = keys.shape[0]
    heads = width // HEAD_DIM
    block_rows = min(block_rows, rows)
    flops = 10 * rows * length * width
    return pl.pallas_call(
        functools.partial(_backward_kernel, heads, HEAD_DIM ** (-0.5)),
        out_shape=(
            jax.ShapeDtypeStruct((rows, width), jnp.float32),
            jax.ShapeDtypeStruct((length, width), jnp.float32),
            jax.ShapeDtypeStruct((length, width), jnp.float32),
        ),
        grid=(rows // block_rows,),
        in_specs=[
            pl.BlockSpec((block_rows, width), lambda i: (i, 0)),
            pl.BlockSpec((length, width), lambda i: (0, 0)),
            pl.BlockSpec((length, width), lambda i: (0, 0)),
            pl.BlockSpec((block_rows, width), lambda i: (i, 0)),
            pl.BlockSpec((block_rows, heads), lambda i: (i, 0)),
        ],
        out_specs=[
            pl.BlockSpec((block_rows, width), lambda i: (i, 0)),
            pl.BlockSpec((length, width), lambda i: (0, 0)),
            pl.BlockSpec((length, width), lambda i: (0, 0)),
        ],
        compiler_params=pltpu.CompilerParams(
            dimension_semantics=("arbitrary",), vmem_limit_bytes=56 * 1024 * 1024
        ),
        cost_estimate=pl.CostEstimate(
            flops=flops,
            transcendentals=rows * length * heads,
            bytes_accessed=2 * (3 * rows * width + 2 * length * width) + 4 * (rows + 2 * length) * width,
        ),
    )(queries, keys, values, grad_out, lse)


def gelu_tanh(values):
    return jax.nn.gelu(values, approximate=True)


def on_device(
    tokens, out_grad, noise_index, qkv_weight, out_weight, up_weight, down_weight, ada_weight
):
    clips = tokens.shape[0]
    patches = tokens.shape[2]
    model_width = tokens.shape[-1]
    local_width = qkv_weight.shape[2]
    rows_here = qkv_weight.shape[0]
    heads_here = local_width // HEAD_DIM
    scaling = HEAD_DIM ** (-0.5)
    groups = lax.axis_size("tensor")
    halves = lax.axis_size("frame")
    replicas = lax.axis_size("dp")

    with jax.named_scope("modulation"):
        levels_all = lax.all_gather(noise_index, ("dp", "frame"), axis=0, tiled=True)
        levels_all = levels_all.reshape(replicas * halves, clips, groups)
        condition_all = jax.nn.silu(level_embedding(levels_all, model_width)).astype(jnp.bfloat16)
        row_block = lax.axis_index("dp") * halves + lax.axis_index("frame")
        my_condition = lax.dynamic_slice_in_dim(
            condition_all, row_block * rows_here, rows_here, axis=3
        )
        partial_mod = jnp.einsum(
            "acgd,dkw->acgkw", my_condition, ada_weight, preferred_element_type=jnp.float32
        )
        summed_mod = jnp.sum(
            lax.all_to_all(partial_mod, ("dp", "frame"), 0, 0, tiled=True), axis=0
        )
        group_mod = lax.all_gather(summed_mod, "tensor", axis=3, tiled=True)
        group_mod = jnp.swapaxes(group_mod, 1, 2)[:, :, :, None, :]
        group_index = lax.axis_index("tensor")
        modulation = lax.dynamic_index_in_dim(group_mod, group_index, axis=2, keepdims=False)

    frame_index = lax.axis_index("frame")

    def order_by_half(mine, other):
        both = jnp.stack([mine, other])
        return jnp.where(frame_index == 0, both, both[::-1])

    def hidden_half(weight):
        half = weight.shape[1] // halves
        blocks = weight.reshape(rows_here, halves, half)
        mine = jnp.take(blocks, frame_index, axis=1)
        sent = jnp.take(blocks, 1 - frame_index, axis=1)
        received = lax.ppermute(sent, "frame", [(0, 1), (1, 0)])
        rows = order_by_half(mine, received).reshape(halves * rows_here, half)
        gathered = lax.all_gather(rows, ("dp", "tensor"), axis=0, tiled=True)
        gathered = gathered.reshape(replicas, groups, halves * rows_here, half)
        return jnp.swapaxes(gathered, 1, 2).reshape(model_width, groups * half)

    def hidden_half_back(total):
        half = total.shape[1] // groups
        blocks = total.reshape(replicas, halves * rows_here, groups, half)
        blocks = jnp.swapaxes(blocks, 1, 2).astype(jnp.bfloat16)
        summed = lax.psum_scatter(
            blocks.reshape(replicas * groups, halves * rows_here, half),
            ("dp", "tensor"),
            scatter_dimension=0,
            tiled=True,
        )[0].reshape(halves, rows_here, half)
        mine = jnp.take(summed, frame_index, axis=0).astype(jnp.float32)
        sent = jnp.take(summed, 1 - frame_index, axis=0)
        received = lax.ppermute(sent, "frame", [(0, 1), (1, 0)]).astype(jnp.float32)
        return jnp.swapaxes(order_by_half(mine, received), 0, 1).reshape(rows_here, halves * half)

    with jax.named_scope("weights"):
        joint_weight, mixer_weight = (
            lax.all_gather(w, ("dp", "frame"), axis=0, tiled=True)
            for w in (qkv_weight, out_weight)
        )
        upward_weight = hidden_half(up_weight)
        downward_weight = hidden_half(down_weight)

    residual = tokens[:, 0].astype(jnp.float32)
    upstream = out_grad[:, 0].astype(jnp.float32)
    with jax.named_scope("group_inputs"):
        group_tokens = lax.all_gather(tokens[:, 0], "tensor", axis=1, tiled=True)
        group_upstream = None
    def gather_halves(values):
        if halves != 2:
            return lax.all_gather(values, "frame", axis=1, tiled=True)
        other = lax.ppermute(values, "frame", [(0, 1), (1, 0)])
        return jnp.concatenate([values, other], axis=1)

    def scatter_halves(values):
        if halves != 2:
            return lax.psum_scatter(
                values.astype(jnp.bfloat16), "frame", scatter_dimension=1, tiled=True
            ).astype(jnp.float32)
        count = values.shape[1] // 2
        mine = values[:, :count]
        other = lax.ppermute(values[:, count:].astype(jnp.bfloat16), "frame", [(0, 1), (1, 0)])
        return mine.astype(jnp.bfloat16).astype(jnp.float32) + other.astype(jnp.float32)

    def clip_pass(residual, upstream, modulation, group_tokens, group_upstream, group_mod):
        clips = residual.shape[0]
        patches = residual.shape[1]
        shift1, scale1, gate1 = modulation[:, 0], modulation[:, 1], modulation[:, 2]
        shift2, scale2, gate2 = modulation[:, 3], modulation[:, 4], modulation[:, 5]
        def gather_tokens(values):
            return lax.all_gather(values, "tensor", axis=1, tiled=True)

        def scatter_tokens(values):
            parts = values.astype(jnp.bfloat16).reshape(
                values.shape[0], groups, -1, values.shape[-1]
            )
            received = lax.all_to_all(parts, "tensor", 1, 1, tiled=True)
            return jnp.sum(received.astype(jnp.float32), axis=1)

        with jax.named_scope("forward"):
            normed_one, inverse_one = normalize(residual)
            group_normed, _ = normalize(
                group_tokens.astype(jnp.float32).reshape(clips, groups, patches, model_width)
            )
            flat_one = (
                (group_normed * (1.0 + group_mod[:, 1]) + group_mod[:, 0])
                .astype(jnp.bfloat16)
                .reshape(clips, groups * patches, model_width)
            )
            token_count = flat_one.shape[1]
            projected = jnp.einsum(
                "crd,dkh->crkh", flat_one, joint_weight, preferred_element_type=jnp.float32
            ).astype(jnp.bfloat16)
            queries = projected[:, :, 0]
            keys_all = gather_halves(projected[:, :, 1])
            values_all = gather_halves(projected[:, :, 2])
            attended, log_totals = attention_forward(queries[0], keys_all[0], values_all[0])
            attended = attended[None]
            partial_one = jnp.einsum(
                "crh,oh->cro", attended, mixer_weight, preferred_element_type=jnp.float32
            )
            branch_one = scatter_tokens(partial_one)
            middle = residual + gate1 * branch_one
            normed_two, inverse_two = normalize(middle)
            entering_two = (normed_two * (1.0 + scale2) + shift2).astype(jnp.bfloat16)
            flat_two = gather_halves(entering_two)
            up_values = jnp.einsum(
                "crd,df->crf", flat_two, upward_weight, preferred_element_type=jnp.float32
            )
            hidden = gelu_tanh(up_values).astype(jnp.bfloat16)
            partial_two = jnp.einsum(
                "crf,of->cro", hidden, downward_weight, preferred_element_type=jnp.float32
            )
            branch_two = scatter_halves(partial_two)
            output = (middle + gate2 * branch_two).astype(jnp.bfloat16)

        with jax.named_scope("backward_ffn"):
            grad_gate_two = jnp.sum(upstream * branch_two, axis=1)
            grad_two_all = gather_halves((gate2 * upstream).astype(jnp.bfloat16))
            grad_hidden = jnp.einsum(
                "cro,of->crf", grad_two_all, downward_weight, preferred_element_type=jnp.float32
            )
            down_total = jnp.einsum(
                "cro,crf->of", grad_two_all, hidden, preferred_element_type=jnp.float32
            )
            _, gelu_pullback = jax.vjp(gelu_tanh, up_values)
            grad_up = gelu_pullback(grad_hidden)[0].astype(jnp.bfloat16)
            up_total = jnp.einsum(
                "crd,crf->df", flat_two, grad_up, preferred_element_type=jnp.float32
            )
            partial_back_two = jnp.einsum(
                "crf,df->crd", grad_up, upward_weight, preferred_element_type=jnp.float32
            )
            grad_entering_two = scatter_halves(partial_back_two)
            grad_shift_two = jnp.sum(grad_entering_two, axis=1)
            grad_scale_two = jnp.sum(grad_entering_two * normed_two, axis=1)
            grad_middle = upstream + norm_back(
                grad_entering_two * (1.0 + scale2), normed_two, inverse_two
            )
            grad_gate_one = jnp.sum(grad_middle * branch_one, axis=1)

        with jax.named_scope("backward_attention"):
            grad_branch_one = (gate1 * grad_middle).astype(jnp.bfloat16)
            grad_one_all = gather_tokens(grad_branch_one)
            grad_attended = jnp.einsum(
                "cro,oh->crh", grad_one_all, mixer_weight, preferred_element_type=jnp.float32
            ).astype(jnp.bfloat16)
            mixer_total = jnp.einsum(
                "cro,crh->oh", grad_one_all, attended, preferred_element_type=jnp.float32
            )
            query_grads, key_grads, value_grads = attention_backward(
                queries[0], keys_all[0], values_all[0], grad_attended[0], log_totals
            )
            query_grads = query_grads[None]
            key_grads = key_grads[None]
            value_grads = value_grads[None]
            key_own, value_own = (
                scatter_halves(grads.reshape(clips, -1, local_width))
                for grads in (key_grads, value_grads)
            )
            grad_projected = jnp.stack([query_grads, key_own, value_own], axis=2).astype(
                jnp.bfloat16
            )
            joint_total = jnp.einsum(
                "crd,crkh->dkh", flat_one, grad_projected, preferred_element_type=jnp.float32
            )
            partial_back_one = jnp.einsum(
                "crkh,dkh->crd", grad_projected, joint_weight, preferred_element_type=jnp.float32
            )
            grad_entering_one = scatter_tokens(partial_back_one)
            grad_shift_one = jnp.sum(grad_entering_one, axis=1)
            grad_scale_one = jnp.sum(grad_entering_one * normed_one, axis=1)
            grad_input = grad_middle + norm_back(
                grad_entering_one * (1.0 + scale1), normed_one, inverse_one
            )


        grad_modulation = jnp.stack(
            [grad_shift_one, grad_scale_one, grad_gate_one, grad_shift_two, grad_scale_two, grad_gate_two],
            axis=1,
        )
        totals = (joint_total, mixer_total, up_total, down_total)
        return output, grad_input.astype(jnp.bfloat16), grad_modulation, totals

    pieces = [
        clip_pass(
            residual[i : i + 1],
            upstream[i : i + 1],
            modulation[i : i + 1],
            group_tokens[i : i + 1],
            None,
            group_mod[i : i + 1],
        )
        for i in range(clips)
    ]
    output = jnp.concatenate([p[0] for p in pieces], axis=0)
    grad_input_low = jnp.concatenate([p[1] for p in pieces], axis=0)
    grad_modulation = jnp.concatenate([p[2] for p in pieces], axis=0)
    joint_total, mixer_total, up_total, down_total = (
        sum(p[3][k] for p in pieces[1:]) + pieces[0][3][k] for k in range(4)
    )
    with jax.named_scope("ada_grad"):
        grad_columns = lax.all_to_all(
            grad_modulation.reshape(clips, 1, 6, model_width), "tensor", 3, 1, tiled=True
        )
        grad_all = lax.all_gather(grad_columns, ("dp", "frame"), axis=0, tiled=True)
        grad_all = grad_all.reshape(replicas * halves, clips, groups, 6, local_width)
        adaptive_total = jnp.einsum(
            "acgd,acgkw->dkw",
            my_condition.astype(jnp.float32),
            grad_all,
            precision=highest,
        )

    with jax.named_scope("weight_grads"):
        joint_sum, mixer_sum = (
            lax.psum_scatter(
                total.astype(jnp.bfloat16), ("dp", "frame"), scatter_dimension=0, tiled=True
            ).astype(jnp.float32)
            for total in (joint_total, mixer_total)
        )
        summed = (joint_sum, mixer_sum, hidden_half_back(up_total), hidden_half_back(down_total))
    result = output[:, None]
    input_grad = grad_input_low[:, None]
    return (result, input_grad, summed[0], summed[1], summed[2], summed[3], adaptive_total)


def solution(mesh):
    return jax.shard_map(
        on_device,
        mesh=mesh,
        in_specs=(
            P("dp", ("frame", "tensor"), None, None),
            P("dp", ("frame", "tensor"), None, None),
            P("dp", "frame"),
            P(("dp", "frame"), None, "tensor"),
            P(("dp", "frame"), "tensor"),
            P(("dp", "frame"), "tensor"),
            P(("dp", "frame"), "tensor"),
            P(("dp", "frame"), None, "tensor"),
        ),
        out_specs=(
            P("dp", ("frame", "tensor"), None, None),
            P("dp", ("frame", "tensor"), None, None),
            P(("dp", "frame"), None, "tensor"),
            P(("dp", "frame"), "tensor"),
            P(("dp", "frame"), "tensor"),
            P(("dp", "frame"), "tensor"),
            P(("dp", "frame"), None, "tensor"),
        ),
        check_vma=False,
    )
```

```python
import functools
import math

import jax
import jax.numpy as jnp
from jax import lax
from jax.experimental import pallas as pl
from jax.experimental.pallas import tpu as pltpu
from jax.sharding import PartitionSpec as P

HEAD_DIM = 64


epsilon = 1e-06
highest = lax.Precision.HIGHEST


def normalize(values):
    center = values - jnp.mean(values, axis=-1, keepdims=True)
    spread = jnp.mean(center * center, axis=-1, keepdims=True)
    inverse = lax.rsqrt(spread + epsilon)
    return (center * inverse, inverse)


def norm_back(upstream, normed, inverse):
    upstream_mean = jnp.mean(upstream, axis=-1, keepdims=True)
    product_mean = jnp.mean(upstream * normed, axis=-1, keepdims=True)
    return inverse * (upstream - upstream_mean - normed * product_mean)


def level_embedding(levels, model_width):
    halfway = model_width // 2
    frequency = jnp.exp(-math.log(10000.0) * jnp.arange(halfway, dtype=jnp.float32) / halfway)
    angles = levels.astype(jnp.float32)[..., None] * frequency
    return jnp.concatenate([jnp.cos(angles), jnp.sin(angles)], axis=-1)


def _nt(a, b):
    return lax.dot_general(a, b, (((1,), (1,)), ((), ())), preferred_element_type=jnp.float32)


def _tn(a, b):
    return lax.dot_general(a, b, (((0,), (0,)), ((), ())), preferred_element_type=jnp.float32)


def _forward_kernel(heads, scaling, q_ref, k_ref, v_ref, o_ref, lse_ref):
    for h in range(heads):
        cols = slice(h * HEAD_DIM, (h + 1) * HEAD_DIM)
        scores = _nt(q_ref[:, cols], k_ref[:, cols]) * scaling
        largest = jnp.max(scores, axis=1, keepdims=True)
        raised = jnp.exp(scores - largest)
        total = jnp.sum(raised, axis=1, keepdims=True)
        probs_low = (raised / total).astype(jnp.bfloat16)
        out = jnp.dot(probs_low, v_ref[:, cols], preferred_element_type=jnp.float32)
        o_ref[:, cols] = out.astype(o_ref.dtype)
        lse_ref[:, h : h + 1] = largest + jnp.log(total)


def _backward_kernel(heads, scaling, q_ref, k_ref, v_ref, g_ref, lse_ref, dq_ref, dk_ref, dv_ref):
    @pl.when(pl.program_id(0) == 0)
    def _():
        dk_ref[...] = jnp.zeros_like(dk_ref)
        dv_ref[...] = jnp.zeros_like(dv_ref)

    for h in range(heads):
        cols = slice(h * HEAD_DIM, (h + 1) * HEAD_DIM)
        q = q_ref[:, cols]
        g = g_ref[:, cols]
        scores = _nt(q, k_ref[:, cols]) * scaling
        probs = jnp.exp(scores - lse_ref[:, h : h + 1])
        grad_probs = _nt(g, v_ref[:, cols])
        dv_ref[:, cols] += _tn(probs.astype(jnp.bfloat16), g)
        row_terms = jnp.sum(probs * grad_probs, axis=1, keepdims=True)
        grad_scores = (probs * (grad_probs - row_terms)).astype(jnp.bfloat16)
        dq_ref[:, cols] = jnp.dot(grad_scores, k_ref[:, cols], preferred_element_type=jnp.float32) * scaling
        dk_ref[:, cols] += _tn(grad_scores, q) * scaling


def attention_forward(queries, keys, values, block_rows=256):
    rows, width = queries.shape
    length = keys.shape[0]
    heads = width // HEAD_DIM
    block_rows = min(block_rows, rows)
    flops = 4 * rows * length * width
    return pl.pallas_call(
        functools.partial(_forward_kernel, heads, HEAD_DIM ** (-0.5)),
        out_shape=(
            jax.ShapeDtypeStruct((rows, width), jnp.bfloat16),
            jax.ShapeDtypeStruct((rows, heads), jnp.float32),
        ),
        grid=(rows // block_rows,),
        in_specs=[
            pl.BlockSpec((block_rows, width), lambda i: (i, 0)),
            pl.BlockSpec((length, width), lambda i: (0, 0)),
            pl.BlockSpec((length, width), lambda i: (0, 0)),
        ],
        out_specs=[
            pl.BlockSpec((block_rows, width), lambda i: (i, 0)),
            pl.BlockSpec((block_rows, heads), lambda i: (i, 0)),
        ],
        compiler_params=pltpu.CompilerParams(
            dimension_semantics=("arbitrary",), vmem_limit_bytes=56 * 1024 * 1024
        ),
        cost_estimate=pl.CostEstimate(
            flops=flops,
            transcendentals=rows * length * heads,
            bytes_accessed=2 * (2 * rows * width + 2 * length * width),
        ),
    )(queries, keys, values)


def attention_backward(queries, keys, values, grad_out, lse, block_rows=256):
    rows, width = queries.shape
    length = keys.shape[0]
    heads = width // HEAD_DIM
    block_rows = min(block_rows, rows)
    flops = 10 * rows * length * width
    return pl.pallas_call(
        functools.partial(_backward_kernel, heads, HEAD_DIM ** (-0.5)),
        out_shape=(
            jax.ShapeDtypeStruct((rows, width), jnp.float32),
            jax.ShapeDtypeStruct((length, width), jnp.float32),
            jax.ShapeDtypeStruct((length, width), jnp.float32),
        ),
        grid=(rows // block_rows,),
        in_specs=[
            pl.BlockSpec((block_rows, width), lambda i: (i, 0)),
            pl.BlockSpec((length, width), lambda i: (0, 0)),
            pl.BlockSpec((length, width), lambda i: (0, 0)),
            pl.BlockSpec((block_rows, width), lambda i: (i, 0)),
            pl.BlockSpec((block_rows, heads), lambda i: (i, 0)),
        ],
        out_specs=[
            pl.BlockSpec((block_rows, width), lambda i: (i, 0)),
            pl.BlockSpec((length, width), lambda i: (0, 0)),
            pl.BlockSpec((length, width), lambda i: (0, 0)),
        ],
        compiler_params=pltpu.CompilerParams(
            dimension_semantics=("arbitrary",), vmem_limit_bytes=56 * 1024 * 1024
        ),
        cost_estimate=pl.CostEstimate(
            flops=flops,
            transcendentals=rows * length * heads,
            bytes_accessed=2 * (3 * rows * width + 2 * length * width) + 4 * (rows + 2 * length) * width,
        ),
    )(queries, keys, values, grad_out, lse)


def gelu_tanh(values):
    return jax.nn.gelu(values, approximate=True)


def on_device(
    tokens, out_grad, noise_index, qkv_weight, out_weight, up_weight, down_weight, ada_weight
):
    clips = tokens.shape[0]
    patches = tokens.shape[2]
    model_width = tokens.shape[-1]
    local_width = qkv_weight.shape[2]
    rows_here = qkv_weight.shape[0]
    heads_here = local_width // HEAD_DIM
    scaling = HEAD_DIM ** (-0.5)
    groups = lax.axis_size("tensor")
    halves = lax.axis_size("frame")
    replicas = lax.axis_size("dp")

    with jax.named_scope("modulation"):
        levels_all = lax.all_gather(noise_index, ("dp", "frame"), axis=0, tiled=True)
        levels_all = levels_all.reshape(replicas * halves, clips, groups)
        condition_all = jax.nn.silu(level_embedding(levels_all, model_width)).astype(jnp.bfloat16)
        row_block = lax.axis_index("dp") * halves + lax.axis_index("frame")
        my_condition = lax.dynamic_slice_in_dim(
            condition_all, row_block * rows_here, rows_here, axis=3
        )
        partial_mod = jnp.einsum(
            "acgd,dkw->acgkw", my_condition, ada_weight, preferred_element_type=jnp.float32
        )
        summed_mod = jnp.sum(
            lax.all_to_all(partial_mod, ("dp", "frame"), 0, 0, tiled=True), axis=0
        )
        group_mod = lax.all_gather(summed_mod, "tensor", axis=3, tiled=True)
        group_mod = jnp.swapaxes(group_mod, 1, 2)[:, :, :, None, :]
        group_index = lax.axis_index("tensor")
        modulation = lax.dynamic_index_in_dim(group_mod, group_index, axis=2, keepdims=False)

    frame_index = lax.axis_index("frame")

    def order_by_half(mine, other):
        both = jnp.stack([mine, other])
        return jnp.where(frame_index == 0, both, both[::-1])

    def hidden_half(weights):
        half = weights[0].shape[1] // halves
        pieces = []
        for weight in weights:
            blocks = weight.reshape(rows_here, halves, half)
            mine = jnp.take(blocks, frame_index, axis=1)
            sent = jnp.take(blocks, 1 - frame_index, axis=1)
            received = lax.ppermute(sent, "frame", [(0, 1), (1, 0)])
            pieces.append(order_by_half(mine, received).reshape(halves * rows_here, half))
        joined = jnp.concatenate(pieces, axis=1)
        gathered = lax.all_gather(joined, ("dp", "tensor"), axis=0, tiled=True)
        gathered = gathered.reshape(replicas, groups, halves * rows_here, len(weights), half)
        return tuple(
            jnp.swapaxes(gathered[:, :, :, k], 1, 2).reshape(model_width, groups * half)
            for k in range(len(weights))
        )

    def hidden_half_back(totals):
        half = totals[0].shape[1] // groups
        blocks = jnp.concatenate(
            [
                jnp.swapaxes(total.reshape(replicas, halves * rows_here, groups, half), 1, 2)
                for total in totals
            ],
            axis=3,
        ).astype(jnp.bfloat16)
        summed = lax.psum_scatter(
            blocks.reshape(replicas * groups, halves * rows_here, len(totals) * half),
            ("dp", "tensor"),
            scatter_dimension=0,
            tiled=True,
        )[0].reshape(halves, rows_here, len(totals) * half)
        mine = jnp.take(summed, frame_index, axis=0).astype(jnp.float32)
        sent = jnp.take(summed, 1 - frame_index, axis=0)
        received = lax.ppermute(sent, "frame", [(0, 1), (1, 0)]).astype(jnp.float32)
        ordered = jnp.swapaxes(order_by_half(mine, received), 0, 1)
        ordered = ordered.reshape(rows_here, halves, len(totals), half)
        return tuple(
            ordered[:, :, k].reshape(rows_here, halves * half) for k in range(len(totals))
        )

    def line_gather(values):
        if groups == 1:
            return values[:, None]
        rightward = [(i, i + 1) for i in range(groups - 1)]
        leftward = [(i + 1, i) for i in range(groups - 1)]
        right, left = values, values
        before, after = [], []
        for _ in range(groups - 1):
            right = lax.ppermute(right, "tensor", rightward)
            left = lax.ppermute(left, "tensor", leftward)
            before.insert(0, right)
            after.append(left)
        stacked = jnp.stack(before + [values] + after, axis=1)
        start = groups - 1 - lax.axis_index("tensor")
        return lax.dynamic_slice_in_dim(stacked, start, groups, axis=1)

    with jax.named_scope("weights"):
        attention_shards = jnp.concatenate(
            [qkv_weight.reshape(rows_here, 3 * local_width), out_weight], axis=1
        )
        attention_weights = lax.all_gather(attention_shards, ("dp", "frame"), axis=0, tiled=True)
        joint_weight = attention_weights[:, : 3 * local_width].reshape(model_width, 3, local_width)
        mixer_weight = attention_weights[:, 3 * local_width :]
        upward_weight, downward_weight = hidden_half((up_weight, down_weight))

    residual = tokens[:, 0].astype(jnp.float32)
    upstream = out_grad[:, 0].astype(jnp.float32)
    with jax.named_scope("group_inputs"):
        group_tokens = line_gather(tokens[:, 0]).reshape(clips, groups * patches, model_width)
        group_upstream = None
    def gather_halves(values):
        if halves != 2:
            return lax.all_gather(values, "frame", axis=1, tiled=True)
        other = lax.ppermute(values, "frame", [(0, 1), (1, 0)])
        return jnp.concatenate([values, other], axis=1)

    def scatter_halves(values):
        if halves != 2:
            return lax.psum_scatter(
                values.astype(jnp.bfloat16), "frame", scatter_dimension=1, tiled=True
            ).astype(jnp.float32)
        count = values.shape[1] // 2
        mine = values[:, :count]
        other = lax.ppermute(values[:, count:].astype(jnp.bfloat16), "frame", [(0, 1), (1, 0)])
        return mine.astype(jnp.bfloat16).astype(jnp.float32) + other.astype(jnp.float32)

    def clip_pass(residual, upstream, modulation, group_tokens, group_upstream, group_mod):
        clips = residual.shape[0]
        patches = residual.shape[1]
        shift1, scale1, gate1 = modulation[:, 0], modulation[:, 1], modulation[:, 2]
        shift2, scale2, gate2 = modulation[:, 3], modulation[:, 4], modulation[:, 5]
        def gather_tokens(values):
            return lax.all_gather(values, "tensor", axis=1, tiled=True)

        def scatter_tokens(values):
            parts = values.astype(jnp.bfloat16).reshape(
                values.shape[0], groups, -1, values.shape[-1]
            )
            received = lax.all_to_all(parts, "tensor", 1, 1, tiled=True)
            return jnp.sum(received.astype(jnp.float32), axis=1)

        with jax.named_scope("forward"):
            normed_one, inverse_one = normalize(residual)
            group_normed, _ = normalize(
                group_tokens.astype(jnp.float32).reshape(clips, groups, patches, model_width)
            )
            flat_one = (
                (group_normed * (1.0 + group_mod[:, 1]) + group_mod[:, 0])
                .astype(jnp.bfloat16)
                .reshape(clips, groups * patches, model_width)
            )
            token_count = flat_one.shape[1]
            projected = jnp.einsum(
                "crd,dkh->crkh", flat_one, joint_weight, preferred_element_type=jnp.float32
            ).astype(jnp.bfloat16)
            queries = projected[:, :, 0]
            keys_all = gather_halves(projected[:, :, 1])
            values_all = gather_halves(projected[:, :, 2])
            attended, log_totals = attention_forward(queries[0], keys_all[0], values_all[0])
            attended = attended[None]
            partial_one = jnp.einsum(
                "crh,oh->cro", attended, mixer_weight, preferred_element_type=jnp.float32
            )
            branch_one = scatter_tokens(partial_one)
            middle = residual + gate1 * branch_one
            normed_two, inverse_two = normalize(middle)
            entering_two = (normed_two * (1.0 + scale2) + shift2).astype(jnp.bfloat16)
            flat_two = gather_halves(entering_two)
            up_values = jnp.einsum(
                "crd,df->crf", flat_two, upward_weight, preferred_element_type=jnp.float32
            )
            hidden = gelu_tanh(up_values).astype(jnp.bfloat16)
            partial_two = jnp.einsum(
                "crf,of->cro", hidden, downward_weight, preferred_element_type=jnp.float32
            )
            branch_two = scatter_halves(partial_two)
            output = (middle + gate2 * branch_two).astype(jnp.bfloat16)

        with jax.named_scope("backward_ffn"):
            grad_gate_two = jnp.sum(upstream * branch_two, axis=1)
            grad_two_all = gather_halves((gate2 * upstream).astype(jnp.bfloat16))
            grad_hidden = jnp.einsum(
                "cro,of->crf", grad_two_all, downward_weight, preferred_element_type=jnp.float32
            )
            down_total = jnp.einsum(
                "cro,crf->of", grad_two_all, hidden, preferred_element_type=jnp.float32
            )
            _, gelu_pullback = jax.vjp(gelu_tanh, up_values)
            grad_up = gelu_pullback(grad_hidden)[0].astype(jnp.bfloat16)
            up_total = jnp.einsum(
                "crd,crf->df", flat_two, grad_up, preferred_element_type=jnp.float32
            )
            partial_back_two = jnp.einsum(
                "crf,df->crd", grad_up, upward_weight, preferred_element_type=jnp.float32
            )
            grad_entering_two = scatter_halves(partial_back_two)
            grad_shift_two = jnp.sum(grad_entering_two, axis=1)
            grad_scale_two = jnp.sum(grad_entering_two * normed_two, axis=1)
            grad_middle = upstream + norm_back(
                grad_entering_two * (1.0 + scale2), normed_two, inverse_two
            )
            grad_gate_one = jnp.sum(grad_middle * branch_one, axis=1)

        with jax.named_scope("backward_attention"):
            grad_branch_one = (gate1 * grad_middle).astype(jnp.bfloat16)
            grad_one_all = gather_tokens(grad_branch_one)
            grad_attended = jnp.einsum(
                "cro,oh->crh", grad_one_all, mixer_weight, preferred_element_type=jnp.float32
            ).astype(jnp.bfloat16)
            mixer_total = jnp.einsum(
                "cro,crh->oh", grad_one_all, attended, preferred_element_type=jnp.float32
            )
            query_grads, key_grads, value_grads = attention_backward(
                queries[0], keys_all[0], values_all[0], grad_attended[0], log_totals
            )
            query_grads = query_grads[None]
            key_grads = key_grads[None]
            value_grads = value_grads[None]
            key_own, value_own = (
                scatter_halves(grads.reshape(clips, -1, local_width))
                for grads in (key_grads, value_grads)
            )
            grad_projected = jnp.stack([query_grads, key_own, value_own], axis=2).astype(
                jnp.bfloat16
            )
            joint_total = jnp.einsum(
                "crd,crkh->dkh", flat_one, grad_projected, preferred_element_type=jnp.float32
            )
            partial_back_one = jnp.einsum(
                "crkh,dkh->crd", grad_projected, joint_weight, preferred_element_type=jnp.float32
            )
            grad_entering_one = scatter_tokens(partial_back_one)
            grad_shift_one = jnp.sum(grad_entering_one, axis=1)
            grad_scale_one = jnp.sum(grad_entering_one * normed_one, axis=1)
            grad_input = grad_middle + norm_back(
                grad_entering_one * (1.0 + scale1), normed_one, inverse_one
            )


        grad_modulation = jnp.stack(
            [grad_shift_one, grad_scale_one, grad_gate_one, grad_shift_two, grad_scale_two, grad_gate_two],
            axis=1,
        )
        totals = (joint_total, mixer_total, up_total, down_total)
        return output, grad_input.astype(jnp.bfloat16), grad_modulation, totals

    pieces = [
        clip_pass(
            residual[i : i + 1],
            upstream[i : i + 1],
            modulation[i : i + 1],
            group_tokens[i : i + 1],
            None,
            group_mod[i : i + 1],
        )
        for i in range(clips)
    ]
    output = jnp.concatenate([p[0] for p in pieces], axis=0)
    grad_input_low = jnp.concatenate([p[1] for p in pieces], axis=0)
    grad_modulation = jnp.concatenate([p[2] for p in pieces], axis=0)
    joint_total, mixer_total, up_total, down_total = (
        sum(p[3][k] for p in pieces[1:]) + pieces[0][3][k] for k in range(4)
    )
    with jax.named_scope("ada_grad"):
        grad_columns = lax.all_to_all(
            grad_modulation.reshape(clips, 1, 6, model_width), "tensor", 3, 1, tiled=True
        )
        grad_all = lax.all_gather(grad_columns, ("dp", "frame"), axis=0, tiled=True)
        grad_all = grad_all.reshape(replicas * halves, clips, groups, 6, local_width)
        adaptive_total = jnp.einsum(
            "acgd,acgkw->dkw",
            my_condition.astype(jnp.float32),
            grad_all,
            precision=highest,
        )

    with jax.named_scope("weight_grads"):
        attention_totals = jnp.concatenate(
            [joint_total.reshape(model_width, 3 * local_width), mixer_total], axis=1
        )
        attention_sums = lax.psum_scatter(
            attention_totals.astype(jnp.bfloat16), ("dp", "frame"), scatter_dimension=0, tiled=True
        ).astype(jnp.float32)
        joint_sum = attention_sums[:, : 3 * local_width].reshape(rows_here, 3, local_width)
        mixer_sum = attention_sums[:, 3 * local_width :]
        up_sum, down_sum = hidden_half_back((up_total, down_total))
        summed = (joint_sum, mixer_sum, up_sum, down_sum)
    result = output[:, None]
    input_grad = grad_input_low[:, None]
    return (result, input_grad, summed[0], summed[1], summed[2], summed[3], adaptive_total)


def solution(mesh):
    return jax.shard_map(
        on_device,
        mesh=mesh,
        in_specs=(
            P("dp", ("frame", "tensor"), None, None),
            P("dp", ("frame", "tensor"), None, None),
            P("dp", "frame"),
            P(("dp", "frame"), None, "tensor"),
            P(("dp", "frame"), "tensor"),
            P(("dp", "frame"), "tensor"),
            P(("dp", "frame"), "tensor"),
            P(("dp", "frame"), None, "tensor"),
        ),
        out_specs=(
            P("dp", ("frame", "tensor"), None, None),
            P("dp", ("frame", "tensor"), None, None),
            P(("dp", "frame"), None, "tensor"),
            P(("dp", "frame"), "tensor"),
            P(("dp", "frame"), "tensor"),
            P(("dp", "frame"), "tensor"),
            P(("dp", "frame"), None, "tensor"),
        ),
        check_vma=False,
    )
```

```python
import functools
import math

import jax
import jax.numpy as jnp
from jax import lax
from jax.experimental import pallas as pl
from jax.experimental.pallas import tpu as pltpu
from jax.sharding import PartitionSpec as P

HEAD_DIM = 64


epsilon = 1e-06
highest = lax.Precision.HIGHEST


def normalize(values):
    center = values - jnp.mean(values, axis=-1, keepdims=True)
    spread = jnp.mean(center * center, axis=-1, keepdims=True)
    inverse = lax.rsqrt(spread + epsilon)
    return (center * inverse, inverse)


def norm_back(upstream, normed, inverse):
    upstream_mean = jnp.mean(upstream, axis=-1, keepdims=True)
    product_mean = jnp.mean(upstream * normed, axis=-1, keepdims=True)
    return inverse * (upstream - upstream_mean - normed * product_mean)


def level_embedding(levels, model_width):
    halfway = model_width // 2
    frequency = jnp.exp(-math.log(10000.0) * jnp.arange(halfway, dtype=jnp.float32) / halfway)
    angles = levels.astype(jnp.float32)[..., None] * frequency
    return jnp.concatenate([jnp.cos(angles), jnp.sin(angles)], axis=-1)


def _nt(a, b):
    return lax.dot_general(a, b, (((1,), (1,)), ((), ())), preferred_element_type=jnp.float32)


def _tn(a, b):
    return lax.dot_general(a, b, (((0,), (0,)), ((), ())), preferred_element_type=jnp.float32)


def _forward_kernel(heads, scaling, q_ref, k_ref, v_ref, o_ref, lse_ref):
    for h in range(heads):
        cols = slice(h * HEAD_DIM, (h + 1) * HEAD_DIM)
        scores = _nt(q_ref[:, cols], k_ref[:, cols]) * scaling
        largest = jnp.max(scores, axis=1, keepdims=True)
        raised = jnp.exp(scores - largest)
        total = jnp.sum(raised, axis=1, keepdims=True)
        probs_low = (raised / total).astype(jnp.bfloat16)
        out = jnp.dot(probs_low, v_ref[:, cols], preferred_element_type=jnp.float32)
        o_ref[:, cols] = out.astype(o_ref.dtype)
        lse_ref[:, h : h + 1] = largest + jnp.log(total)


def _backward_kernel(heads, scaling, q_ref, k_ref, v_ref, g_ref, lse_ref, dq_ref, dk_ref, dv_ref):
    @pl.when(pl.program_id(0) == 0)
    def _():
        dk_ref[...] = jnp.zeros_like(dk_ref)
        dv_ref[...] = jnp.zeros_like(dv_ref)

    for h in range(heads):
        cols = slice(h * HEAD_DIM, (h + 1) * HEAD_DIM)
        q = q_ref[:, cols]
        g = g_ref[:, cols]
        scores = _nt(q, k_ref[:, cols]) * scaling
        probs = jnp.exp(scores - lse_ref[:, h : h + 1])
        grad_probs = _nt(g, v_ref[:, cols])
        dv_ref[:, cols] += _tn(probs.astype(jnp.bfloat16), g)
        row_terms = jnp.sum(probs * grad_probs, axis=1, keepdims=True)
        grad_scores = (probs * (grad_probs - row_terms)).astype(jnp.bfloat16)
        dq_ref[:, cols] = jnp.dot(grad_scores, k_ref[:, cols], preferred_element_type=jnp.float32) * scaling
        dk_ref[:, cols] += _tn(grad_scores, q) * scaling


def attention_forward(queries, keys, values, block_rows=256):
    rows, width = queries.shape
    length = keys.shape[0]
    heads = width // HEAD_DIM
    block_rows = min(block_rows, rows)
    flops = 4 * rows * length * width
    return pl.pallas_call(
        functools.partial(_forward_kernel, heads, HEAD_DIM ** (-0.5)),
        out_shape=(
            jax.ShapeDtypeStruct((rows, width), jnp.bfloat16),
            jax.ShapeDtypeStruct((rows, heads), jnp.float32),
        ),
        grid=(rows // block_rows,),
        in_specs=[
            pl.BlockSpec((block_rows, width), lambda i: (i, 0)),
            pl.BlockSpec((length, width), lambda i: (0, 0)),
            pl.BlockSpec((length, width), lambda i: (0, 0)),
        ],
        out_specs=[
            pl.BlockSpec((block_rows, width), lambda i: (i, 0)),
            pl.BlockSpec((block_rows, heads), lambda i: (i, 0)),
        ],
        compiler_params=pltpu.CompilerParams(
            dimension_semantics=("arbitrary",), vmem_limit_bytes=56 * 1024 * 1024
        ),
        cost_estimate=pl.CostEstimate(
            flops=flops,
            transcendentals=rows * length * heads,
            bytes_accessed=2 * (2 * rows * width + 2 * length * width),
        ),
    )(queries, keys, values)


def attention_backward(queries, keys, values, grad_out, lse, block_rows=256):
    rows, width = queries.shape
    length = keys.shape[0]
    heads = width // HEAD_DIM
    block_rows = min(block_rows, rows)
    flops = 10 * rows * length * width
    return pl.pallas_call(
        functools.partial(_backward_kernel, heads, HEAD_DIM ** (-0.5)),
        out_shape=(
            jax.ShapeDtypeStruct((rows, width), jnp.float32),
            jax.ShapeDtypeStruct((length, width), jnp.float32),
            jax.ShapeDtypeStruct((length, width), jnp.float32),
        ),
        grid=(rows // block_rows,),
        in_specs=[
            pl.BlockSpec((block_rows, width), lambda i: (i, 0)),
            pl.BlockSpec((length, width), lambda i: (0, 0)),
            pl.BlockSpec((length, width), lambda i: (0, 0)),
            pl.BlockSpec((block_rows, width), lambda i: (i, 0)),
            pl.BlockSpec((block_rows, heads), lambda i: (i, 0)),
        ],
        out_specs=[
            pl.BlockSpec((block_rows, width), lambda i: (i, 0)),
            pl.BlockSpec((length, width), lambda i: (0, 0)),
            pl.BlockSpec((length, width), lambda i: (0, 0)),
        ],
        compiler_params=pltpu.CompilerParams(
            dimension_semantics=("arbitrary",), vmem_limit_bytes=56 * 1024 * 1024
        ),
        cost_estimate=pl.CostEstimate(
            flops=flops,
            transcendentals=rows * length * heads,
            bytes_accessed=2 * (3 * rows * width + 2 * length * width) + 4 * (rows + 2 * length) * width,
        ),
    )(queries, keys, values, grad_out, lse)


def gelu_tanh(values):
    return jax.nn.gelu(values, approximate=True)


def on_device(
    tokens, out_grad, noise_index, qkv_weight, out_weight, up_weight, down_weight, ada_weight
):
    clips = tokens.shape[0]
    patches = tokens.shape[2]
    model_width = tokens.shape[-1]
    local_width = qkv_weight.shape[2]
    rows_here = qkv_weight.shape[0]
    heads_here = local_width // HEAD_DIM
    scaling = HEAD_DIM ** (-0.5)
    groups = lax.axis_size("tensor")
    halves = lax.axis_size("frame")
    replicas = lax.axis_size("dp")

    with jax.named_scope("modulation"):
        levels_all = lax.all_gather(noise_index, ("dp", "frame"), axis=0, tiled=True)
        levels_all = levels_all.reshape(replicas * halves, clips, groups)
        condition_all = jax.nn.silu(level_embedding(levels_all, model_width)).astype(jnp.bfloat16)
        row_block = lax.axis_index("dp") * halves + lax.axis_index("frame")
        my_condition = lax.dynamic_slice_in_dim(
            condition_all, row_block * rows_here, rows_here, axis=3
        )
        partial_mod = jnp.einsum(
            "acgd,dkw->acgkw", my_condition, ada_weight, preferred_element_type=jnp.float32
        )
        summed_mod = jnp.sum(
            lax.all_to_all(partial_mod, ("dp", "frame"), 0, 0, tiled=True), axis=0
        )
        group_mod = lax.all_gather(summed_mod, "tensor", axis=3, tiled=True)
        group_mod = jnp.swapaxes(group_mod, 1, 2)[:, :, :, None, :]
        group_index = lax.axis_index("tensor")
        modulation = lax.dynamic_index_in_dim(group_mod, group_index, axis=2, keepdims=False)

    frame_index = lax.axis_index("frame")

    def order_by_half(mine, other):
        both = jnp.stack([mine, other])
        return jnp.where(frame_index == 0, both, both[::-1])

    def hidden_half(weights):
        half = weights[0].shape[1] // halves
        pieces = []
        for weight in weights:
            blocks = weight.reshape(rows_here, halves, half)
            mine = jnp.take(blocks, frame_index, axis=1)
            sent = jnp.take(blocks, 1 - frame_index, axis=1)
            received = lax.ppermute(sent, "frame", [(0, 1), (1, 0)])
            pieces.append(order_by_half(mine, received).reshape(halves * rows_here, half))
        joined = jnp.concatenate(pieces, axis=1)
        gathered = lax.all_gather(joined, ("dp", "tensor"), axis=0, tiled=True)
        gathered = gathered.reshape(replicas, groups, halves * rows_here, len(weights), half)
        return tuple(
            jnp.swapaxes(gathered[:, :, :, k], 1, 2).reshape(model_width, groups * half)
            for k in range(len(weights))
        )

    def hidden_half_back(totals):
        half = totals[0].shape[1] // groups
        blocks = jnp.concatenate(
            [
                jnp.swapaxes(total.reshape(replicas, halves * rows_here, groups, half), 1, 2)
                for total in totals
            ],
            axis=3,
        ).astype(jnp.bfloat16)
        summed = lax.psum_scatter(
            blocks.reshape(replicas * groups, halves * rows_here, len(totals) * half),
            ("dp", "tensor"),
            scatter_dimension=0,
            tiled=True,
        )[0].reshape(halves, rows_here, len(totals) * half)
        mine = jnp.take(summed, frame_index, axis=0).astype(jnp.float32)
        sent = jnp.take(summed, 1 - frame_index, axis=0)
        received = lax.ppermute(sent, "frame", [(0, 1), (1, 0)]).astype(jnp.float32)
        ordered = jnp.swapaxes(order_by_half(mine, received), 0, 1)
        ordered = ordered.reshape(rows_here, halves, len(totals), half)
        return tuple(
            ordered[:, :, k].reshape(rows_here, halves * half) for k in range(len(totals))
        )

    with jax.named_scope("weights"):
        joint_weight, mixer_weight = (
            lax.all_gather(w, ("dp", "frame"), axis=0, tiled=True)
            for w in (qkv_weight, out_weight)
        )
        upward_weight, downward_weight = hidden_half((up_weight, down_weight))

    residual = tokens[:, 0].astype(jnp.float32)
    upstream = out_grad[:, 0].astype(jnp.float32)
    with jax.named_scope("group_inputs"):
        group_tokens = lax.all_gather(tokens[:, 0], "tensor", axis=1, tiled=True)
        group_upstream = None
    def gather_halves(values):
        if halves != 2:
            return lax.all_gather(values, "frame", axis=1, tiled=True)
        other = lax.ppermute(values, "frame", [(0, 1), (1, 0)])
        return jnp.concatenate([values, other], axis=1)

    def scatter_halves(values):
        if halves != 2:
            return lax.psum_scatter(
                values.astype(jnp.bfloat16), "frame", scatter_dimension=1, tiled=True
            ).astype(jnp.float32)
        count = values.shape[1] // 2
        mine = values[:, :count]
        other = lax.ppermute(values[:, count:].astype(jnp.bfloat16), "frame", [(0, 1), (1, 0)])
        return mine.astype(jnp.bfloat16).astype(jnp.float32) + other.astype(jnp.float32)

    def clip_pass(residual, upstream, modulation, group_tokens, group_upstream, group_mod):
        clips = residual.shape[0]
        patches = residual.shape[1]
        shift1, scale1, gate1 = modulation[:, 0], modulation[:, 1], modulation[:, 2]
        shift2, scale2, gate2 = modulation[:, 3], modulation[:, 4], modulation[:, 5]
        def gather_tokens(values):
            return lax.all_gather(values, "tensor", axis=1, tiled=True)

        def scatter_tokens(values):
            parts = values.astype(jnp.bfloat16).reshape(
                values.shape[0], groups, -1, values.shape[-1]
            )
            received = lax.all_to_all(parts, "tensor", 1, 1, tiled=True)
            return jnp.sum(received.astype(jnp.float32), axis=1)

        with jax.named_scope("forward"):
            normed_one, inverse_one = normalize(residual)
            group_normed, _ = normalize(
                group_tokens.astype(jnp.float32).reshape(clips, groups, patches, model_width)
            )
            flat_one = (
                (group_normed * (1.0 + group_mod[:, 1]) + group_mod[:, 0])
                .astype(jnp.bfloat16)
                .reshape(clips, groups * patches, model_width)
            )
            token_count = flat_one.shape[1]
            projected = jnp.einsum(
                "crd,dkh->crkh", flat_one, joint_weight, preferred_element_type=jnp.float32
            ).astype(jnp.bfloat16)
            queries = projected[:, :, 0]
            keys_all = gather_halves(projected[:, :, 1])
            values_all = gather_halves(projected[:, :, 2])
            attended, log_totals = attention_forward(queries[0], keys_all[0], values_all[0])
            attended = attended[None]
            partial_one = jnp.einsum(
                "crh,oh->cro", attended, mixer_weight, preferred_element_type=jnp.float32
            )
            branch_one = scatter_tokens(partial_one)
            middle = residual + gate1 * branch_one
            normed_two, inverse_two = normalize(middle)
            entering_two = (normed_two * (1.0 + scale2) + shift2).astype(jnp.bfloat16)
            flat_two = gather_halves(entering_two)
            up_values = jnp.einsum(
                "crd,df->crf", flat_two, upward_weight, preferred_element_type=jnp.float32
            )
            hidden = gelu_tanh(up_values).astype(jnp.bfloat16)
            partial_two = jnp.einsum(
                "crf,of->cro", hidden, downward_weight, preferred_element_type=jnp.float32
            )
            branch_two = scatter_halves(partial_two)
            output = (middle + gate2 * branch_two).astype(jnp.bfloat16)

        with jax.named_scope("backward_ffn"):
            grad_gate_two = jnp.sum(upstream * branch_two, axis=1)
            grad_two_all = gather_halves((gate2 * upstream).astype(jnp.bfloat16))
            grad_hidden = jnp.einsum(
                "cro,of->crf", grad_two_all, downward_weight, preferred_element_type=jnp.float32
            )
            down_total = jnp.einsum(
                "cro,crf->of", grad_two_all, hidden, preferred_element_type=jnp.float32
            )
            _, gelu_pullback = jax.vjp(gelu_tanh, up_values)
            grad_up = gelu_pullback(grad_hidden)[0].astype(jnp.bfloat16)
            up_total = jnp.einsum(
                "crd,crf->df", flat_two, grad_up, preferred_element_type=jnp.float32
            )
            partial_back_two = jnp.einsum(
                "crf,df->crd", grad_up, upward_weight, preferred_element_type=jnp.float32
            )
            grad_entering_two = scatter_halves(partial_back_two)
            grad_shift_two = jnp.sum(grad_entering_two, axis=1)
            grad_scale_two = jnp.sum(grad_entering_two * normed_two, axis=1)
            grad_middle = upstream + norm_back(
                grad_entering_two * (1.0 + scale2), normed_two, inverse_two
            )
            grad_gate_one = jnp.sum(grad_middle * branch_one, axis=1)

        with jax.named_scope("backward_attention"):
            grad_branch_one = (gate1 * grad_middle).astype(jnp.bfloat16)
            grad_one_all = gather_tokens(grad_branch_one)
            grad_attended = jnp.einsum(
                "cro,oh->crh", grad_one_all, mixer_weight, preferred_element_type=jnp.float32
            ).astype(jnp.bfloat16)
            mixer_total = jnp.einsum(
                "cro,crh->oh", grad_one_all, attended, preferred_element_type=jnp.float32
            )
            query_grads, key_grads, value_grads = attention_backward(
                queries[0], keys_all[0], values_all[0], grad_attended[0], log_totals
            )
            query_grads = query_grads[None]
            key_grads = key_grads[None]
            value_grads = value_grads[None]
            key_own, value_own = (
                scatter_halves(grads.reshape(clips, -1, local_width))
                for grads in (key_grads, value_grads)
            )
            grad_projected = jnp.stack([query_grads, key_own, value_own], axis=2).astype(
                jnp.bfloat16
            )
            joint_total = jnp.einsum(
                "crd,crkh->dkh", flat_one, grad_projected, preferred_element_type=jnp.float32
            )
            partial_back_one = jnp.einsum(
                "crkh,dkh->crd", grad_projected, joint_weight, preferred_element_type=jnp.float32
            )
            grad_entering_one = scatter_tokens(partial_back_one)
            grad_shift_one = jnp.sum(grad_entering_one, axis=1)
            grad_scale_one = jnp.sum(grad_entering_one * normed_one, axis=1)
            grad_input = grad_middle + norm_back(
                grad_entering_one * (1.0 + scale1), normed_one, inverse_one
            )


        grad_modulation = jnp.stack(
            [grad_shift_one, grad_scale_one, grad_gate_one, grad_shift_two, grad_scale_two, grad_gate_two],
            axis=1,
        )
        totals = (joint_total, mixer_total, up_total, down_total)
        return output, grad_input.astype(jnp.bfloat16), grad_modulation, totals

    pieces = [
        clip_pass(
            residual[i : i + 1],
            upstream[i : i + 1],
            modulation[i : i + 1],
            group_tokens[i : i + 1],
            None,
            group_mod[i : i + 1],
        )
        for i in range(clips)
    ]
    output = jnp.concatenate([p[0] for p in pieces], axis=0)
    grad_input_low = jnp.concatenate([p[1] for p in pieces], axis=0)
    grad_modulation = jnp.concatenate([p[2] for p in pieces], axis=0)
    joint_total, mixer_total, up_total, down_total = (
        sum(p[3][k] for p in pieces[1:]) + pieces[0][3][k] for k in range(4)
    )
    with jax.named_scope("ada_grad"):
        grad_columns = lax.all_to_all(
            grad_modulation.reshape(clips, 1, 6, model_width), "tensor", 3, 1, tiled=True
        )
        grad_all = lax.all_gather(grad_columns, ("dp", "frame"), axis=0, tiled=True)
        grad_all = grad_all.reshape(replicas * halves, clips, groups, 6, local_width)
        adaptive_total = jnp.einsum(
            "acgd,acgkw->dkw",
            my_condition.astype(jnp.float32),
            grad_all,
            precision=highest,
        )

    with jax.named_scope("weight_grads"):
        joint_sum, mixer_sum = (
            lax.psum_scatter(
                total.astype(jnp.bfloat16), ("dp", "frame"), scatter_dimension=0, tiled=True
            ).astype(jnp.float32)
            for total in (joint_total, mixer_total)
        )
        up_sum, down_sum = hidden_half_back((up_total, down_total))
        summed = (joint_sum, mixer_sum, up_sum, down_sum)
    result = output[:, None]
    input_grad = grad_input_low[:, None]
    return (result, input_grad, summed[0], summed[1], summed[2], summed[3], adaptive_total)


def solution(mesh):
    return jax.shard_map(
        on_device,
        mesh=mesh,
        in_specs=(
            P("dp", ("frame", "tensor"), None, None),
            P("dp", ("frame", "tensor"), None, None),
            P("dp", "frame"),
            P(("dp", "frame"), None, "tensor"),
            P(("dp", "frame"), "tensor"),
            P(("dp", "frame"), "tensor"),
            P(("dp", "frame"), "tensor"),
            P(("dp", "frame"), None, "tensor"),
        ),
        out_specs=(
            P("dp", ("frame", "tensor"), None, None),
            P("dp", ("frame", "tensor"), None, None),
            P(("dp", "frame"), None, "tensor"),
            P(("dp", "frame"), "tensor"),
            P(("dp", "frame"), "tensor"),
            P(("dp", "frame"), "tensor"),
            P(("dp", "frame"), None, "tensor"),
        ),
        check_vma=False,
    )
```

```python
import functools
import math

import jax
import jax.numpy as jnp
from jax import lax
from jax.experimental import pallas as pl
from jax.experimental.pallas import tpu as pltpu
from jax.sharding import PartitionSpec as P

HEAD_DIM = 64


epsilon = 1e-06
highest = lax.Precision.HIGHEST


def normalize(values):
    center = values - jnp.mean(values, axis=-1, keepdims=True)
    spread = jnp.mean(center * center, axis=-1, keepdims=True)
    inverse = lax.rsqrt(spread + epsilon)
    return (center * inverse, inverse)


def norm_back(upstream, normed, inverse):
    upstream_mean = jnp.mean(upstream, axis=-1, keepdims=True)
    product_mean = jnp.mean(upstream * normed, axis=-1, keepdims=True)
    return inverse * (upstream - upstream_mean - normed * product_mean)


def level_embedding(levels, model_width):
    halfway = model_width // 2
    frequency = jnp.exp(-math.log(10000.0) * jnp.arange(halfway, dtype=jnp.float32) / halfway)
    angles = levels.astype(jnp.float32)[..., None] * frequency
    return jnp.concatenate([jnp.cos(angles), jnp.sin(angles)], axis=-1)


def _nt(a, b):
    return lax.dot_general(a, b, (((1,), (1,)), ((), ())), preferred_element_type=jnp.float32)


def _tn(a, b):
    return lax.dot_general(a, b, (((0,), (0,)), ((), ())), preferred_element_type=jnp.float32)


def _forward_kernel(heads, scaling, q_ref, k_ref, v_ref, o_ref, lse_ref):
    for h in range(heads):
        cols = slice(h * HEAD_DIM, (h + 1) * HEAD_DIM)
        scores = _nt(q_ref[:, cols], k_ref[:, cols]) * scaling
        largest = jnp.max(scores, axis=1, keepdims=True)
        raised = jnp.exp(scores - largest)
        total = jnp.sum(raised, axis=1, keepdims=True)
        probs_low = (raised / total).astype(jnp.bfloat16)
        out = jnp.dot(probs_low, v_ref[:, cols], preferred_element_type=jnp.float32)
        o_ref[:, cols] = out.astype(o_ref.dtype)
        lse_ref[:, h : h + 1] = largest + jnp.log(total)


def _backward_kernel(heads, scaling, q_ref, k_ref, v_ref, g_ref, lse_ref, dq_ref, dk_ref, dv_ref):
    @pl.when(pl.program_id(0) == 0)
    def _():
        dk_ref[...] = jnp.zeros_like(dk_ref)
        dv_ref[...] = jnp.zeros_like(dv_ref)

    for h in range(heads):
        cols = slice(h * HEAD_DIM, (h + 1) * HEAD_DIM)
        q = q_ref[:, cols]
        g = g_ref[:, cols]
        scores = _nt(q, k_ref[:, cols]) * scaling
        probs = jnp.exp(scores - lse_ref[:, h : h + 1])
        grad_probs = _nt(g, v_ref[:, cols])
        dv_ref[:, cols] += _tn(probs.astype(jnp.bfloat16), g)
        row_terms = jnp.sum(probs * grad_probs, axis=1, keepdims=True)
        grad_scores = (probs * (grad_probs - row_terms)).astype(jnp.bfloat16)
        dq_ref[:, cols] = jnp.dot(grad_scores, k_ref[:, cols], preferred_element_type=jnp.float32) * scaling
        dk_ref[:, cols] += _tn(grad_scores, q) * scaling


def attention_forward(queries, keys, values, block_rows=256):
    rows, width = queries.shape
    length = keys.shape[0]
    heads = width // HEAD_DIM
    block_rows = min(block_rows, rows)
    flops = 4 * rows * length * width
    return pl.pallas_call(
        functools.partial(_forward_kernel, heads, HEAD_DIM ** (-0.5)),
        out_shape=(
            jax.ShapeDtypeStruct((rows, width), jnp.bfloat16),
            jax.ShapeDtypeStruct((rows, heads), jnp.float32),
        ),
        grid=(rows // block_rows,),
        in_specs=[
            pl.BlockSpec((block_rows, width), lambda i: (i, 0)),
            pl.BlockSpec((length, width), lambda i: (0, 0)),
            pl.BlockSpec((length, width), lambda i: (0, 0)),
        ],
        out_specs=[
            pl.BlockSpec((block_rows, width), lambda i: (i, 0)),
            pl.BlockSpec((block_rows, heads), lambda i: (i, 0)),
        ],
        compiler_params=pltpu.CompilerParams(
            dimension_semantics=("arbitrary",), vmem_limit_bytes=56 * 1024 * 1024
        ),
        cost_estimate=pl.CostEstimate(
            flops=flops,
            transcendentals=rows * length * heads,
            bytes_accessed=2 * (2 * rows * width + 2 * length * width),
        ),
    )(queries, keys, values)


def attention_backward(queries, keys, values, grad_out, lse, block_rows=256):
    rows, width = queries.shape
    length = keys.shape[0]
    heads = width // HEAD_DIM
    block_rows = min(block_rows, rows)
    flops = 10 * rows * length * width
    return pl.pallas_call(
        functools.partial(_backward_kernel, heads, HEAD_DIM ** (-0.5)),
        out_shape=(
            jax.ShapeDtypeStruct((rows, width), jnp.float32),
            jax.ShapeDtypeStruct((length, width), jnp.float32),
            jax.ShapeDtypeStruct((length, width), jnp.float32),
        ),
        grid=(rows // block_rows,),
        in_specs=[
            pl.BlockSpec((block_rows, width), lambda i: (i, 0)),
            pl.BlockSpec((length, width), lambda i: (0, 0)),
            pl.BlockSpec((length, width), lambda i: (0, 0)),
            pl.BlockSpec((block_rows, width), lambda i: (i, 0)),
            pl.BlockSpec((block_rows, heads), lambda i: (i, 0)),
        ],
        out_specs=[
            pl.BlockSpec((block_rows, width), lambda i: (i, 0)),
            pl.BlockSpec((length, width), lambda i: (0, 0)),
            pl.BlockSpec((length, width), lambda i: (0, 0)),
        ],
        compiler_params=pltpu.CompilerParams(
            dimension_semantics=("arbitrary",), vmem_limit_bytes=56 * 1024 * 1024
        ),
        cost_estimate=pl.CostEstimate(
            flops=flops,
            transcendentals=rows * length * heads,
            bytes_accessed=2 * (3 * rows * width + 2 * length * width) + 4 * (rows + 2 * length) * width,
        ),
    )(queries, keys, values, grad_out, lse)


def gelu_tanh(values):
    return jax.nn.gelu(values, approximate=True)


def on_device(
    tokens, out_grad, noise_index, qkv_weight, out_weight, up_weight, down_weight, ada_weight
):
    clips = tokens.shape[0]
    patches = tokens.shape[2]
    model_width = tokens.shape[-1]
    local_width = qkv_weight.shape[2]
    rows_here = qkv_weight.shape[0]
    heads_here = local_width // HEAD_DIM
    scaling = HEAD_DIM ** (-0.5)
    groups = lax.axis_size("tensor")
    halves = lax.axis_size("frame")
    replicas = lax.axis_size("dp")

    with jax.named_scope("modulation"):
        levels_all = lax.all_gather(noise_index, ("dp", "frame"), axis=0, tiled=True)
        levels_all = levels_all.reshape(replicas * halves, clips, groups)
        condition_all = jax.nn.silu(level_embedding(levels_all, model_width)).astype(jnp.bfloat16)
        row_block = lax.axis_index("dp") * halves + lax.axis_index("frame")
        my_condition = lax.dynamic_slice_in_dim(
            condition_all, row_block * rows_here, rows_here, axis=3
        )
        partial_mod = jnp.einsum(
            "acgd,dkw->acgkw", my_condition, ada_weight, preferred_element_type=jnp.float32
        )
        summed_mod = jnp.sum(
            lax.all_to_all(partial_mod, ("dp", "frame"), 0, 0, tiled=True), axis=0
        )
        group_mod = lax.all_gather(summed_mod, "tensor", axis=3, tiled=True)
        group_mod = jnp.swapaxes(group_mod, 1, 2)[:, :, :, None, :]
        group_index = lax.axis_index("tensor")
        modulation = lax.dynamic_index_in_dim(group_mod, group_index, axis=2, keepdims=False)

    frame_index = lax.axis_index("frame")

    def order_by_half(mine, other):
        both = jnp.stack([mine, other])
        return jnp.where(frame_index == 0, both, both[::-1])

    def hidden_half(weights):
        half = weights[0].shape[1] // halves
        pieces = []
        for weight in weights:
            blocks = weight.reshape(rows_here, halves, half)
            mine = jnp.take(blocks, frame_index, axis=1)
            sent = jnp.take(blocks, 1 - frame_index, axis=1)
            received = lax.ppermute(sent, "frame", [(0, 1), (1, 0)])
            pieces.append(order_by_half(mine, received).reshape(halves * rows_here, half))
        joined = jnp.concatenate(pieces, axis=1)
        gathered = lax.all_gather(joined, "tensor", axis=0, tiled=True)
        gathered = lax.all_gather(gathered, "dp", axis=0, tiled=True)
        gathered = gathered.reshape(replicas, groups, halves * rows_here, len(weights), half)
        return tuple(
            jnp.swapaxes(gathered[:, :, :, k], 1, 2).reshape(model_width, groups * half)
            for k in range(len(weights))
        )

    def hidden_half_back(totals):
        half = totals[0].shape[1] // groups
        blocks = jnp.concatenate(
            [
                jnp.swapaxes(total.reshape(replicas, halves * rows_here, groups, half), 1, 2)
                for total in totals
            ],
            axis=3,
        ).astype(jnp.bfloat16)
        summed = lax.psum_scatter(
            blocks.reshape(replicas * groups, halves * rows_here, len(totals) * half),
            "dp",
            scatter_dimension=0,
            tiled=True,
        )
        summed = lax.psum_scatter(summed, "tensor", scatter_dimension=0, tiled=True)
        summed = summed[0].reshape(halves, rows_here, len(totals) * half)
        mine = jnp.take(summed, frame_index, axis=0).astype(jnp.float32)
        sent = jnp.take(summed, 1 - frame_index, axis=0)
        received = lax.ppermute(sent, "frame", [(0, 1), (1, 0)]).astype(jnp.float32)
        ordered = jnp.swapaxes(order_by_half(mine, received), 0, 1)
        ordered = ordered.reshape(rows_here, halves, len(totals), half)
        return tuple(
            ordered[:, :, k].reshape(rows_here, halves * half) for k in range(len(totals))
        )

    with jax.named_scope("weights"):
        joint_weight, mixer_weight = (
            lax.all_gather(w, ("dp", "frame"), axis=0, tiled=True)
            for w in (qkv_weight, out_weight)
        )
        upward_weight, downward_weight = hidden_half((up_weight, down_weight))

    residual = tokens[:, 0].astype(jnp.float32)
    upstream = out_grad[:, 0].astype(jnp.float32)
    with jax.named_scope("group_inputs"):
        group_tokens = lax.all_gather(tokens[:, 0], "tensor", axis=1, tiled=True)
        group_upstream = None
    def gather_halves(values):
        if halves != 2:
            return lax.all_gather(values, "frame", axis=1, tiled=True)
        other = lax.ppermute(values, "frame", [(0, 1), (1, 0)])
        return jnp.concatenate([values, other], axis=1)

    def scatter_halves(values):
        if halves != 2:
            return lax.psum_scatter(
                values.astype(jnp.bfloat16), "frame", scatter_dimension=1, tiled=True
            ).astype(jnp.float32)
        count = values.shape[1] // 2
        mine = values[:, :count]
        other = lax.ppermute(values[:, count:].astype(jnp.bfloat16), "frame", [(0, 1), (1, 0)])
        return mine.astype(jnp.bfloat16).astype(jnp.float32) + other.astype(jnp.float32)

    def clip_pass(residual, upstream, modulation, group_tokens, group_upstream, group_mod):
        clips = residual.shape[0]
        patches = residual.shape[1]
        shift1, scale1, gate1 = modulation[:, 0], modulation[:, 1], modulation[:, 2]
        shift2, scale2, gate2 = modulation[:, 3], modulation[:, 4], modulation[:, 5]
        def gather_tokens(values):
            return lax.all_gather(values, "tensor", axis=1, tiled=True)

        def scatter_tokens(values):
            parts = values.astype(jnp.bfloat16).reshape(
                values.shape[0], groups, -1, values.shape[-1]
            )
            received = lax.all_to_all(parts, "tensor", 1, 1, tiled=True)
            return jnp.sum(received.astype(jnp.float32), axis=1)

        with jax.named_scope("forward"):
            normed_one, inverse_one = normalize(residual)
            group_normed, _ = normalize(
                group_tokens.astype(jnp.float32).reshape(clips, groups, patches, model_width)
            )
            flat_one = (
                (group_normed * (1.0 + group_mod[:, 1]) + group_mod[:, 0])
                .astype(jnp.bfloat16)
                .reshape(clips, groups * patches, model_width)
            )
            token_count = flat_one.shape[1]
            projected = jnp.einsum(
                "crd,dkh->crkh", flat_one, joint_weight, preferred_element_type=jnp.float32
            ).astype(jnp.bfloat16)
            queries = projected[:, :, 0]
            keys_all = gather_halves(projected[:, :, 1])
            values_all = gather_halves(projected[:, :, 2])
            attended, log_totals = attention_forward(queries[0], keys_all[0], values_all[0])
            attended = attended[None]
            partial_one = jnp.einsum(
                "crh,oh->cro", attended, mixer_weight, preferred_element_type=jnp.float32
            )
            branch_one = scatter_tokens(partial_one)
            middle = residual + gate1 * branch_one
            normed_two, inverse_two = normalize(middle)
            entering_two = (normed_two * (1.0 + scale2) + shift2).astype(jnp.bfloat16)
            flat_two = gather_halves(entering_two)
            up_values = jnp.einsum(
                "crd,df->crf", flat_two, upward_weight, preferred_element_type=jnp.float32
            )
            hidden = gelu_tanh(up_values).astype(jnp.bfloat16)
            partial_two = jnp.einsum(
                "crf,of->cro", hidden, downward_weight, preferred_element_type=jnp.float32
            )
            branch_two = scatter_halves(partial_two)
            output = (middle + gate2 * branch_two).astype(jnp.bfloat16)

        with jax.named_scope("backward_ffn"):
            grad_gate_two = jnp.sum(upstream * branch_two, axis=1)
            grad_two_all = gather_halves((gate2 * upstream).astype(jnp.bfloat16))
            grad_hidden = jnp.einsum(
                "cro,of->crf", grad_two_all, downward_weight, preferred_element_type=jnp.float32
            )
            down_total = jnp.einsum(
                "cro,crf->of", grad_two_all, hidden, preferred_element_type=jnp.float32
            )
            _, gelu_pullback = jax.vjp(gelu_tanh, up_values)
            grad_up = gelu_pullback(grad_hidden)[0].astype(jnp.bfloat16)
            up_total = jnp.einsum(
                "crd,crf->df", flat_two, grad_up, preferred_element_type=jnp.float32
            )
            partial_back_two = jnp.einsum(
                "crf,df->crd", grad_up, upward_weight, preferred_element_type=jnp.float32
            )
            grad_entering_two = scatter_halves(partial_back_two)
            grad_shift_two = jnp.sum(grad_entering_two, axis=1)
            grad_scale_two = jnp.sum(grad_entering_two * normed_two, axis=1)
            grad_middle = upstream + norm_back(
                grad_entering_two * (1.0 + scale2), normed_two, inverse_two
            )
            grad_gate_one = jnp.sum(grad_middle * branch_one, axis=1)

        with jax.named_scope("backward_attention"):
            grad_branch_one = (gate1 * grad_middle).astype(jnp.bfloat16)
            grad_one_all = gather_tokens(grad_branch_one)
            grad_attended = jnp.einsum(
                "cro,oh->crh", grad_one_all, mixer_weight, preferred_element_type=jnp.float32
            ).astype(jnp.bfloat16)
            mixer_total = jnp.einsum(
                "cro,crh->oh", grad_one_all, attended, preferred_element_type=jnp.float32
            )
            query_grads, key_grads, value_grads = attention_backward(
                queries[0], keys_all[0], values_all[0], grad_attended[0], log_totals
            )
            query_grads = query_grads[None]
            key_grads = key_grads[None]
            value_grads = value_grads[None]
            key_own, value_own = (
                scatter_halves(grads.reshape(clips, -1, local_width))
                for grads in (key_grads, value_grads)
            )
            grad_projected = jnp.stack([query_grads, key_own, value_own], axis=2).astype(
                jnp.bfloat16
            )
            joint_total = jnp.einsum(
                "crd,crkh->dkh", flat_one, grad_projected, preferred_element_type=jnp.float32
            )
            partial_back_one = jnp.einsum(
                "crkh,dkh->crd", grad_projected, joint_weight, preferred_element_type=jnp.float32
            )
            grad_entering_one = scatter_tokens(partial_back_one)
            grad_shift_one = jnp.sum(grad_entering_one, axis=1)
            grad_scale_one = jnp.sum(grad_entering_one * normed_one, axis=1)
            grad_input = grad_middle + norm_back(
                grad_entering_one * (1.0 + scale1), normed_one, inverse_one
            )


        grad_modulation = jnp.stack(
            [grad_shift_one, grad_scale_one, grad_gate_one, grad_shift_two, grad_scale_two, grad_gate_two],
            axis=1,
        )
        totals = (joint_total, mixer_total, up_total, down_total)
        return output, grad_input.astype(jnp.bfloat16), grad_modulation, totals

    pieces = [
        clip_pass(
            residual[i : i + 1],
            upstream[i : i + 1],
            modulation[i : i + 1],
            group_tokens[i : i + 1],
            None,
            group_mod[i : i + 1],
        )
        for i in range(clips)
    ]
    output = jnp.concatenate([p[0] for p in pieces], axis=0)
    grad_input_low = jnp.concatenate([p[1] for p in pieces], axis=0)
    grad_modulation = jnp.concatenate([p[2] for p in pieces], axis=0)
    joint_total, mixer_total, up_total, down_total = (
        sum(p[3][k] for p in pieces[1:]) + pieces[0][3][k] for k in range(4)
    )
    with jax.named_scope("ada_grad"):
        grad_columns = lax.all_to_all(
            grad_modulation.reshape(clips, 1, 6, model_width), "tensor", 3, 1, tiled=True
        )
        grad_all = lax.all_gather(grad_columns, ("dp", "frame"), axis=0, tiled=True)
        grad_all = grad_all.reshape(replicas * halves, clips, groups, 6, local_width)
        adaptive_total = jnp.einsum(
            "acgd,acgkw->dkw",
            my_condition.astype(jnp.float32),
            grad_all,
            precision=highest,
        )

    with jax.named_scope("weight_grads"):
        joint_sum, mixer_sum = (
            lax.psum_scatter(
                total.astype(jnp.bfloat16), ("dp", "frame"), scatter_dimension=0, tiled=True
            ).astype(jnp.float32)
            for total in (joint_total, mixer_total)
        )
        up_sum, down_sum = hidden_half_back((up_total, down_total))
        summed = (joint_sum, mixer_sum, up_sum, down_sum)
    result = output[:, None]
    input_grad = grad_input_low[:, None]
    return (result, input_grad, summed[0], summed[1], summed[2], summed[3], adaptive_total)


def solution(mesh):
    return jax.shard_map(
        on_device,
        mesh=mesh,
        in_specs=(
            P("dp", ("frame", "tensor"), None, None),
            P("dp", ("frame", "tensor"), None, None),
            P("dp", "frame"),
            P(("dp", "frame"), None, "tensor"),
            P(("dp", "frame"), "tensor"),
            P(("dp", "frame"), "tensor"),
            P(("dp", "frame"), "tensor"),
            P(("dp", "frame"), None, "tensor"),
        ),
        out_specs=(
            P("dp", ("frame", "tensor"), None, None),
            P("dp", ("frame", "tensor"), None, None),
            P(("dp", "frame"), None, "tensor"),
            P(("dp", "frame"), "tensor"),
            P(("dp", "frame"), "tensor"),
            P(("dp", "frame"), "tensor"),
            P(("dp", "frame"), None, "tensor"),
        ),
        check_vma=False,
    )
```

```python
import functools
import math

import jax
import jax.numpy as jnp
from jax import lax
from jax.experimental import pallas as pl
from jax.experimental.pallas import tpu as pltpu
from jax.sharding import PartitionSpec as P

HEAD_DIM = 64


epsilon = 1e-06
highest = lax.Precision.HIGHEST


def normalize(values):
    center = values - jnp.mean(values, axis=-1, keepdims=True)
    spread = jnp.mean(center * center, axis=-1, keepdims=True)
    inverse = lax.rsqrt(spread + epsilon)
    return (center * inverse, inverse)


def norm_back(upstream, normed, inverse):
    upstream_mean = jnp.mean(upstream, axis=-1, keepdims=True)
    product_mean = jnp.mean(upstream * normed, axis=-1, keepdims=True)
    return inverse * (upstream - upstream_mean - normed * product_mean)


def level_embedding(levels, model_width):
    halfway = model_width // 2
    frequency = jnp.exp(-math.log(10000.0) * jnp.arange(halfway, dtype=jnp.float32) / halfway)
    angles = levels.astype(jnp.float32)[..., None] * frequency
    return jnp.concatenate([jnp.cos(angles), jnp.sin(angles)], axis=-1)


def _nt(a, b):
    return lax.dot_general(a, b, (((1,), (1,)), ((), ())), preferred_element_type=jnp.float32)


def _tn(a, b):
    return lax.dot_general(a, b, (((0,), (0,)), ((), ())), preferred_element_type=jnp.float32)


def _forward_kernel(heads, scaling, q_ref, k_ref, v_ref, o_ref, lse_ref):
    for h in range(heads):
        cols = slice(h * HEAD_DIM, (h + 1) * HEAD_DIM)
        scores = _nt(q_ref[:, cols], k_ref[:, cols]) * scaling
        largest = jnp.max(scores, axis=1, keepdims=True)
        raised = jnp.exp(scores - largest)
        total = jnp.sum(raised, axis=1, keepdims=True)
        probs_low = (raised / total).astype(jnp.bfloat16)
        out = jnp.dot(probs_low, v_ref[:, cols], preferred_element_type=jnp.float32)
        o_ref[:, cols] = out.astype(o_ref.dtype)
        lse_ref[:, h : h + 1] = largest + jnp.log(total)


def _backward_kernel(heads, scaling, q_ref, k_ref, v_ref, g_ref, lse_ref, dq_ref, dk_ref, dv_ref):
    @pl.when(pl.program_id(0) == 0)
    def _():
        dk_ref[...] = jnp.zeros_like(dk_ref)
        dv_ref[...] = jnp.zeros_like(dv_ref)

    for h in range(heads):
        cols = slice(h * HEAD_DIM, (h + 1) * HEAD_DIM)
        q = q_ref[:, cols]
        g = g_ref[:, cols]
        scores = _nt(q, k_ref[:, cols]) * scaling
        probs = jnp.exp(scores - lse_ref[:, h : h + 1])
        grad_probs = _nt(g, v_ref[:, cols])
        dv_ref[:, cols] += _tn(probs.astype(jnp.bfloat16), g)
        row_terms = jnp.sum(probs * grad_probs, axis=1, keepdims=True)
        grad_scores = (probs * (grad_probs - row_terms)).astype(jnp.bfloat16)
        dq_ref[:, cols] = jnp.dot(grad_scores, k_ref[:, cols], preferred_element_type=jnp.float32) * scaling
        dk_ref[:, cols] += _tn(grad_scores, q) * scaling


def attention_forward(queries, keys, values, block_rows=256):
    rows, width = queries.shape
    length = keys.shape[0]
    heads = width // HEAD_DIM
    block_rows = min(block_rows, rows)
    flops = 4 * rows * length * width
    return pl.pallas_call(
        functools.partial(_forward_kernel, heads, HEAD_DIM ** (-0.5)),
        out_shape=(
            jax.ShapeDtypeStruct((rows, width), jnp.bfloat16),
            jax.ShapeDtypeStruct((rows, heads), jnp.float32),
        ),
        grid=(rows // block_rows,),
        in_specs=[
            pl.BlockSpec((block_rows, width), lambda i: (i, 0)),
            pl.BlockSpec((length, width), lambda i: (0, 0)),
            pl.BlockSpec((length, width), lambda i: (0, 0)),
        ],
        out_specs=[
            pl.BlockSpec((block_rows, width), lambda i: (i, 0)),
            pl.BlockSpec((block_rows, heads), lambda i: (i, 0)),
        ],
        compiler_params=pltpu.CompilerParams(
            dimension_semantics=("arbitrary",), vmem_limit_bytes=56 * 1024 * 1024
        ),
        cost_estimate=pl.CostEstimate(
            flops=flops,
            transcendentals=rows * length * heads,
            bytes_accessed=2 * (2 * rows * width + 2 * length * width),
        ),
    )(queries, keys, values)


def attention_backward(queries, keys, values, grad_out, lse, block_rows=256):
    rows, width = queries.shape
    length = keys.shape[0]
    heads = width // HEAD_DIM
    block_rows = min(block_rows, rows)
    flops = 10 * rows * length * width
    return pl.pallas_call(
        functools.partial(_backward_kernel, heads, HEAD_DIM ** (-0.5)),
        out_shape=(
            jax.ShapeDtypeStruct((rows, width), jnp.float32),
            jax.ShapeDtypeStruct((length, width), jnp.float32),
            jax.ShapeDtypeStruct((length, width), jnp.float32),
        ),
        grid=(rows // block_rows,),
        in_specs=[
            pl.BlockSpec((block_rows, width), lambda i: (i, 0)),
            pl.BlockSpec((length, width), lambda i: (0, 0)),
            pl.BlockSpec((length, width), lambda i: (0, 0)),
            pl.BlockSpec((block_rows, width), lambda i: (i, 0)),
            pl.BlockSpec((block_rows, heads), lambda i: (i, 0)),
        ],
        out_specs=[
            pl.BlockSpec((block_rows, width), lambda i: (i, 0)),
            pl.BlockSpec((length, width), lambda i: (0, 0)),
            pl.BlockSpec((length, width), lambda i: (0, 0)),
        ],
        compiler_params=pltpu.CompilerParams(
            dimension_semantics=("arbitrary",), vmem_limit_bytes=56 * 1024 * 1024
        ),
        cost_estimate=pl.CostEstimate(
            flops=flops,
            transcendentals=rows * length * heads,
            bytes_accessed=2 * (3 * rows * width + 2 * length * width) + 4 * (rows + 2 * length) * width,
        ),
    )(queries, keys, values, grad_out, lse)


def gelu_tanh(values):
    return jax.nn.gelu(values, approximate=True)


def on_device(
    tokens, out_grad, noise_index, qkv_weight, out_weight, up_weight, down_weight, ada_weight
):
    clips = tokens.shape[0]
    patches = tokens.shape[2]
    model_width = tokens.shape[-1]
    local_width = qkv_weight.shape[2]
    rows_here = qkv_weight.shape[0]
    heads_here = local_width // HEAD_DIM
    scaling = HEAD_DIM ** (-0.5)
    groups = lax.axis_size("tensor")
    halves = lax.axis_size("frame")
    replicas = lax.axis_size("dp")

    with jax.named_scope("modulation"):
        levels_all = lax.all_gather(noise_index, ("dp", "frame"), axis=0, tiled=True)
        levels_all = levels_all.reshape(replicas * halves, clips, groups)
        condition_all = jax.nn.silu(level_embedding(levels_all, model_width)).astype(jnp.bfloat16)
        row_block = lax.axis_index("dp") * halves + lax.axis_index("frame")
        my_condition = lax.dynamic_slice_in_dim(
            condition_all, row_block * rows_here, rows_here, axis=3
        )
        partial_mod = jnp.einsum(
            "acgd,dkw->acgkw", my_condition, ada_weight, preferred_element_type=jnp.float32
        )
        summed_mod = jnp.sum(
            lax.all_to_all(partial_mod, ("dp", "frame"), 0, 0, tiled=True), axis=0
        )
        group_mod = lax.all_gather(summed_mod, "tensor", axis=3, tiled=True)
        group_mod = jnp.swapaxes(group_mod, 1, 2)[:, :, :, None, :]
        group_index = lax.axis_index("tensor")
        modulation = lax.dynamic_index_in_dim(group_mod, group_index, axis=2, keepdims=False)

    frame_index = lax.axis_index("frame")

    def order_by_half(mine, other):
        both = jnp.stack([mine, other])
        return jnp.where(frame_index == 0, both, both[::-1])

    def hidden_half(weights):
        half = weights[0].shape[1] // halves
        pieces = []
        for weight in weights:
            blocks = weight.reshape(rows_here, halves, half)
            mine = jnp.take(blocks, frame_index, axis=1)
            sent = jnp.take(blocks, 1 - frame_index, axis=1)
            received = lax.ppermute(sent, "frame", [(0, 1), (1, 0)])
            pieces.append(order_by_half(mine, received).reshape(halves * rows_here, half))
        joined = jnp.concatenate(pieces, axis=0)
        gathered = lax.all_gather(joined, "tensor", axis=0, tiled=True)
        gathered = lax.all_gather(gathered, "dp", axis=0, tiled=True)
        gathered = gathered.reshape(replicas, groups, len(weights), halves * rows_here, half)
        return tuple(gathered[:, :, k] for k in range(len(weights)))

    def hidden_half_back(totals):
        half = totals[0].shape[-1]
        blocks = jnp.concatenate(totals, axis=2).astype(jnp.bfloat16)
        summed = lax.psum_scatter(blocks, "dp", scatter_dimension=0, tiled=True)
        summed = lax.psum_scatter(summed, "tensor", scatter_dimension=1, tiled=True)
        summed = summed.reshape(len(totals), halves, rows_here, half)
        mine = jnp.take(summed, frame_index, axis=1).astype(jnp.float32)
        sent = jnp.take(summed, 1 - frame_index, axis=1)
        received = lax.ppermute(sent, "frame", [(0, 1), (1, 0)]).astype(jnp.float32)
        both = jnp.stack([mine, received], axis=1)
        ordered = jnp.where(frame_index == 0, both, both[:, ::-1])
        return tuple(
            jnp.swapaxes(ordered[k], 0, 1).reshape(rows_here, halves * half)
            for k in range(len(totals))
        )

    with jax.named_scope("weights"):
        joint_weight, mixer_weight = (
            lax.all_gather(w, ("dp", "frame"), axis=0, tiled=True)
            for w in (qkv_weight, out_weight)
        )
        upward_weight, downward_weight = hidden_half((up_weight, down_weight))

    residual = tokens[:, 0].astype(jnp.float32)
    upstream = out_grad[:, 0].astype(jnp.float32)
    with jax.named_scope("group_inputs"):
        group_tokens = lax.all_gather(tokens[:, 0], "tensor", axis=1, tiled=True)
        group_upstream = None
    def gather_halves(values):
        if halves != 2:
            return lax.all_gather(values, "frame", axis=1, tiled=True)
        other = lax.ppermute(values, "frame", [(0, 1), (1, 0)])
        return jnp.concatenate([values, other], axis=1)

    def scatter_halves(values):
        if halves != 2:
            return lax.psum_scatter(
                values.astype(jnp.bfloat16), "frame", scatter_dimension=1, tiled=True
            ).astype(jnp.float32)
        count = values.shape[1] // 2
        mine = values[:, :count]
        other = lax.ppermute(values[:, count:].astype(jnp.bfloat16), "frame", [(0, 1), (1, 0)])
        return mine.astype(jnp.bfloat16).astype(jnp.float32) + other.astype(jnp.float32)

    def clip_pass(residual, upstream, modulation, group_tokens, group_upstream, group_mod):
        clips = residual.shape[0]
        patches = residual.shape[1]
        shift1, scale1, gate1 = modulation[:, 0], modulation[:, 1], modulation[:, 2]
        shift2, scale2, gate2 = modulation[:, 3], modulation[:, 4], modulation[:, 5]
        def gather_tokens(values):
            return lax.all_gather(values, "tensor", axis=1, tiled=True)

        def scatter_tokens(values):
            parts = values.astype(jnp.bfloat16).reshape(
                values.shape[0], groups, -1, values.shape[-1]
            )
            received = lax.all_to_all(parts, "tensor", 1, 1, tiled=True)
            return jnp.sum(received.astype(jnp.float32), axis=1)

        with jax.named_scope("forward"):
            normed_one, inverse_one = normalize(residual)
            group_normed, _ = normalize(
                group_tokens.astype(jnp.float32).reshape(clips, groups, patches, model_width)
            )
            flat_one = (
                (group_normed * (1.0 + group_mod[:, 1]) + group_mod[:, 0])
                .astype(jnp.bfloat16)
                .reshape(clips, groups * patches, model_width)
            )
            token_count = flat_one.shape[1]
            projected = jnp.einsum(
                "crd,dkh->crkh", flat_one, joint_weight, preferred_element_type=jnp.float32
            ).astype(jnp.bfloat16)
            queries = projected[:, :, 0]
            keys_all = gather_halves(projected[:, :, 1])
            values_all = gather_halves(projected[:, :, 2])
            attended, log_totals = attention_forward(queries[0], keys_all[0], values_all[0])
            attended = attended[None]
            partial_one = jnp.einsum(
                "crh,oh->cro", attended, mixer_weight, preferred_element_type=jnp.float32
            )
            branch_one = scatter_tokens(partial_one)
            middle = residual + gate1 * branch_one
            normed_two, inverse_two = normalize(middle)
            entering_two = (normed_two * (1.0 + scale2) + shift2).astype(jnp.bfloat16)
            flat_two = gather_halves(entering_two)
            blocked_two = flat_two.reshape(clips, -1, replicas, halves * rows_here)
            up_values = jnp.einsum(
                "crad,atdj->crtj", blocked_two, upward_weight, preferred_element_type=jnp.float32
            )
            hidden = gelu_tanh(up_values).astype(jnp.bfloat16)
            partial_two = jnp.einsum(
                "crtj,atdj->crad", hidden, downward_weight, preferred_element_type=jnp.float32
            ).reshape(clips, -1, model_width)
            branch_two = scatter_halves(partial_two)
            output = (middle + gate2 * branch_two).astype(jnp.bfloat16)

        with jax.named_scope("backward_ffn"):
            grad_gate_two = jnp.sum(upstream * branch_two, axis=1)
            grad_two_all = gather_halves((gate2 * upstream).astype(jnp.bfloat16))
            blocked_grad = grad_two_all.reshape(clips, -1, replicas, halves * rows_here)
            grad_hidden = jnp.einsum(
                "crad,atdj->crtj", blocked_grad, downward_weight, preferred_element_type=jnp.float32
            )
            down_total = jnp.einsum(
                "crad,crtj->atdj", blocked_grad, hidden, preferred_element_type=jnp.float32
            )
            _, gelu_pullback = jax.vjp(gelu_tanh, up_values)
            grad_up = gelu_pullback(grad_hidden)[0].astype(jnp.bfloat16)
            up_total = jnp.einsum(
                "crad,crtj->atdj", blocked_two, grad_up, preferred_element_type=jnp.float32
            )
            partial_back_two = jnp.einsum(
                "crtj,atdj->crad", grad_up, upward_weight, preferred_element_type=jnp.float32
            ).reshape(clips, -1, model_width)
            grad_entering_two = scatter_halves(partial_back_two)
            grad_shift_two = jnp.sum(grad_entering_two, axis=1)
            grad_scale_two = jnp.sum(grad_entering_two * normed_two, axis=1)
            grad_middle = upstream + norm_back(
                grad_entering_two * (1.0 + scale2), normed_two, inverse_two
            )
            grad_gate_one = jnp.sum(grad_middle * branch_one, axis=1)

        with jax.named_scope("backward_attention"):
            grad_branch_one = (gate1 * grad_middle).astype(jnp.bfloat16)
            grad_one_all = gather_tokens(grad_branch_one)
            grad_attended = jnp.einsum(
                "cro,oh->crh", grad_one_all, mixer_weight, preferred_element_type=jnp.float32
            ).astype(jnp.bfloat16)
            mixer_total = jnp.einsum(
                "cro,crh->oh", grad_one_all, attended, preferred_element_type=jnp.float32
            )
            query_grads, key_grads, value_grads = attention_backward(
                queries[0], keys_all[0], values_all[0], grad_attended[0], log_totals
            )
            query_grads = query_grads[None]
            key_grads = key_grads[None]
            value_grads = value_grads[None]
            key_own, value_own = (
                scatter_halves(grads.reshape(clips, -1, local_width))
                for grads in (key_grads, value_grads)
            )
            grad_projected = jnp.stack([query_grads, key_own, value_own], axis=2).astype(
                jnp.bfloat16
            )
            joint_total = jnp.einsum(
                "crd,crkh->dkh", flat_one, grad_projected, preferred_element_type=jnp.float32
            )
            partial_back_one = jnp.einsum(
                "crkh,dkh->crd", grad_projected, joint_weight, preferred_element_type=jnp.float32
            )
            grad_entering_one = scatter_tokens(partial_back_one)
            grad_shift_one = jnp.sum(grad_entering_one, axis=1)
            grad_scale_one = jnp.sum(grad_entering_one * normed_one, axis=1)
            grad_input = grad_middle + norm_back(
                grad_entering_one * (1.0 + scale1), normed_one, inverse_one
            )


        grad_modulation = jnp.stack(
            [grad_shift_one, grad_scale_one, grad_gate_one, grad_shift_two, grad_scale_two, grad_gate_two],
            axis=1,
        )
        totals = (joint_total, mixer_total, up_total, down_total)
        return output, grad_input.astype(jnp.bfloat16), grad_modulation, totals

    pieces = [
        clip_pass(
            residual[i : i + 1],
            upstream[i : i + 1],
            modulation[i : i + 1],
            group_tokens[i : i + 1],
            None,
            group_mod[i : i + 1],
        )
        for i in range(clips)
    ]
    output = jnp.concatenate([p[0] for p in pieces], axis=0)
    grad_input_low = jnp.concatenate([p[1] for p in pieces], axis=0)
    grad_modulation = jnp.concatenate([p[2] for p in pieces], axis=0)
    joint_total, mixer_total, up_total, down_total = (
        sum(p[3][k] for p in pieces[1:]) + pieces[0][3][k] for k in range(4)
    )
    with jax.named_scope("ada_grad"):
        grad_columns = lax.all_to_all(
            grad_modulation.reshape(clips, 1, 6, model_width), "tensor", 3, 1, tiled=True
        )
        grad_all = lax.all_gather(grad_columns, ("dp", "frame"), axis=0, tiled=True)
        grad_all = grad_all.reshape(replicas * halves, clips, groups, 6, local_width)
        adaptive_total = jnp.einsum(
            "acgd,acgkw->dkw",
            my_condition.astype(jnp.float32),
            grad_all,
            precision=highest,
        )

    with jax.named_scope("weight_grads"):
        joint_sum, mixer_sum = (
            lax.psum_scatter(
                total.astype(jnp.bfloat16), ("dp", "frame"), scatter_dimension=0, tiled=True
            ).astype(jnp.float32)
            for total in (joint_total, mixer_total)
        )
        up_sum, down_sum = hidden_half_back((up_total, down_total))
        summed = (joint_sum, mixer_sum, up_sum, down_sum)
    result = output[:, None]
    input_grad = grad_input_low[:, None]
    return (result, input_grad, summed[0], summed[1], summed[2], summed[3], adaptive_total)


def solution(mesh):
    return jax.shard_map(
        on_device,
        mesh=mesh,
        in_specs=(
            P("dp", ("frame", "tensor"), None, None),
            P("dp", ("frame", "tensor"), None, None),
            P("dp", "frame"),
            P(("dp", "frame"), None, "tensor"),
            P(("dp", "frame"), "tensor"),
            P(("dp", "frame"), "tensor"),
            P(("dp", "frame"), "tensor"),
            P(("dp", "frame"), None, "tensor"),
        ),
        out_specs=(
            P("dp", ("frame", "tensor"), None, None),
            P("dp", ("frame", "tensor"), None, None),
            P(("dp", "frame"), None, "tensor"),
            P(("dp", "frame"), "tensor"),
            P(("dp", "frame"), "tensor"),
            P(("dp", "frame"), "tensor"),
            P(("dp", "frame"), None, "tensor"),
        ),
        check_vma=False,
    )
```

```python
import functools
import math

import jax
import jax.numpy as jnp
from jax import lax
from jax.experimental import pallas as pl
from jax.experimental.pallas import tpu as pltpu
from jax.sharding import PartitionSpec as P

HEAD_DIM = 64


epsilon = 1e-06
highest = lax.Precision.HIGHEST


def normalize(values):
    center = values - jnp.mean(values, axis=-1, keepdims=True)
    spread = jnp.mean(center * center, axis=-1, keepdims=True)
    inverse = lax.rsqrt(spread + epsilon)
    return (center * inverse, inverse)


def norm_back(upstream, normed, inverse):
    upstream_mean = jnp.mean(upstream, axis=-1, keepdims=True)
    product_mean = jnp.mean(upstream * normed, axis=-1, keepdims=True)
    return inverse * (upstream - upstream_mean - normed * product_mean)


def level_embedding(levels, model_width):
    halfway = model_width // 2
    frequency = jnp.exp(-math.log(10000.0) * jnp.arange(halfway, dtype=jnp.float32) / halfway)
    angles = levels.astype(jnp.float32)[..., None] * frequency
    return jnp.concatenate([jnp.cos(angles), jnp.sin(angles)], axis=-1)


def _nt(a, b):
    return lax.dot_general(a, b, (((1,), (1,)), ((), ())), preferred_element_type=jnp.float32)


def _tn(a, b):
    return lax.dot_general(a, b, (((0,), (0,)), ((), ())), preferred_element_type=jnp.float32)


def _forward_kernel(heads, scaling, q_ref, k_ref, v_ref, o_ref, lse_ref):
    for h in range(heads):
        cols = slice(h * HEAD_DIM, (h + 1) * HEAD_DIM)
        scores = _nt(q_ref[:, cols], k_ref[:, cols]) * scaling
        largest = jnp.max(scores, axis=1, keepdims=True)
        raised = jnp.exp(scores - largest)
        total = jnp.sum(raised, axis=1, keepdims=True)
        probs_low = (raised / total).astype(jnp.bfloat16)
        out = jnp.dot(probs_low, v_ref[:, cols], preferred_element_type=jnp.float32)
        o_ref[:, cols] = out.astype(o_ref.dtype)
        lse_ref[:, h : h + 1] = largest + jnp.log(total)


def _backward_kernel(heads, scaling, q_ref, k_ref, v_ref, g_ref, lse_ref, dq_ref, dk_ref, dv_ref):
    @pl.when(pl.program_id(0) == 0)
    def _():
        dk_ref[...] = jnp.zeros_like(dk_ref)
        dv_ref[...] = jnp.zeros_like(dv_ref)

    for h in range(heads):
        cols = slice(h * HEAD_DIM, (h + 1) * HEAD_DIM)
        q = q_ref[:, cols]
        g = g_ref[:, cols]
        scores = _nt(q, k_ref[:, cols]) * scaling
        probs = jnp.exp(scores - lse_ref[:, h : h + 1])
        grad_probs = _nt(g, v_ref[:, cols])
        dv_ref[:, cols] += _tn(probs.astype(jnp.bfloat16), g)
        row_terms = jnp.sum(probs * grad_probs, axis=1, keepdims=True)
        grad_scores = (probs * (grad_probs - row_terms)).astype(jnp.bfloat16)
        dq_ref[:, cols] = jnp.dot(grad_scores, k_ref[:, cols], preferred_element_type=jnp.float32) * scaling
        dk_ref[:, cols] += _tn(grad_scores, q) * scaling


def attention_forward(queries, keys, values, block_rows=256):
    rows, width = queries.shape
    length = keys.shape[0]
    heads = width // HEAD_DIM
    block_rows = min(block_rows, rows)
    flops = 4 * rows * length * width
    return pl.pallas_call(
        functools.partial(_forward_kernel, heads, HEAD_DIM ** (-0.5)),
        out_shape=(
            jax.ShapeDtypeStruct((rows, width), jnp.bfloat16),
            jax.ShapeDtypeStruct((rows, heads), jnp.float32),
        ),
        grid=(rows // block_rows,),
        in_specs=[
            pl.BlockSpec((block_rows, width), lambda i: (i, 0)),
            pl.BlockSpec((length, width), lambda i: (0, 0)),
            pl.BlockSpec((length, width), lambda i: (0, 0)),
        ],
        out_specs=[
            pl.BlockSpec((block_rows, width), lambda i: (i, 0)),
            pl.BlockSpec((block_rows, heads), lambda i: (i, 0)),
        ],
        compiler_params=pltpu.CompilerParams(
            dimension_semantics=("arbitrary",), vmem_limit_bytes=56 * 1024 * 1024
        ),
        cost_estimate=pl.CostEstimate(
            flops=flops,
            transcendentals=rows * length * heads,
            bytes_accessed=2 * (2 * rows * width + 2 * length * width),
        ),
    )(queries, keys, values)


def attention_backward(queries, keys, values, grad_out, lse, block_rows=256):
    rows, width = queries.shape
    length = keys.shape[0]
    heads = width // HEAD_DIM
    block_rows = min(block_rows, rows)
    flops = 10 * rows * length * width
    return pl.pallas_call(
        functools.partial(_backward_kernel, heads, HEAD_DIM ** (-0.5)),
        out_shape=(
            jax.ShapeDtypeStruct((rows, width), jnp.float32),
            jax.ShapeDtypeStruct((length, width), jnp.float32),
            jax.ShapeDtypeStruct((length, width), jnp.float32),
        ),
        grid=(rows // block_rows,),
        in_specs=[
            pl.BlockSpec((block_rows, width), lambda i: (i, 0)),
            pl.BlockSpec((length, width), lambda i: (0, 0)),
            pl.BlockSpec((length, width), lambda i: (0, 0)),
            pl.BlockSpec((block_rows, width), lambda i: (i, 0)),
            pl.BlockSpec((block_rows, heads), lambda i: (i, 0)),
        ],
        out_specs=[
            pl.BlockSpec((block_rows, width), lambda i: (i, 0)),
            pl.BlockSpec((length, width), lambda i: (0, 0)),
            pl.BlockSpec((length, width), lambda i: (0, 0)),
        ],
        compiler_params=pltpu.CompilerParams(
            dimension_semantics=("arbitrary",), vmem_limit_bytes=56 * 1024 * 1024
        ),
        cost_estimate=pl.CostEstimate(
            flops=flops,
            transcendentals=rows * length * heads,
            bytes_accessed=2 * (3 * rows * width + 2 * length * width) + 4 * (rows + 2 * length) * width,
        ),
    )(queries, keys, values, grad_out, lse)


def gelu_tanh(values):
    return jax.nn.gelu(values, approximate=True)


def on_device(
    tokens, out_grad, noise_index, qkv_weight, out_weight, up_weight, down_weight, ada_weight
):
    clips = tokens.shape[0]
    patches = tokens.shape[2]
    model_width = tokens.shape[-1]
    local_width = qkv_weight.shape[2]
    rows_here = qkv_weight.shape[0]
    heads_here = local_width // HEAD_DIM
    scaling = HEAD_DIM ** (-0.5)
    groups = lax.axis_size("tensor")
    halves = lax.axis_size("frame")
    replicas = lax.axis_size("dp")

    with jax.named_scope("modulation"):
        levels_all = lax.all_gather(noise_index, ("dp", "frame"), axis=0, tiled=True)
        levels_all = levels_all.reshape(replicas * halves, clips, groups)
        condition_all = jax.nn.silu(level_embedding(levels_all, model_width)).astype(jnp.bfloat16)
        row_block = lax.axis_index("dp") * halves + lax.axis_index("frame")
        my_condition = lax.dynamic_slice_in_dim(
            condition_all, row_block * rows_here, rows_here, axis=3
        )
        partial_mod = jnp.einsum(
            "acgd,dkw->acgkw", my_condition, ada_weight, preferred_element_type=jnp.float32
        )
        summed_mod = jnp.sum(
            lax.all_to_all(partial_mod, ("dp", "frame"), 0, 0, tiled=True), axis=0
        )
        group_mod = lax.all_gather(summed_mod, "tensor", axis=3, tiled=True)
        group_mod = jnp.swapaxes(group_mod, 1, 2)[:, :, :, None, :]
        group_index = lax.axis_index("tensor")
        modulation = lax.dynamic_index_in_dim(group_mod, group_index, axis=2, keepdims=False)

    frame_index = lax.axis_index("frame")

    def order_by_half(mine, other):
        both = jnp.stack([mine, other])
        return jnp.where(frame_index == 0, both, both[::-1])

    def hidden_half(weights):
        half = weights[0].shape[1] // halves
        pieces = []
        for weight in weights:
            blocks = weight.reshape(rows_here, halves, half)
            mine = jnp.take(blocks, frame_index, axis=1)
            sent = jnp.take(blocks, 1 - frame_index, axis=1)
            received = lax.ppermute(sent, "frame", [(0, 1), (1, 0)])
            pieces.append(order_by_half(mine, received).reshape(halves * rows_here, half))
        joined = jnp.concatenate(pieces, axis=0)
        gathered = lax.all_gather(joined, "tensor", axis=0, tiled=True)
        gathered = lax.all_gather(gathered, "dp", axis=0, tiled=True)
        gathered = gathered.reshape(replicas, groups, len(weights), halves * rows_here, half)
        return tuple(gathered[:, :, k] for k in range(len(weights)))

    def hidden_half_back(totals):
        half = totals[0].shape[-1]
        blocks = jnp.concatenate(totals, axis=2).astype(jnp.bfloat16)
        blocks = blocks.reshape(replicas * groups, len(totals) * halves * rows_here, half)
        summed = lax.psum_scatter(blocks, "dp", scatter_dimension=0, tiled=True)
        summed = lax.psum_scatter(summed, "tensor", scatter_dimension=0, tiled=True)
        summed = summed.reshape(len(totals), halves, rows_here, half)
        mine = jnp.take(summed, frame_index, axis=1).astype(jnp.float32)
        sent = jnp.take(summed, 1 - frame_index, axis=1)
        received = lax.ppermute(sent, "frame", [(0, 1), (1, 0)]).astype(jnp.float32)
        both = jnp.stack([mine, received], axis=1)
        ordered = jnp.where(frame_index == 0, both, both[:, ::-1])
        return tuple(
            jnp.swapaxes(ordered[k], 0, 1).reshape(rows_here, halves * half)
            for k in range(len(totals))
        )

    with jax.named_scope("weights"):
        joint_weight, mixer_weight = (
            lax.all_gather(w, ("dp", "frame"), axis=0, tiled=True)
            for w in (qkv_weight, out_weight)
        )
        upward_weight, downward_weight = hidden_half((up_weight, down_weight))

    residual = tokens[:, 0].astype(jnp.float32)
    upstream = out_grad[:, 0].astype(jnp.float32)
    with jax.named_scope("group_inputs"):
        group_tokens = lax.all_gather(tokens[:, 0], "tensor", axis=1, tiled=True)
        group_upstream = None
    def gather_halves(values):
        if halves != 2:
            return lax.all_gather(values, "frame", axis=1, tiled=True)
        other = lax.ppermute(values, "frame", [(0, 1), (1, 0)])
        return jnp.concatenate([values, other], axis=1)

    def scatter_halves(values):
        if halves != 2:
            return lax.psum_scatter(
                values.astype(jnp.bfloat16), "frame", scatter_dimension=1, tiled=True
            ).astype(jnp.float32)
        count = values.shape[1] // 2
        mine = values[:, :count]
        other = lax.ppermute(values[:, count:].astype(jnp.bfloat16), "frame", [(0, 1), (1, 0)])
        return mine.astype(jnp.bfloat16).astype(jnp.float32) + other.astype(jnp.float32)

    def clip_pass(residual, upstream, modulation, group_tokens, group_upstream, group_mod):
        clips = residual.shape[0]
        patches = residual.shape[1]
        shift1, scale1, gate1 = modulation[:, 0], modulation[:, 1], modulation[:, 2]
        shift2, scale2, gate2 = modulation[:, 3], modulation[:, 4], modulation[:, 5]
        def gather_tokens(values):
            return lax.all_gather(values, "tensor", axis=1, tiled=True)

        def scatter_tokens(values):
            parts = values.astype(jnp.bfloat16).reshape(
                values.shape[0], groups, -1, values.shape[-1]
            )
            received = lax.all_to_all(parts, "tensor", 1, 1, tiled=True)
            return jnp.sum(received.astype(jnp.float32), axis=1)

        with jax.named_scope("forward"):
            normed_one, inverse_one = normalize(residual)
            group_normed, _ = normalize(
                group_tokens.astype(jnp.float32).reshape(clips, groups, patches, model_width)
            )
            flat_one = (
                (group_normed * (1.0 + group_mod[:, 1]) + group_mod[:, 0])
                .astype(jnp.bfloat16)
                .reshape(clips, groups * patches, model_width)
            )
            token_count = flat_one.shape[1]
            projected = jnp.einsum(
                "crd,dkh->crkh", flat_one, joint_weight, preferred_element_type=jnp.float32
            ).astype(jnp.bfloat16)
            queries = projected[:, :, 0]
            keys_all = gather_halves(projected[:, :, 1])
            values_all = gather_halves(projected[:, :, 2])
            attended, log_totals = attention_forward(queries[0], keys_all[0], values_all[0])
            attended = attended[None]
            partial_one = jnp.einsum(
                "crh,oh->cro", attended, mixer_weight, preferred_element_type=jnp.float32
            )
            branch_one = scatter_tokens(partial_one)
            middle = residual + gate1 * branch_one
            normed_two, inverse_two = normalize(middle)
            entering_two = (normed_two * (1.0 + scale2) + shift2).astype(jnp.bfloat16)
            flat_two = gather_halves(entering_two)
            blocked_two = flat_two.reshape(clips, -1, replicas, halves * rows_here)
            up_values = jnp.einsum(
                "crad,atdj->crtj", blocked_two, upward_weight, preferred_element_type=jnp.float32
            )
            hidden = gelu_tanh(up_values).astype(jnp.bfloat16)
            partial_two = jnp.einsum(
                "crtj,atdj->crad", hidden, downward_weight, preferred_element_type=jnp.float32
            ).reshape(clips, -1, model_width)
            branch_two = scatter_halves(partial_two)
            output = (middle + gate2 * branch_two).astype(jnp.bfloat16)

        with jax.named_scope("backward_ffn"):
            grad_gate_two = jnp.sum(upstream * branch_two, axis=1)
            grad_two_all = gather_halves((gate2 * upstream).astype(jnp.bfloat16))
            blocked_grad = grad_two_all.reshape(clips, -1, replicas, halves * rows_here)
            grad_hidden = jnp.einsum(
                "crad,atdj->crtj", blocked_grad, downward_weight, preferred_element_type=jnp.float32
            )
            down_total = jnp.einsum(
                "crad,crtj->atdj", blocked_grad, hidden, preferred_element_type=jnp.float32
            )
            _, gelu_pullback = jax.vjp(gelu_tanh, up_values)
            grad_up = gelu_pullback(grad_hidden)[0].astype(jnp.bfloat16)
            up_total = jnp.einsum(
                "crad,crtj->atdj", blocked_two, grad_up, preferred_element_type=jnp.float32
            )
            partial_back_two = jnp.einsum(
                "crtj,atdj->crad", grad_up, upward_weight, preferred_element_type=jnp.float32
            ).reshape(clips, -1, model_width)
            grad_entering_two = scatter_halves(partial_back_two)
            grad_shift_two = jnp.sum(grad_entering_two, axis=1)
            grad_scale_two = jnp.sum(grad_entering_two * normed_two, axis=1)
            grad_middle = upstream + norm_back(
                grad_entering_two * (1.0 + scale2), normed_two, inverse_two
            )
            grad_gate_one = jnp.sum(grad_middle * branch_one, axis=1)

        with jax.named_scope("backward_attention"):
            grad_branch_one = (gate1 * grad_middle).astype(jnp.bfloat16)
            grad_one_all = gather_tokens(grad_branch_one)
            grad_attended = jnp.einsum(
                "cro,oh->crh", grad_one_all, mixer_weight, preferred_element_type=jnp.float32
            ).astype(jnp.bfloat16)
            mixer_total = jnp.einsum(
                "cro,crh->oh", grad_one_all, attended, preferred_element_type=jnp.float32
            )
            query_grads, key_grads, value_grads = attention_backward(
                queries[0], keys_all[0], values_all[0], grad_attended[0], log_totals
            )
            query_grads = query_grads[None]
            key_grads = key_grads[None]
            value_grads = value_grads[None]
            key_own, value_own = (
                scatter_halves(grads.reshape(clips, -1, local_width))
                for grads in (key_grads, value_grads)
            )
            grad_projected = jnp.stack([query_grads, key_own, value_own], axis=2).astype(
                jnp.bfloat16
            )
            joint_total = jnp.einsum(
                "crd,crkh->dkh", flat_one, grad_projected, preferred_element_type=jnp.float32
            )
            partial_back_one = jnp.einsum(
                "crkh,dkh->crd", grad_projected, joint_weight, preferred_element_type=jnp.float32
            )
            grad_entering_one = scatter_tokens(partial_back_one)
            grad_shift_one = jnp.sum(grad_entering_one, axis=1)
            grad_scale_one = jnp.sum(grad_entering_one * normed_one, axis=1)
            grad_input = grad_middle + norm_back(
                grad_entering_one * (1.0 + scale1), normed_one, inverse_one
            )


        grad_modulation = jnp.stack(
            [grad_shift_one, grad_scale_one, grad_gate_one, grad_shift_two, grad_scale_two, grad_gate_two],
            axis=1,
        )
        totals = (joint_total, mixer_total, up_total, down_total)
        return output, grad_input.astype(jnp.bfloat16), grad_modulation, totals

    pieces = [
        clip_pass(
            residual[i : i + 1],
            upstream[i : i + 1],
            modulation[i : i + 1],
            group_tokens[i : i + 1],
            None,
            group_mod[i : i + 1],
        )
        for i in range(clips)
    ]
    output = jnp.concatenate([p[0] for p in pieces], axis=0)
    grad_input_low = jnp.concatenate([p[1] for p in pieces], axis=0)
    grad_modulation = jnp.concatenate([p[2] for p in pieces], axis=0)
    joint_total, mixer_total, up_total, down_total = (
        sum(p[3][k] for p in pieces[1:]) + pieces[0][3][k] for k in range(4)
    )
    with jax.named_scope("ada_grad"):
        grad_columns = lax.all_to_all(
            grad_modulation.reshape(clips, 1, 6, model_width), "tensor", 3, 1, tiled=True
        )
        grad_all = lax.all_gather(grad_columns, ("dp", "frame"), axis=0, tiled=True)
        grad_all = grad_all.reshape(replicas * halves, clips, groups, 6, local_width)
        adaptive_total = jnp.einsum(
            "acgd,acgkw->dkw",
            my_condition.astype(jnp.float32),
            grad_all,
            precision=highest,
        )

    with jax.named_scope("weight_grads"):
        joint_sum, mixer_sum = (
            lax.psum_scatter(
                total.astype(jnp.bfloat16), ("dp", "frame"), scatter_dimension=0, tiled=True
            ).astype(jnp.float32)
            for total in (joint_total, mixer_total)
        )
        up_sum, down_sum = hidden_half_back((up_total, down_total))
        summed = (joint_sum, mixer_sum, up_sum, down_sum)
    result = output[:, None]
    input_grad = grad_input_low[:, None]
    return (result, input_grad, summed[0], summed[1], summed[2], summed[3], adaptive_total)


def solution(mesh):
    return jax.shard_map(
        on_device,
        mesh=mesh,
        in_specs=(
            P("dp", ("frame", "tensor"), None, None),
            P("dp", ("frame", "tensor"), None, None),
            P("dp", "frame"),
            P(("dp", "frame"), None, "tensor"),
            P(("dp", "frame"), "tensor"),
            P(("dp", "frame"), "tensor"),
            P(("dp", "frame"), "tensor"),
            P(("dp", "frame"), None, "tensor"),
        ),
        out_specs=(
            P("dp", ("frame", "tensor"), None, None),
            P("dp", ("frame", "tensor"), None, None),
            P(("dp", "frame"), None, "tensor"),
            P(("dp", "frame"), "tensor"),
            P(("dp", "frame"), "tensor"),
            P(("dp", "frame"), "tensor"),
            P(("dp", "frame"), None, "tensor"),
        ),
        check_vma=False,
    )
```

```python
import functools
import math

import jax
import jax.numpy as jnp
from jax import lax
from jax.experimental import pallas as pl
from jax.experimental.pallas import tpu as pltpu
from jax.sharding import PartitionSpec as P

HEAD_DIM = 64


epsilon = 1e-06
highest = lax.Precision.HIGHEST


def normalize(values):
    center = values - jnp.mean(values, axis=-1, keepdims=True)
    spread = jnp.mean(center * center, axis=-1, keepdims=True)
    inverse = lax.rsqrt(spread + epsilon)
    return (center * inverse, inverse)


def norm_back(upstream, normed, inverse):
    upstream_mean = jnp.mean(upstream, axis=-1, keepdims=True)
    product_mean = jnp.mean(upstream * normed, axis=-1, keepdims=True)
    return inverse * (upstream - upstream_mean - normed * product_mean)


def level_embedding(levels, model_width):
    halfway = model_width // 2
    frequency = jnp.exp(-math.log(10000.0) * jnp.arange(halfway, dtype=jnp.float32) / halfway)
    angles = levels.astype(jnp.float32)[..., None] * frequency
    return jnp.concatenate([jnp.cos(angles), jnp.sin(angles)], axis=-1)


def _nt(a, b):
    return lax.dot_general(a, b, (((1,), (1,)), ((), ())), preferred_element_type=jnp.float32)


def _tn(a, b):
    return lax.dot_general(a, b, (((0,), (0,)), ((), ())), preferred_element_type=jnp.float32)


def _forward_kernel(heads, scaling, q_ref, k_ref, v_ref, o_ref, lse_ref):
    for h in range(heads):
        cols = slice(h * HEAD_DIM, (h + 1) * HEAD_DIM)
        scores = _nt(q_ref[:, cols], k_ref[:, cols]) * scaling
        largest = jnp.max(scores, axis=1, keepdims=True)
        raised = jnp.exp(scores - largest)
        total = jnp.sum(raised, axis=1, keepdims=True)
        probs_low = (raised / total).astype(jnp.bfloat16)
        out = jnp.dot(probs_low, v_ref[:, cols], preferred_element_type=jnp.float32)
        o_ref[:, cols] = out.astype(o_ref.dtype)
        lse_ref[:, h : h + 1] = largest + jnp.log(total)


def _backward_kernel(heads, scaling, q_ref, k_ref, v_ref, g_ref, lse_ref, dq_ref, dk_ref, dv_ref):
    @pl.when(pl.program_id(0) == 0)
    def _():
        dk_ref[...] = jnp.zeros_like(dk_ref)
        dv_ref[...] = jnp.zeros_like(dv_ref)

    for h in range(heads):
        cols = slice(h * HEAD_DIM, (h + 1) * HEAD_DIM)
        q = q_ref[:, cols]
        g = g_ref[:, cols]
        scores = _nt(q, k_ref[:, cols]) * scaling
        probs = jnp.exp(scores - lse_ref[:, h : h + 1])
        grad_probs = _nt(g, v_ref[:, cols])
        dv_ref[:, cols] += _tn(probs.astype(jnp.bfloat16), g)
        row_terms = jnp.sum(probs * grad_probs, axis=1, keepdims=True)
        grad_scores = (probs * (grad_probs - row_terms)).astype(jnp.bfloat16)
        dq_ref[:, cols] = jnp.dot(grad_scores, k_ref[:, cols], preferred_element_type=jnp.float32) * scaling
        dk_ref[:, cols] += _tn(grad_scores, q) * scaling


def attention_forward(queries, keys, values, block_rows=256):
    rows, width = queries.shape
    length = keys.shape[0]
    heads = width // HEAD_DIM
    block_rows = min(block_rows, rows)
    flops = 4 * rows * length * width
    return pl.pallas_call(
        functools.partial(_forward_kernel, heads, HEAD_DIM ** (-0.5)),
        out_shape=(
            jax.ShapeDtypeStruct((rows, width), jnp.bfloat16),
            jax.ShapeDtypeStruct((rows, heads), jnp.float32),
        ),
        grid=(rows // block_rows,),
        in_specs=[
            pl.BlockSpec((block_rows, width), lambda i: (i, 0)),
            pl.BlockSpec((length, width), lambda i: (0, 0)),
            pl.BlockSpec((length, width), lambda i: (0, 0)),
        ],
        out_specs=[
            pl.BlockSpec((block_rows, width), lambda i: (i, 0)),
            pl.BlockSpec((block_rows, heads), lambda i: (i, 0)),
        ],
        compiler_params=pltpu.CompilerParams(
            dimension_semantics=("arbitrary",), vmem_limit_bytes=56 * 1024 * 1024
        ),
        cost_estimate=pl.CostEstimate(
            flops=flops,
            transcendentals=rows * length * heads,
            bytes_accessed=2 * (2 * rows * width + 2 * length * width),
        ),
    )(queries, keys, values)


def attention_backward(queries, keys, values, grad_out, lse, block_rows=256):
    rows, width = queries.shape
    length = keys.shape[0]
    heads = width // HEAD_DIM
    block_rows = min(block_rows, rows)
    flops = 10 * rows * length * width
    return pl.pallas_call(
        functools.partial(_backward_kernel, heads, HEAD_DIM ** (-0.5)),
        out_shape=(
            jax.ShapeDtypeStruct((rows, width), jnp.float32),
            jax.ShapeDtypeStruct((length, width), jnp.float32),
            jax.ShapeDtypeStruct((length, width), jnp.float32),
        ),
        grid=(rows // block_rows,),
        in_specs=[
            pl.BlockSpec((block_rows, width), lambda i: (i, 0)),
            pl.BlockSpec((length, width), lambda i: (0, 0)),
            pl.BlockSpec((length, width), lambda i: (0, 0)),
            pl.BlockSpec((block_rows, width), lambda i: (i, 0)),
            pl.BlockSpec((block_rows, heads), lambda i: (i, 0)),
        ],
        out_specs=[
            pl.BlockSpec((block_rows, width), lambda i: (i, 0)),
            pl.BlockSpec((length, width), lambda i: (0, 0)),
            pl.BlockSpec((length, width), lambda i: (0, 0)),
        ],
        compiler_params=pltpu.CompilerParams(
            dimension_semantics=("arbitrary",), vmem_limit_bytes=56 * 1024 * 1024
        ),
        cost_estimate=pl.CostEstimate(
            flops=flops,
            transcendentals=rows * length * heads,
            bytes_accessed=2 * (3 * rows * width + 2 * length * width) + 4 * (rows + 2 * length) * width,
        ),
    )(queries, keys, values, grad_out, lse)


def gelu_tanh(values):
    return jax.nn.gelu(values, approximate=True)


def on_device(
    tokens, out_grad, noise_index, qkv_weight, out_weight, up_weight, down_weight, ada_weight
):
    clips = tokens.shape[0]
    patches = tokens.shape[2]
    model_width = tokens.shape[-1]
    local_width = qkv_weight.shape[2]
    rows_here = qkv_weight.shape[0]
    heads_here = local_width // HEAD_DIM
    scaling = HEAD_DIM ** (-0.5)
    groups = lax.axis_size("tensor")
    halves = lax.axis_size("frame")
    replicas = lax.axis_size("dp")

    with jax.named_scope("modulation"):
        levels_all = lax.all_gather(noise_index, ("dp", "frame"), axis=0, tiled=True)
        levels_all = levels_all.reshape(replicas * halves, clips, groups)
        condition_all = jax.nn.silu(level_embedding(levels_all, model_width)).astype(jnp.bfloat16)
        row_block = lax.axis_index("dp") * halves + lax.axis_index("frame")
        my_condition = lax.dynamic_slice_in_dim(
            condition_all, row_block * rows_here, rows_here, axis=3
        )
        partial_mod = jnp.einsum(
            "acgd,dkw->acgkw", my_condition, ada_weight, preferred_element_type=jnp.float32
        )
        summed_mod = jnp.sum(
            lax.all_to_all(partial_mod, ("dp", "frame"), 0, 0, tiled=True), axis=0
        )
        group_mod = lax.all_gather(summed_mod, "tensor", axis=3, tiled=True)
        group_mod = jnp.swapaxes(group_mod, 1, 2)[:, :, :, None, :]
        group_index = lax.axis_index("tensor")
        modulation = lax.dynamic_index_in_dim(group_mod, group_index, axis=2, keepdims=False)

    frame_index = lax.axis_index("frame")

    def order_by_half(mine, other):
        both = jnp.stack([mine, other])
        return jnp.where(frame_index == 0, both, both[::-1])

    def hidden_half(weights):
        half = weights[0].shape[1] // halves
        pieces = []
        for weight in weights:
            blocks = weight.reshape(rows_here, halves, half)
            mine = jnp.take(blocks, frame_index, axis=1)
            sent = jnp.take(blocks, 1 - frame_index, axis=1)
            received = lax.ppermute(sent, "frame", [(0, 1), (1, 0)])
            pieces.append(order_by_half(mine, received).reshape(halves * rows_here, half))
        joined = jnp.concatenate(pieces, axis=0)
        gathered = lax.all_gather(joined, "tensor", axis=0, tiled=True)
        gathered = lax.all_gather(gathered, "dp", axis=0, tiled=True)
        gathered = gathered.reshape(replicas, groups, len(weights), halves * rows_here, half)
        return tuple(gathered[:, :, k] for k in range(len(weights)))

    def hidden_half_back(totals):
        half = totals[0].shape[-1]
        blocks = jnp.concatenate(totals, axis=2).astype(jnp.bfloat16)
        blocks = blocks.reshape(replicas * groups, len(totals) * halves * rows_here, half)
        summed = lax.psum_scatter(blocks, "dp", scatter_dimension=0, tiled=True)
        summed = lax.psum_scatter(summed, "tensor", scatter_dimension=0, tiled=True)
        summed = summed.reshape(len(totals), halves, rows_here, half)
        mine = jnp.take(summed, frame_index, axis=1).astype(jnp.float32)
        sent = jnp.take(summed, 1 - frame_index, axis=1)
        received = lax.ppermute(sent, "frame", [(0, 1), (1, 0)]).astype(jnp.float32)
        both = jnp.stack([mine, received], axis=1)
        ordered = jnp.where(frame_index == 0, both, both[:, ::-1])
        return tuple(
            jnp.swapaxes(ordered[k], 0, 1).reshape(rows_here, halves * half)
            for k in range(len(totals))
        )

    with jax.named_scope("weights"):
        joint_weight, mixer_weight = (
            lax.all_gather(w, ("dp", "frame"), axis=0, tiled=True)
            for w in (qkv_weight, out_weight)
        )

    residual = tokens[:, 0].astype(jnp.float32)
    upstream = out_grad[:, 0].astype(jnp.float32)
    with jax.named_scope("group_inputs"):
        group_tokens = lax.all_gather(tokens[:, 0], "tensor", axis=1, tiled=True)
        group_upstream = None
    with jax.named_scope("ffn_weights"):
        group_tokens, joint_weight, mixer_weight, ffn_shards = lax.optimization_barrier(
            (group_tokens, joint_weight, mixer_weight, (up_weight, down_weight))
        )
        upward_weight, downward_weight = hidden_half(ffn_shards)
    def gather_halves(values):
        if halves != 2:
            return lax.all_gather(values, "frame", axis=1, tiled=True)
        other = lax.ppermute(values, "frame", [(0, 1), (1, 0)])
        return jnp.concatenate([values, other], axis=1)

    def scatter_halves(values):
        if halves != 2:
            return lax.psum_scatter(
                values.astype(jnp.bfloat16), "frame", scatter_dimension=1, tiled=True
            ).astype(jnp.float32)
        count = values.shape[1] // 2
        mine = values[:, :count]
        other = lax.ppermute(values[:, count:].astype(jnp.bfloat16), "frame", [(0, 1), (1, 0)])
        return mine.astype(jnp.bfloat16).astype(jnp.float32) + other.astype(jnp.float32)

    def clip_pass(residual, upstream, modulation, group_tokens, group_upstream, group_mod):
        clips = residual.shape[0]
        patches = residual.shape[1]
        shift1, scale1, gate1 = modulation[:, 0], modulation[:, 1], modulation[:, 2]
        shift2, scale2, gate2 = modulation[:, 3], modulation[:, 4], modulation[:, 5]
        def gather_tokens(values):
            return lax.all_gather(values, "tensor", axis=1, tiled=True)

        def scatter_tokens(values):
            parts = values.astype(jnp.bfloat16).reshape(
                values.shape[0], groups, -1, values.shape[-1]
            )
            received = lax.all_to_all(parts, "tensor", 1, 1, tiled=True)
            return jnp.sum(received.astype(jnp.float32), axis=1)

        with jax.named_scope("forward"):
            normed_one, inverse_one = normalize(residual)
            group_normed, _ = normalize(
                group_tokens.astype(jnp.float32).reshape(clips, groups, patches, model_width)
            )
            flat_one = (
                (group_normed * (1.0 + group_mod[:, 1]) + group_mod[:, 0])
                .astype(jnp.bfloat16)
                .reshape(clips, groups * patches, model_width)
            )
            token_count = flat_one.shape[1]
            projected = jnp.einsum(
                "crd,dkh->crkh", flat_one, joint_weight, preferred_element_type=jnp.float32
            ).astype(jnp.bfloat16)
            queries = projected[:, :, 0]
            keys_all = gather_halves(projected[:, :, 1])
            values_all = gather_halves(projected[:, :, 2])
            attended, log_totals = attention_forward(queries[0], keys_all[0], values_all[0])
            attended = attended[None]
            partial_one = jnp.einsum(
                "crh,oh->cro", attended, mixer_weight, preferred_element_type=jnp.float32
            )
            branch_one = scatter_tokens(partial_one)
            middle = residual + gate1 * branch_one
            normed_two, inverse_two = normalize(middle)
            entering_two = (normed_two * (1.0 + scale2) + shift2).astype(jnp.bfloat16)
            flat_two = gather_halves(entering_two)
            blocked_two = flat_two.reshape(clips, -1, replicas, halves * rows_here)
            up_values = jnp.einsum(
                "crad,atdj->crtj", blocked_two, upward_weight, preferred_element_type=jnp.float32
            )
            hidden = gelu_tanh(up_values).astype(jnp.bfloat16)
            partial_two = jnp.einsum(
                "crtj,atdj->crad", hidden, downward_weight, preferred_element_type=jnp.float32
            ).reshape(clips, -1, model_width)
            branch_two = scatter_halves(partial_two)
            output = (middle + gate2 * branch_two).astype(jnp.bfloat16)

        with jax.named_scope("backward_ffn"):
            grad_gate_two = jnp.sum(upstream * branch_two, axis=1)
            grad_two_all = gather_halves((gate2 * upstream).astype(jnp.bfloat16))
            blocked_grad = grad_two_all.reshape(clips, -1, replicas, halves * rows_here)
            grad_hidden = jnp.einsum(
                "crad,atdj->crtj", blocked_grad, downward_weight, preferred_element_type=jnp.float32
            )
            down_total = jnp.einsum(
                "crad,crtj->atdj", blocked_grad, hidden, preferred_element_type=jnp.float32
            )
            _, gelu_pullback = jax.vjp(gelu_tanh, up_values)
            grad_up = gelu_pullback(grad_hidden)[0].astype(jnp.bfloat16)
            up_total = jnp.einsum(
                "crad,crtj->atdj", blocked_two, grad_up, preferred_element_type=jnp.float32
            )
            partial_back_two = jnp.einsum(
                "crtj,atdj->crad", grad_up, upward_weight, preferred_element_type=jnp.float32
            ).reshape(clips, -1, model_width)
            grad_entering_two = scatter_halves(partial_back_two)
            grad_shift_two = jnp.sum(grad_entering_two, axis=1)
            grad_scale_two = jnp.sum(grad_entering_two * normed_two, axis=1)
            grad_middle = upstream + norm_back(
                grad_entering_two * (1.0 + scale2), normed_two, inverse_two
            )
            grad_gate_one = jnp.sum(grad_middle * branch_one, axis=1)

        with jax.named_scope("backward_attention"):
            grad_branch_one = (gate1 * grad_middle).astype(jnp.bfloat16)
            grad_one_all = gather_tokens(grad_branch_one)
            grad_attended = jnp.einsum(
                "cro,oh->crh", grad_one_all, mixer_weight, preferred_element_type=jnp.float32
            ).astype(jnp.bfloat16)
            mixer_total = jnp.einsum(
                "cro,crh->oh", grad_one_all, attended, preferred_element_type=jnp.float32
            )
            query_grads, key_grads, value_grads = attention_backward(
                queries[0], keys_all[0], values_all[0], grad_attended[0], log_totals
            )
            query_grads = query_grads[None]
            key_grads = key_grads[None]
            value_grads = value_grads[None]
            key_own, value_own = (
                scatter_halves(grads.reshape(clips, -1, local_width))
                for grads in (key_grads, value_grads)
            )
            grad_projected = jnp.stack([query_grads, key_own, value_own], axis=2).astype(
                jnp.bfloat16
            )
            joint_total = jnp.einsum(
                "crd,crkh->dkh", flat_one, grad_projected, preferred_element_type=jnp.float32
            )
            partial_back_one = jnp.einsum(
                "crkh,dkh->crd", grad_projected, joint_weight, preferred_element_type=jnp.float32
            )
            grad_entering_one = scatter_tokens(partial_back_one)
            grad_shift_one = jnp.sum(grad_entering_one, axis=1)
            grad_scale_one = jnp.sum(grad_entering_one * normed_one, axis=1)
            grad_input = grad_middle + norm_back(
                grad_entering_one * (1.0 + scale1), normed_one, inverse_one
            )


        grad_modulation = jnp.stack(
            [grad_shift_one, grad_scale_one, grad_gate_one, grad_shift_two, grad_scale_two, grad_gate_two],
            axis=1,
        )
        totals = (joint_total, mixer_total, up_total, down_total)
        return output, grad_input.astype(jnp.bfloat16), grad_modulation, totals

    pieces = [
        clip_pass(
            residual[i : i + 1],
            upstream[i : i + 1],
            modulation[i : i + 1],
            group_tokens[i : i + 1],
            None,
            group_mod[i : i + 1],
        )
        for i in range(clips)
    ]
    output = jnp.concatenate([p[0] for p in pieces], axis=0)
    grad_input_low = jnp.concatenate([p[1] for p in pieces], axis=0)
    grad_modulation = jnp.concatenate([p[2] for p in pieces], axis=0)
    joint_total, mixer_total, up_total, down_total = (
        sum(p[3][k] for p in pieces[1:]) + pieces[0][3][k] for k in range(4)
    )
    with jax.named_scope("ada_grad"):
        grad_columns = lax.all_to_all(
            grad_modulation.reshape(clips, 1, 6, model_width), "tensor", 3, 1, tiled=True
        )
        grad_all = lax.all_gather(grad_columns, ("dp", "frame"), axis=0, tiled=True)
        grad_all = grad_all.reshape(replicas * halves, clips, groups, 6, local_width)
        adaptive_total = jnp.einsum(
            "acgd,acgkw->dkw",
            my_condition.astype(jnp.float32),
            grad_all,
            precision=highest,
        )

    with jax.named_scope("weight_grads"):
        joint_sum, mixer_sum = (
            lax.psum_scatter(
                total.astype(jnp.bfloat16), ("dp", "frame"), scatter_dimension=0, tiled=True
            ).astype(jnp.float32)
            for total in (joint_total, mixer_total)
        )
        up_sum, down_sum = hidden_half_back((up_total, down_total))
        summed = (joint_sum, mixer_sum, up_sum, down_sum)
    result = output[:, None]
    input_grad = grad_input_low[:, None]
    return (result, input_grad, summed[0], summed[1], summed[2], summed[3], adaptive_total)


def solution(mesh):
    return jax.shard_map(
        on_device,
        mesh=mesh,
        in_specs=(
            P("dp", ("frame", "tensor"), None, None),
            P("dp", ("frame", "tensor"), None, None),
            P("dp", "frame"),
            P(("dp", "frame"), None, "tensor"),
            P(("dp", "frame"), "tensor"),
            P(("dp", "frame"), "tensor"),
            P(("dp", "frame"), "tensor"),
            P(("dp", "frame"), None, "tensor"),
        ),
        out_specs=(
            P("dp", ("frame", "tensor"), None, None),
            P("dp", ("frame", "tensor"), None, None),
            P(("dp", "frame"), None, "tensor"),
            P(("dp", "frame"), "tensor"),
            P(("dp", "frame"), "tensor"),
            P(("dp", "frame"), "tensor"),
            P(("dp", "frame"), None, "tensor"),
        ),
        check_vma=False,
    )
```

```python
import functools
import math

import jax
import jax.numpy as jnp
from jax import lax
from jax.experimental import pallas as pl
from jax.experimental.pallas import tpu as pltpu
from jax.sharding import PartitionSpec as P

HEAD_DIM = 64


epsilon = 1e-06
highest = lax.Precision.HIGHEST


def normalize(values):
    center = values - jnp.mean(values, axis=-1, keepdims=True)
    spread = jnp.mean(center * center, axis=-1, keepdims=True)
    inverse = lax.rsqrt(spread + epsilon)
    return (center * inverse, inverse)


def norm_back(upstream, normed, inverse):
    upstream_mean = jnp.mean(upstream, axis=-1, keepdims=True)
    product_mean = jnp.mean(upstream * normed, axis=-1, keepdims=True)
    return inverse * (upstream - upstream_mean - normed * product_mean)


def level_embedding(levels, model_width):
    halfway = model_width // 2
    frequency = jnp.exp(-math.log(10000.0) * jnp.arange(halfway, dtype=jnp.float32) / halfway)
    angles = levels.astype(jnp.float32)[..., None] * frequency
    return jnp.concatenate([jnp.cos(angles), jnp.sin(angles)], axis=-1)


def _nt(a, b):
    return lax.dot_general(a, b, (((1,), (1,)), ((), ())), preferred_element_type=jnp.float32)


def _tn(a, b):
    return lax.dot_general(a, b, (((0,), (0,)), ((), ())), preferred_element_type=jnp.float32)


def _forward_kernel(heads, scaling, q_ref, k_ref, v_ref, o_ref, lse_ref):
    for h in range(heads):
        cols = slice(h * HEAD_DIM, (h + 1) * HEAD_DIM)
        scores = _nt(q_ref[:, cols], k_ref[:, cols]) * scaling
        largest = jnp.max(scores, axis=1, keepdims=True)
        raised = jnp.exp(scores - largest)
        total = jnp.sum(raised, axis=1, keepdims=True)
        probs_low = (raised / total).astype(jnp.bfloat16)
        out = jnp.dot(probs_low, v_ref[:, cols], preferred_element_type=jnp.float32)
        o_ref[:, cols] = out.astype(o_ref.dtype)
        lse_ref[:, h : h + 1] = largest + jnp.log(total)


def _backward_kernel(heads, scaling, q_ref, k_ref, v_ref, g_ref, lse_ref, dq_ref, dk_ref, dv_ref):
    @pl.when(pl.program_id(0) == 0)
    def _():
        dk_ref[...] = jnp.zeros_like(dk_ref)
        dv_ref[...] = jnp.zeros_like(dv_ref)

    for h in range(heads):
        cols = slice(h * HEAD_DIM, (h + 1) * HEAD_DIM)
        q = q_ref[:, cols]
        g = g_ref[:, cols]
        scores = _nt(q, k_ref[:, cols]) * scaling
        probs = jnp.exp(scores - lse_ref[:, h : h + 1])
        grad_probs = _nt(g, v_ref[:, cols])
        dv_ref[:, cols] += _tn(probs.astype(jnp.bfloat16), g)
        row_terms = jnp.sum(probs * grad_probs, axis=1, keepdims=True)
        grad_scores = (probs * (grad_probs - row_terms)).astype(jnp.bfloat16)
        dq_ref[:, cols] = jnp.dot(grad_scores, k_ref[:, cols], preferred_element_type=jnp.float32) * scaling
        dk_ref[:, cols] += _tn(grad_scores, q) * scaling


def attention_forward(queries, keys, values, block_rows=256):
    rows, width = queries.shape
    length = keys.shape[0]
    heads = width // HEAD_DIM
    block_rows = min(block_rows, rows)
    flops = 4 * rows * length * width
    return pl.pallas_call(
        functools.partial(_forward_kernel, heads, HEAD_DIM ** (-0.5)),
        out_shape=(
            jax.ShapeDtypeStruct((rows, width), jnp.bfloat16),
            jax.ShapeDtypeStruct((rows, heads), jnp.float32),
        ),
        grid=(rows // block_rows,),
        in_specs=[
            pl.BlockSpec((block_rows, width), lambda i: (i, 0)),
            pl.BlockSpec((length, width), lambda i: (0, 0)),
            pl.BlockSpec((length, width), lambda i: (0, 0)),
        ],
        out_specs=[
            pl.BlockSpec((block_rows, width), lambda i: (i, 0)),
            pl.BlockSpec((block_rows, heads), lambda i: (i, 0)),
        ],
        compiler_params=pltpu.CompilerParams(
            dimension_semantics=("arbitrary",), vmem_limit_bytes=56 * 1024 * 1024
        ),
        cost_estimate=pl.CostEstimate(
            flops=flops,
            transcendentals=rows * length * heads,
            bytes_accessed=2 * (2 * rows * width + 2 * length * width),
        ),
    )(queries, keys, values)


def attention_backward(queries, keys, values, grad_out, lse, block_rows=256):
    rows, width = queries.shape
    length = keys.shape[0]
    heads = width // HEAD_DIM
    block_rows = min(block_rows, rows)
    flops = 10 * rows * length * width
    return pl.pallas_call(
        functools.partial(_backward_kernel, heads, HEAD_DIM ** (-0.5)),
        out_shape=(
            jax.ShapeDtypeStruct((rows, width), jnp.float32),
            jax.ShapeDtypeStruct((length, width), jnp.float32),
            jax.ShapeDtypeStruct((length, width), jnp.float32),
        ),
        grid=(rows // block_rows,),
        in_specs=[
            pl.BlockSpec((block_rows, width), lambda i: (i, 0)),
            pl.BlockSpec((length, width), lambda i: (0, 0)),
            pl.BlockSpec((length, width), lambda i: (0, 0)),
            pl.BlockSpec((block_rows, width), lambda i: (i, 0)),
            pl.BlockSpec((block_rows, heads), lambda i: (i, 0)),
        ],
        out_specs=[
            pl.BlockSpec((block_rows, width), lambda i: (i, 0)),
            pl.BlockSpec((length, width), lambda i: (0, 0)),
            pl.BlockSpec((length, width), lambda i: (0, 0)),
        ],
        compiler_params=pltpu.CompilerParams(
            dimension_semantics=("arbitrary",), vmem_limit_bytes=56 * 1024 * 1024
        ),
        cost_estimate=pl.CostEstimate(
            flops=flops,
            transcendentals=rows * length * heads,
            bytes_accessed=2 * (3 * rows * width + 2 * length * width) + 4 * (rows + 2 * length) * width,
        ),
    )(queries, keys, values, grad_out, lse)


def gelu_tanh(values):
    return jax.nn.gelu(values, approximate=True)


def on_device(
    tokens, out_grad, noise_index, qkv_weight, out_weight, up_weight, down_weight, ada_weight
):
    clips = tokens.shape[0]
    patches = tokens.shape[2]
    model_width = tokens.shape[-1]
    local_width = qkv_weight.shape[2]
    rows_here = qkv_weight.shape[0]
    heads_here = local_width // HEAD_DIM
    scaling = HEAD_DIM ** (-0.5)
    groups = lax.axis_size("tensor")
    halves = lax.axis_size("frame")
    replicas = lax.axis_size("dp")

    with jax.named_scope("modulation"):
        ada_rows = lax.all_gather(ada_weight, ("dp", "frame"), axis=0, tiled=True)
        local_condition = jax.nn.silu(level_embedding(noise_index, model_width)).astype(
            jnp.bfloat16
        )
        local_mod = jnp.einsum(
            "cgd,dkw->cgkw", local_condition, ada_rows, preferred_element_type=jnp.float32
        )
        group_mod = lax.all_gather(local_mod, "tensor", axis=3, tiled=True)
        group_mod = jnp.swapaxes(group_mod, 1, 2)[:, :, :, None, :]
        group_index = lax.axis_index("tensor")
        modulation = lax.dynamic_index_in_dim(group_mod, group_index, axis=2, keepdims=False)

    frame_index = lax.axis_index("frame")

    def order_by_half(mine, other):
        both = jnp.stack([mine, other])
        return jnp.where(frame_index == 0, both, both[::-1])

    def hidden_half(weights):
        half = weights[0].shape[1] // halves
        pieces = []
        for weight in weights:
            blocks = weight.reshape(rows_here, halves, half)
            mine = jnp.take(blocks, frame_index, axis=1)
            sent = jnp.take(blocks, 1 - frame_index, axis=1)
            received = lax.ppermute(sent, "frame", [(0, 1), (1, 0)])
            pieces.append(order_by_half(mine, received).reshape(halves * rows_here, half))
        joined = jnp.concatenate(pieces, axis=0)
        gathered = lax.all_gather(joined, "tensor", axis=0, tiled=True)
        gathered = lax.all_gather(gathered, "dp", axis=0, tiled=True)
        gathered = gathered.reshape(replicas, groups, len(weights), halves * rows_here, half)
        return tuple(gathered[:, :, k] for k in range(len(weights)))

    def hidden_half_back(totals):
        half = totals[0].shape[-1]
        blocks = jnp.concatenate(totals, axis=2).astype(jnp.bfloat16)
        blocks = blocks.reshape(replicas * groups, len(totals) * halves * rows_here, half)
        summed = lax.psum_scatter(blocks, "dp", scatter_dimension=0, tiled=True)
        summed = lax.psum_scatter(summed, "tensor", scatter_dimension=0, tiled=True)
        summed = summed.reshape(len(totals), halves, rows_here, half)
        mine = jnp.take(summed, frame_index, axis=1).astype(jnp.float32)
        sent = jnp.take(summed, 1 - frame_index, axis=1)
        received = lax.ppermute(sent, "frame", [(0, 1), (1, 0)]).astype(jnp.float32)
        both = jnp.stack([mine, received], axis=1)
        ordered = jnp.where(frame_index == 0, both, both[:, ::-1])
        return tuple(
            jnp.swapaxes(ordered[k], 0, 1).reshape(rows_here, halves * half)
            for k in range(len(totals))
        )

    with jax.named_scope("weights"):
        joint_weight, mixer_weight = (
            lax.all_gather(w, ("dp", "frame"), axis=0, tiled=True)
            for w in (qkv_weight, out_weight)
        )

    residual = tokens[:, 0].astype(jnp.float32)
    upstream = out_grad[:, 0].astype(jnp.float32)
    with jax.named_scope("group_inputs"):
        group_tokens = lax.all_gather(tokens[:, 0], "tensor", axis=1, tiled=True)
        group_upstream = None
    with jax.named_scope("ffn_weights"):
        group_tokens, joint_weight, mixer_weight, ffn_shards = lax.optimization_barrier(
            (group_tokens, joint_weight, mixer_weight, (up_weight, down_weight))
        )
        upward_weight, downward_weight = hidden_half(ffn_shards)
    def gather_halves(values):
        if halves != 2:
            return lax.all_gather(values, "frame", axis=1, tiled=True)
        other = lax.ppermute(values, "frame", [(0, 1), (1, 0)])
        return jnp.concatenate([values, other], axis=1)

    def scatter_halves(values):
        if halves != 2:
            return lax.psum_scatter(
                values.astype(jnp.bfloat16), "frame", scatter_dimension=1, tiled=True
            ).astype(jnp.float32)
        count = values.shape[1] // 2
        mine = values[:, :count]
        other = lax.ppermute(values[:, count:].astype(jnp.bfloat16), "frame", [(0, 1), (1, 0)])
        return mine.astype(jnp.bfloat16).astype(jnp.float32) + other.astype(jnp.float32)

    def clip_pass(residual, upstream, modulation, group_tokens, group_upstream, group_mod):
        clips = residual.shape[0]
        patches = residual.shape[1]
        shift1, scale1, gate1 = modulation[:, 0], modulation[:, 1], modulation[:, 2]
        shift2, scale2, gate2 = modulation[:, 3], modulation[:, 4], modulation[:, 5]
        def gather_tokens(values):
            return lax.all_gather(values, "tensor", axis=1, tiled=True)

        def scatter_tokens(values):
            parts = values.astype(jnp.bfloat16).reshape(
                values.shape[0], groups, -1, values.shape[-1]
            )
            received = lax.all_to_all(parts, "tensor", 1, 1, tiled=True)
            return jnp.sum(received.astype(jnp.float32), axis=1)

        with jax.named_scope("forward"):
            normed_one, inverse_one = normalize(residual)
            group_normed, _ = normalize(
                group_tokens.astype(jnp.float32).reshape(clips, groups, patches, model_width)
            )
            flat_one = (
                (group_normed * (1.0 + group_mod[:, 1]) + group_mod[:, 0])
                .astype(jnp.bfloat16)
                .reshape(clips, groups * patches, model_width)
            )
            token_count = flat_one.shape[1]
            projected = jnp.einsum(
                "crd,dkh->crkh", flat_one, joint_weight, preferred_element_type=jnp.float32
            ).astype(jnp.bfloat16)
            queries = projected[:, :, 0]
            keys_all = gather_halves(projected[:, :, 1])
            values_all = gather_halves(projected[:, :, 2])
            attended, log_totals = attention_forward(queries[0], keys_all[0], values_all[0])
            attended = attended[None]
            partial_one = jnp.einsum(
                "crh,oh->cro", attended, mixer_weight, preferred_element_type=jnp.float32
            )
            branch_one = scatter_tokens(partial_one)
            middle = residual + gate1 * branch_one
            normed_two, inverse_two = normalize(middle)
            entering_two = (normed_two * (1.0 + scale2) + shift2).astype(jnp.bfloat16)
            flat_two = gather_halves(entering_two)
            blocked_two = flat_two.reshape(clips, -1, replicas, halves * rows_here)
            up_values = jnp.einsum(
                "crad,atdj->crtj", blocked_two, upward_weight, preferred_element_type=jnp.float32
            )
            hidden = gelu_tanh(up_values).astype(jnp.bfloat16)
            partial_two = jnp.einsum(
                "crtj,atdj->crad", hidden, downward_weight, preferred_element_type=jnp.float32
            ).reshape(clips, -1, model_width)
            branch_two = scatter_halves(partial_two)
            output = (middle + gate2 * branch_two).astype(jnp.bfloat16)

        with jax.named_scope("backward_ffn"):
            grad_gate_two = jnp.sum(upstream * branch_two, axis=1)
            grad_two_all = gather_halves((gate2 * upstream).astype(jnp.bfloat16))
            blocked_grad = grad_two_all.reshape(clips, -1, replicas, halves * rows_here)
            grad_hidden = jnp.einsum(
                "crad,atdj->crtj", blocked_grad, downward_weight, preferred_element_type=jnp.float32
            )
            down_total = jnp.einsum(
                "crad,crtj->atdj", blocked_grad, hidden, preferred_element_type=jnp.float32
            )
            _, gelu_pullback = jax.vjp(gelu_tanh, up_values)
            grad_up = gelu_pullback(grad_hidden)[0].astype(jnp.bfloat16)
            up_total = jnp.einsum(
                "crad,crtj->atdj", blocked_two, grad_up, preferred_element_type=jnp.float32
            )
            partial_back_two = jnp.einsum(
                "crtj,atdj->crad", grad_up, upward_weight, preferred_element_type=jnp.float32
            ).reshape(clips, -1, model_width)
            grad_entering_two = scatter_halves(partial_back_two)
            grad_shift_two = jnp.sum(grad_entering_two, axis=1)
            grad_scale_two = jnp.sum(grad_entering_two * normed_two, axis=1)
            grad_middle = upstream + norm_back(
                grad_entering_two * (1.0 + scale2), normed_two, inverse_two
            )
            grad_gate_one = jnp.sum(grad_middle * branch_one, axis=1)

        with jax.named_scope("backward_attention"):
            grad_branch_one = (gate1 * grad_middle).astype(jnp.bfloat16)
            grad_one_all = gather_tokens(grad_branch_one)
            grad_attended = jnp.einsum(
                "cro,oh->crh", grad_one_all, mixer_weight, preferred_element_type=jnp.float32
            ).astype(jnp.bfloat16)
            mixer_total = jnp.einsum(
                "cro,crh->oh", grad_one_all, attended, preferred_element_type=jnp.float32
            )
            query_grads, key_grads, value_grads = attention_backward(
                queries[0], keys_all[0], values_all[0], grad_attended[0], log_totals
            )
            query_grads = query_grads[None]
            key_grads = key_grads[None]
            value_grads = value_grads[None]
            key_own, value_own = (
                scatter_halves(grads.reshape(clips, -1, local_width))
                for grads in (key_grads, value_grads)
            )
            grad_projected = jnp.stack([query_grads, key_own, value_own], axis=2).astype(
                jnp.bfloat16
            )
            joint_total = jnp.einsum(
                "crd,crkh->dkh", flat_one, grad_projected, preferred_element_type=jnp.float32
            )
            partial_back_one = jnp.einsum(
                "crkh,dkh->crd", grad_projected, joint_weight, preferred_element_type=jnp.float32
            )
            grad_entering_one = scatter_tokens(partial_back_one)
            grad_shift_one = jnp.sum(grad_entering_one, axis=1)
            grad_scale_one = jnp.sum(grad_entering_one * normed_one, axis=1)
            grad_input = grad_middle + norm_back(
                grad_entering_one * (1.0 + scale1), normed_one, inverse_one
            )


        grad_modulation = jnp.stack(
            [grad_shift_one, grad_scale_one, grad_gate_one, grad_shift_two, grad_scale_two, grad_gate_two],
            axis=1,
        )
        totals = (joint_total, mixer_total, up_total, down_total)
        return output, grad_input.astype(jnp.bfloat16), grad_modulation, totals

    pieces = [
        clip_pass(
            residual[i : i + 1],
            upstream[i : i + 1],
            modulation[i : i + 1],
            group_tokens[i : i + 1],
            None,
            group_mod[i : i + 1],
        )
        for i in range(clips)
    ]
    output = jnp.concatenate([p[0] for p in pieces], axis=0)
    grad_input_low = jnp.concatenate([p[1] for p in pieces], axis=0)
    grad_modulation = jnp.concatenate([p[2] for p in pieces], axis=0)
    joint_total, mixer_total, up_total, down_total = (
        sum(p[3][k] for p in pieces[1:]) + pieces[0][3][k] for k in range(4)
    )
    with jax.named_scope("ada_grad"):
        levels_all = lax.all_gather(noise_index, ("dp", "frame"), axis=0, tiled=True)
        levels_all = levels_all.reshape(replicas * halves, clips, groups)
        condition_all = jax.nn.silu(level_embedding(levels_all, model_width)).astype(jnp.bfloat16)
        row_block = lax.axis_index("dp") * halves + lax.axis_index("frame")
        my_condition = lax.dynamic_slice_in_dim(
            condition_all, row_block * rows_here, rows_here, axis=3
        )
        grad_columns = lax.all_to_all(
            grad_modulation.reshape(clips, 1, 6, model_width), "tensor", 3, 1, tiled=True
        )
        grad_all = lax.all_gather(grad_columns, ("dp", "frame"), axis=0, tiled=True)
        grad_all = grad_all.reshape(replicas * halves, clips, groups, 6, local_width)
        adaptive_total = jnp.einsum(
            "acgd,acgkw->dkw",
            my_condition.astype(jnp.float32),
            grad_all,
            precision=highest,
        )

    with jax.named_scope("weight_grads"):
        up_sum, down_sum = hidden_half_back((up_total, down_total))
        joint_total, mixer_total, up_sum, down_sum = lax.optimization_barrier(
            (joint_total, mixer_total, up_sum, down_sum)
        )
        joint_sum, mixer_sum = (
            lax.psum_scatter(
                total.astype(jnp.bfloat16), ("dp", "frame"), scatter_dimension=0, tiled=True
            ).astype(jnp.float32)
            for total in (joint_total, mixer_total)
        )
        summed = (joint_sum, mixer_sum, up_sum, down_sum)
    result = output[:, None]
    input_grad = grad_input_low[:, None]
    return (result, input_grad, summed[0], summed[1], summed[2], summed[3], adaptive_total)


def solution(mesh):
    return jax.shard_map(
        on_device,
        mesh=mesh,
        in_specs=(
            P("dp", ("frame", "tensor"), None, None),
            P("dp", ("frame", "tensor"), None, None),
            P("dp", "frame"),
            P(("dp", "frame"), None, "tensor"),
            P(("dp", "frame"), "tensor"),
            P(("dp", "frame"), "tensor"),
            P(("dp", "frame"), "tensor"),
            P(("dp", "frame"), None, "tensor"),
        ),
        out_specs=(
            P("dp", ("frame", "tensor"), None, None),
            P("dp", ("frame", "tensor"), None, None),
            P(("dp", "frame"), None, "tensor"),
            P(("dp", "frame"), "tensor"),
            P(("dp", "frame"), "tensor"),
            P(("dp", "frame"), "tensor"),
            P(("dp", "frame"), None, "tensor"),
        ),
        check_vma=False,
    )
```

```python
import functools
import math

import jax
import jax.numpy as jnp
from jax import lax
from jax.experimental import pallas as pl
from jax.experimental.pallas import tpu as pltpu
from jax.sharding import PartitionSpec as P

HEAD_DIM = 64


epsilon = 1e-06
highest = lax.Precision.HIGHEST


def normalize(values):
    center = values - jnp.mean(values, axis=-1, keepdims=True)
    spread = jnp.mean(center * center, axis=-1, keepdims=True)
    inverse = lax.rsqrt(spread + epsilon)
    return (center * inverse, inverse)


def norm_back(upstream, normed, inverse):
    upstream_mean = jnp.mean(upstream, axis=-1, keepdims=True)
    product_mean = jnp.mean(upstream * normed, axis=-1, keepdims=True)
    return inverse * (upstream - upstream_mean - normed * product_mean)


def level_embedding(levels, model_width):
    halfway = model_width // 2
    frequency = jnp.exp(-math.log(10000.0) * jnp.arange(halfway, dtype=jnp.float32) / halfway)
    angles = levels.astype(jnp.float32)[..., None] * frequency
    return jnp.concatenate([jnp.cos(angles), jnp.sin(angles)], axis=-1)


def _nt(a, b):
    return lax.dot_general(a, b, (((1,), (1,)), ((), ())), preferred_element_type=jnp.float32)


def _tn(a, b):
    return lax.dot_general(a, b, (((0,), (0,)), ((), ())), preferred_element_type=jnp.float32)


def _forward_kernel(heads, scaling, q_ref, k_ref, v_ref, o_ref, lse_ref):
    for h in range(heads):
        cols = slice(h * HEAD_DIM, (h + 1) * HEAD_DIM)
        scores = _nt(q_ref[:, cols], k_ref[:, cols]) * scaling
        largest = jnp.max(scores, axis=1, keepdims=True)
        raised = jnp.exp(scores - largest)
        total = jnp.sum(raised, axis=1, keepdims=True)
        probs_low = (raised / total).astype(jnp.bfloat16)
        out = jnp.dot(probs_low, v_ref[:, cols], preferred_element_type=jnp.float32)
        o_ref[:, cols] = out.astype(o_ref.dtype)
        lse_ref[:, h : h + 1] = largest + jnp.log(total)


def _backward_kernel(heads, scaling, q_ref, k_ref, v_ref, g_ref, lse_ref, dq_ref, dk_ref, dv_ref):
    @pl.when(pl.program_id(0) == 0)
    def _():
        dk_ref[...] = jnp.zeros_like(dk_ref)
        dv_ref[...] = jnp.zeros_like(dv_ref)

    for h in range(heads):
        cols = slice(h * HEAD_DIM, (h + 1) * HEAD_DIM)
        q = q_ref[:, cols]
        g = g_ref[:, cols]
        scores = _nt(q, k_ref[:, cols]) * scaling
        probs = jnp.exp(scores - lse_ref[:, h : h + 1])
        grad_probs = _nt(g, v_ref[:, cols])
        dv_ref[:, cols] += _tn(probs.astype(jnp.bfloat16), g)
        row_terms = jnp.sum(probs * grad_probs, axis=1, keepdims=True)
        grad_scores = (probs * (grad_probs - row_terms)).astype(jnp.bfloat16)
        dq_ref[:, cols] = jnp.dot(grad_scores, k_ref[:, cols], preferred_element_type=jnp.float32) * scaling
        dk_ref[:, cols] += _tn(grad_scores, q) * scaling


def attention_forward(queries, keys, values, block_rows=256):
    rows, width = queries.shape
    length = keys.shape[0]
    heads = width // HEAD_DIM
    block_rows = min(block_rows, rows)
    flops = 4 * rows * length * width
    return pl.pallas_call(
        functools.partial(_forward_kernel, heads, HEAD_DIM ** (-0.5)),
        out_shape=(
            jax.ShapeDtypeStruct((rows, width), jnp.bfloat16),
            jax.ShapeDtypeStruct((rows, heads), jnp.float32),
        ),
        grid=(rows // block_rows,),
        in_specs=[
            pl.BlockSpec((block_rows, width), lambda i: (i, 0)),
            pl.BlockSpec((length, width), lambda i: (0, 0)),
            pl.BlockSpec((length, width), lambda i: (0, 0)),
        ],
        out_specs=[
            pl.BlockSpec((block_rows, width), lambda i: (i, 0)),
            pl.BlockSpec((block_rows, heads), lambda i: (i, 0)),
        ],
        compiler_params=pltpu.CompilerParams(
            dimension_semantics=("arbitrary",), vmem_limit_bytes=56 * 1024 * 1024
        ),
        cost_estimate=pl.CostEstimate(
            flops=flops,
            transcendentals=rows * length * heads,
            bytes_accessed=2 * (2 * rows * width + 2 * length * width),
        ),
    )(queries, keys, values)


def attention_backward(queries, keys, values, grad_out, lse, block_rows=256):
    rows, width = queries.shape
    length = keys.shape[0]
    heads = width // HEAD_DIM
    block_rows = min(block_rows, rows)
    flops = 10 * rows * length * width
    return pl.pallas_call(
        functools.partial(_backward_kernel, heads, HEAD_DIM ** (-0.5)),
        out_shape=(
            jax.ShapeDtypeStruct((rows, width), jnp.float32),
            jax.ShapeDtypeStruct((length, width), jnp.float32),
            jax.ShapeDtypeStruct((length, width), jnp.float32),
        ),
        grid=(rows // block_rows,),
        in_specs=[
            pl.BlockSpec((block_rows, width), lambda i: (i, 0)),
            pl.BlockSpec((length, width), lambda i: (0, 0)),
            pl.BlockSpec((length, width), lambda i: (0, 0)),
            pl.BlockSpec((block_rows, width), lambda i: (i, 0)),
            pl.BlockSpec((block_rows, heads), lambda i: (i, 0)),
        ],
        out_specs=[
            pl.BlockSpec((block_rows, width), lambda i: (i, 0)),
            pl.BlockSpec((length, width), lambda i: (0, 0)),
            pl.BlockSpec((length, width), lambda i: (0, 0)),
        ],
        compiler_params=pltpu.CompilerParams(
            dimension_semantics=("arbitrary",), vmem_limit_bytes=56 * 1024 * 1024
        ),
        cost_estimate=pl.CostEstimate(
            flops=flops,
            transcendentals=rows * length * heads,
            bytes_accessed=2 * (3 * rows * width + 2 * length * width) + 4 * (rows + 2 * length) * width,
        ),
    )(queries, keys, values, grad_out, lse)


def gelu_tanh(values):
    return jax.nn.gelu(values, approximate=True)


def on_device(
    tokens, out_grad, noise_index, qkv_weight, out_weight, up_weight, down_weight, ada_weight
):
    clips = tokens.shape[0]
    patches = tokens.shape[2]
    model_width = tokens.shape[-1]
    local_width = qkv_weight.shape[2]
    rows_here = qkv_weight.shape[0]
    heads_here = local_width // HEAD_DIM
    scaling = HEAD_DIM ** (-0.5)
    groups = lax.axis_size("tensor")
    halves = lax.axis_size("frame")
    replicas = lax.axis_size("dp")

    with jax.named_scope("modulation"):
        ada_rows = lax.all_gather(ada_weight, ("dp", "frame"), axis=0, tiled=True)
        token_input, ada_rows = lax.optimization_barrier((tokens[:, 0], ada_rows))
        group_tokens = lax.all_gather(token_input, "tensor", axis=1, tiled=True)
        group_tokens, qkv_input, out_input = lax.optimization_barrier(
            (group_tokens, qkv_weight, out_weight)
        )
        local_condition = jax.nn.silu(level_embedding(noise_index, model_width)).astype(
            jnp.bfloat16
        )
        local_mod = jnp.einsum(
            "cgd,dkw->cgkw", local_condition, ada_rows, preferred_element_type=jnp.float32
        )
        group_mod = lax.all_gather(local_mod, "tensor", axis=3, tiled=True)
        group_mod = jnp.swapaxes(group_mod, 1, 2)[:, :, :, None, :]
        group_index = lax.axis_index("tensor")
        modulation = lax.dynamic_index_in_dim(group_mod, group_index, axis=2, keepdims=False)

    frame_index = lax.axis_index("frame")

    def order_by_half(mine, other):
        both = jnp.stack([mine, other])
        return jnp.where(frame_index == 0, both, both[::-1])

    def hidden_half(weights):
        half = weights[0].shape[1] // halves
        pieces = []
        for weight in weights:
            blocks = weight.reshape(rows_here, halves, half)
            mine = jnp.take(blocks, frame_index, axis=1)
            sent = jnp.take(blocks, 1 - frame_index, axis=1)
            received = lax.ppermute(sent, "frame", [(0, 1), (1, 0)])
            pieces.append(order_by_half(mine, received).reshape(halves * rows_here, half))
        joined = jnp.concatenate(pieces, axis=0)
        gathered = lax.all_gather(joined, "tensor", axis=0, tiled=True)
        gathered = lax.all_gather(gathered, "dp", axis=0, tiled=True)
        gathered = gathered.reshape(replicas, groups, len(weights), halves * rows_here, half)
        return tuple(gathered[:, :, k] for k in range(len(weights)))

    def hidden_half_back(totals):
        half = totals[0].shape[-1]
        blocks = jnp.concatenate(totals, axis=2).astype(jnp.bfloat16)
        blocks = blocks.reshape(replicas * groups, len(totals) * halves * rows_here, half)
        summed = lax.psum_scatter(blocks, "dp", scatter_dimension=0, tiled=True)
        summed = lax.psum_scatter(summed, "tensor", scatter_dimension=0, tiled=True)
        summed = summed.reshape(len(totals), halves, rows_here, half)
        mine = jnp.take(summed, frame_index, axis=1).astype(jnp.float32)
        sent = jnp.take(summed, 1 - frame_index, axis=1)
        received = lax.ppermute(sent, "frame", [(0, 1), (1, 0)]).astype(jnp.float32)
        both = jnp.stack([mine, received], axis=1)
        ordered = jnp.where(frame_index == 0, both, both[:, ::-1])
        return tuple(
            jnp.swapaxes(ordered[k], 0, 1).reshape(rows_here, halves * half)
            for k in range(len(totals))
        )

    with jax.named_scope("weights"):
        joint_weight, mixer_weight = (
            lax.all_gather(w, ("dp", "frame"), axis=0, tiled=True)
            for w in (qkv_input, out_input)
        )
        joint_weight, mixer_weight, ffn_shards = lax.optimization_barrier(
            (joint_weight, mixer_weight, (up_weight, down_weight))
        )
        upward_weight, downward_weight = hidden_half(ffn_shards)

    residual = tokens[:, 0].astype(jnp.float32)
    upstream = out_grad[:, 0].astype(jnp.float32)
    with jax.named_scope("group_inputs"):
        group_upstream = None
    def gather_halves(values):
        if halves != 2:
            return lax.all_gather(values, "frame", axis=1, tiled=True)
        other = lax.ppermute(values, "frame", [(0, 1), (1, 0)])
        return jnp.concatenate([values, other], axis=1)

    def scatter_halves(values):
        if halves != 2:
            return lax.psum_scatter(
                values.astype(jnp.bfloat16), "frame", scatter_dimension=1, tiled=True
            ).astype(jnp.float32)
        count = values.shape[1] // 2
        mine = values[:, :count]
        other = lax.ppermute(values[:, count:].astype(jnp.bfloat16), "frame", [(0, 1), (1, 0)])
        return mine.astype(jnp.bfloat16).astype(jnp.float32) + other.astype(jnp.float32)

    def clip_pass(residual, upstream, modulation, group_tokens, group_upstream, group_mod):
        clips = residual.shape[0]
        patches = residual.shape[1]
        shift1, scale1, gate1 = modulation[:, 0], modulation[:, 1], modulation[:, 2]
        shift2, scale2, gate2 = modulation[:, 3], modulation[:, 4], modulation[:, 5]
        def gather_tokens(values):
            return lax.all_gather(values, "tensor", axis=1, tiled=True)

        def scatter_tokens(values):
            parts = values.astype(jnp.bfloat16).reshape(
                values.shape[0], groups, -1, values.shape[-1]
            )
            received = lax.all_to_all(parts, "tensor", 1, 1, tiled=True)
            return jnp.sum(received.astype(jnp.float32), axis=1)

        with jax.named_scope("forward"):
            normed_one, inverse_one = normalize(residual)
            group_normed, _ = normalize(
                group_tokens.astype(jnp.float32).reshape(clips, groups, patches, model_width)
            )
            flat_one = (
                (group_normed * (1.0 + group_mod[:, 1]) + group_mod[:, 0])
                .astype(jnp.bfloat16)
                .reshape(clips, groups * patches, model_width)
            )
            token_count = flat_one.shape[1]
            projected = jnp.einsum(
                "crd,dkh->crkh", flat_one, joint_weight, preferred_element_type=jnp.float32
            ).astype(jnp.bfloat16)
            queries = projected[:, :, 0]
            keys_all = gather_halves(projected[:, :, 1])
            values_all = gather_halves(projected[:, :, 2])
            attended, log_totals = attention_forward(queries[0], keys_all[0], values_all[0])
            attended = attended[None]
            partial_one = jnp.einsum(
                "crh,oh->cro", attended, mixer_weight, preferred_element_type=jnp.float32
            )
            branch_one = scatter_tokens(partial_one)
            middle = residual + gate1 * branch_one
            normed_two, inverse_two = normalize(middle)
            entering_two = (normed_two * (1.0 + scale2) + shift2).astype(jnp.bfloat16)
            flat_two = gather_halves(entering_two)
            blocked_two = flat_two.reshape(clips, -1, replicas, halves * rows_here)
            up_values = jnp.einsum(
                "crad,atdj->crtj", blocked_two, upward_weight, preferred_element_type=jnp.float32
            )
            hidden = gelu_tanh(up_values).astype(jnp.bfloat16)
            partial_two = jnp.einsum(
                "crtj,atdj->crad", hidden, downward_weight, preferred_element_type=jnp.float32
            ).reshape(clips, -1, model_width)
            branch_two = scatter_halves(partial_two)
            output = (middle + gate2 * branch_two).astype(jnp.bfloat16)

        with jax.named_scope("backward_ffn"):
            grad_gate_two = jnp.sum(upstream * branch_two, axis=1)
            grad_two_all = gather_halves((gate2 * upstream).astype(jnp.bfloat16))
            blocked_grad = grad_two_all.reshape(clips, -1, replicas, halves * rows_here)
            grad_hidden = jnp.einsum(
                "crad,atdj->crtj", blocked_grad, downward_weight, preferred_element_type=jnp.float32
            )
            down_total = jnp.einsum(
                "crad,crtj->atdj", blocked_grad, hidden, preferred_element_type=jnp.float32
            )
            _, gelu_pullback = jax.vjp(gelu_tanh, up_values)
            grad_up = gelu_pullback(grad_hidden)[0].astype(jnp.bfloat16)
            up_total = jnp.einsum(
                "crad,crtj->atdj", blocked_two, grad_up, preferred_element_type=jnp.float32
            )
            partial_back_two = jnp.einsum(
                "crtj,atdj->crad", grad_up, upward_weight, preferred_element_type=jnp.float32
            ).reshape(clips, -1, model_width)
            grad_entering_two = scatter_halves(partial_back_two)
            grad_shift_two = jnp.sum(grad_entering_two, axis=1)
            grad_scale_two = jnp.sum(grad_entering_two * normed_two, axis=1)
            grad_middle = upstream + norm_back(
                grad_entering_two * (1.0 + scale2), normed_two, inverse_two
            )
            grad_gate_one = jnp.sum(grad_middle * branch_one, axis=1)

        with jax.named_scope("backward_attention"):
            grad_branch_one = (gate1 * grad_middle).astype(jnp.bfloat16)
            grad_one_all = gather_tokens(grad_branch_one)
            grad_attended = jnp.einsum(
                "cro,oh->crh", grad_one_all, mixer_weight, preferred_element_type=jnp.float32
            ).astype(jnp.bfloat16)
            mixer_total = jnp.einsum(
                "cro,crh->oh", grad_one_all, attended, preferred_element_type=jnp.float32
            )
            query_grads, key_grads, value_grads = attention_backward(
                queries[0], keys_all[0], values_all[0], grad_attended[0], log_totals
            )
            query_grads = query_grads[None]
            key_grads = key_grads[None]
            value_grads = value_grads[None]
            key_own, value_own = (
                scatter_halves(grads.reshape(clips, -1, local_width))
                for grads in (key_grads, value_grads)
            )
            grad_projected = jnp.stack([query_grads, key_own, value_own], axis=2).astype(
                jnp.bfloat16
            )
            joint_total = jnp.einsum(
                "crd,crkh->dkh", flat_one, grad_projected, preferred_element_type=jnp.float32
            )
            partial_back_one = jnp.einsum(
                "crkh,dkh->crd", grad_projected, joint_weight, preferred_element_type=jnp.float32
            )
            grad_entering_one = scatter_tokens(partial_back_one)
            grad_shift_one = jnp.sum(grad_entering_one, axis=1)
            grad_scale_one = jnp.sum(grad_entering_one * normed_one, axis=1)
            grad_input = grad_middle + norm_back(
                grad_entering_one * (1.0 + scale1), normed_one, inverse_one
            )


        grad_modulation = jnp.stack(
            [grad_shift_one, grad_scale_one, grad_gate_one, grad_shift_two, grad_scale_two, grad_gate_two],
            axis=1,
        )
        totals = (joint_total, mixer_total, up_total, down_total)
        return output, grad_input.astype(jnp.bfloat16), grad_modulation, totals

    pieces = [
        clip_pass(
            residual[i : i + 1],
            upstream[i : i + 1],
            modulation[i : i + 1],
            group_tokens[i : i + 1],
            None,
            group_mod[i : i + 1],
        )
        for i in range(clips)
    ]
    output = jnp.concatenate([p[0] for p in pieces], axis=0)
    grad_input_low = jnp.concatenate([p[1] for p in pieces], axis=0)
    grad_modulation = jnp.concatenate([p[2] for p in pieces], axis=0)
    joint_total, mixer_total, up_total, down_total = (
        sum(p[3][k] for p in pieces[1:]) + pieces[0][3][k] for k in range(4)
    )
    with jax.named_scope("ada_grad"):
        levels_all = lax.all_gather(noise_index, ("dp", "frame"), axis=0, tiled=True)
        levels_all = levels_all.reshape(replicas * halves, clips, groups)
        condition_all = jax.nn.silu(level_embedding(levels_all, model_width)).astype(jnp.bfloat16)
        row_block = lax.axis_index("dp") * halves + lax.axis_index("frame")
        my_condition = lax.dynamic_slice_in_dim(
            condition_all, row_block * rows_here, rows_here, axis=3
        )
        grad_columns = lax.all_to_all(
            grad_modulation.reshape(clips, 1, 6, model_width), "tensor", 3, 1, tiled=True
        )
        grad_all = lax.all_gather(grad_columns, ("dp", "frame"), axis=0, tiled=True)
        grad_all = grad_all.reshape(replicas * halves, clips, groups, 6, local_width)
        adaptive_total = jnp.einsum(
            "acgd,acgkw->dkw",
            my_condition.astype(jnp.float32),
            grad_all,
            precision=highest,
        )

    with jax.named_scope("weight_grads"):
        joint_sum, mixer_sum = (
            lax.psum_scatter(
                total.astype(jnp.bfloat16), ("dp", "frame"), scatter_dimension=0, tiled=True
            ).astype(jnp.float32)
            for total in (joint_total, mixer_total)
        )
        up_sum, down_sum = hidden_half_back((up_total, down_total))
        summed = (joint_sum, mixer_sum, up_sum, down_sum)
    result = output[:, None]
    input_grad = grad_input_low[:, None]
    return (result, input_grad, summed[0], summed[1], summed[2], summed[3], adaptive_total)


def solution(mesh):
    return jax.shard_map(
        on_device,
        mesh=mesh,
        in_specs=(
            P("dp", ("frame", "tensor"), None, None),
            P("dp", ("frame", "tensor"), None, None),
            P("dp", "frame"),
            P(("dp", "frame"), None, "tensor"),
            P(("dp", "frame"), "tensor"),
            P(("dp", "frame"), "tensor"),
            P(("dp", "frame"), "tensor"),
            P(("dp", "frame"), None, "tensor"),
        ),
        out_specs=(
            P("dp", ("frame", "tensor"), None, None),
            P("dp", ("frame", "tensor"), None, None),
            P(("dp", "frame"), None, "tensor"),
            P(("dp", "frame"), "tensor"),
            P(("dp", "frame"), "tensor"),
            P(("dp", "frame"), "tensor"),
            P(("dp", "frame"), None, "tensor"),
        ),
        check_vma=False,
    )
```

```python
import functools
import math

import jax
import jax.numpy as jnp
from jax import lax
from jax.experimental import pallas as pl
from jax.experimental.pallas import tpu as pltpu
from jax.sharding import PartitionSpec as P

HEAD_DIM = 64


epsilon = 1e-06
highest = lax.Precision.HIGHEST


def normalize(values):
    center = values - jnp.mean(values, axis=-1, keepdims=True)
    spread = jnp.mean(center * center, axis=-1, keepdims=True)
    inverse = lax.rsqrt(spread + epsilon)
    return (center * inverse, inverse)


def norm_back(upstream, normed, inverse):
    upstream_mean = jnp.mean(upstream, axis=-1, keepdims=True)
    product_mean = jnp.mean(upstream * normed, axis=-1, keepdims=True)
    return inverse * (upstream - upstream_mean - normed * product_mean)


def level_embedding(levels, model_width):
    halfway = model_width // 2
    frequency = jnp.exp(-math.log(10000.0) * jnp.arange(halfway, dtype=jnp.float32) / halfway)
    angles = levels.astype(jnp.float32)[..., None] * frequency
    return jnp.concatenate([jnp.cos(angles), jnp.sin(angles)], axis=-1)


def _nt(a, b):
    return lax.dot_general(a, b, (((1,), (1,)), ((), ())), preferred_element_type=jnp.float32)


def _tn(a, b):
    return lax.dot_general(a, b, (((0,), (0,)), ((), ())), preferred_element_type=jnp.float32)


def _forward_kernel(heads, scaling, q_ref, k_ref, v_ref, o_ref, lse_ref):
    for h in range(heads):
        cols = slice(h * HEAD_DIM, (h + 1) * HEAD_DIM)
        scores = _nt(q_ref[:, cols], k_ref[:, cols]) * scaling
        largest = jnp.max(scores, axis=1, keepdims=True)
        raised = jnp.exp(scores - largest)
        total = jnp.sum(raised, axis=1, keepdims=True)
        probs_low = (raised / total).astype(jnp.bfloat16)
        out = jnp.dot(probs_low, v_ref[:, cols], preferred_element_type=jnp.float32)
        o_ref[:, cols] = out.astype(o_ref.dtype)
        lse_ref[:, h : h + 1] = largest + jnp.log(total)


def _backward_kernel(heads, scaling, q_ref, k_ref, v_ref, g_ref, lse_ref, dq_ref, dk_ref, dv_ref):
    @pl.when(pl.program_id(0) == 0)
    def _():
        dk_ref[...] = jnp.zeros_like(dk_ref)
        dv_ref[...] = jnp.zeros_like(dv_ref)

    for h in range(heads):
        cols = slice(h * HEAD_DIM, (h + 1) * HEAD_DIM)
        q = q_ref[:, cols]
        g = g_ref[:, cols]
        scores = _nt(q, k_ref[:, cols]) * scaling
        probs = jnp.exp(scores - lse_ref[:, h : h + 1])
        grad_probs = _nt(g, v_ref[:, cols])
        dv_ref[:, cols] += _tn(probs.astype(jnp.bfloat16), g)
        row_terms = jnp.sum(probs * grad_probs, axis=1, keepdims=True)
        grad_scores = (probs * (grad_probs - row_terms)).astype(jnp.bfloat16)
        dq_ref[:, cols] = jnp.dot(grad_scores, k_ref[:, cols], preferred_element_type=jnp.float32) * scaling
        dk_ref[:, cols] += _tn(grad_scores, q) * scaling


def attention_forward(queries, keys, values, block_rows=256):
    rows, width = queries.shape
    length = keys.shape[0]
    heads = width // HEAD_DIM
    block_rows = min(block_rows, rows)
    flops = 4 * rows * length * width
    return pl.pallas_call(
        functools.partial(_forward_kernel, heads, HEAD_DIM ** (-0.5)),
        out_shape=(
            jax.ShapeDtypeStruct((rows, width), jnp.bfloat16),
            jax.ShapeDtypeStruct((rows, heads), jnp.float32),
        ),
        grid=(rows // block_rows,),
        in_specs=[
            pl.BlockSpec((block_rows, width), lambda i: (i, 0)),
            pl.BlockSpec((length, width), lambda i: (0, 0)),
            pl.BlockSpec((length, width), lambda i: (0, 0)),
        ],
        out_specs=[
            pl.BlockSpec((block_rows, width), lambda i: (i, 0)),
            pl.BlockSpec((block_rows, heads), lambda i: (i, 0)),
        ],
        compiler_params=pltpu.CompilerParams(
            dimension_semantics=("arbitrary",), vmem_limit_bytes=56 * 1024 * 1024
        ),
        cost_estimate=pl.CostEstimate(
            flops=flops,
            transcendentals=rows * length * heads,
            bytes_accessed=2 * (2 * rows * width + 2 * length * width),
        ),
    )(queries, keys, values)


def attention_backward(queries, keys, values, grad_out, lse, block_rows=256):
    rows, width = queries.shape
    length = keys.shape[0]
    heads = width // HEAD_DIM
    block_rows = min(block_rows, rows)
    flops = 10 * rows * length * width
    return pl.pallas_call(
        functools.partial(_backward_kernel, heads, HEAD_DIM ** (-0.5)),
        out_shape=(
            jax.ShapeDtypeStruct((rows, width), jnp.float32),
            jax.ShapeDtypeStruct((length, width), jnp.float32),
            jax.ShapeDtypeStruct((length, width), jnp.float32),
        ),
        grid=(rows // block_rows,),
        in_specs=[
            pl.BlockSpec((block_rows, width), lambda i: (i, 0)),
            pl.BlockSpec((length, width), lambda i: (0, 0)),
            pl.BlockSpec((length, width), lambda i: (0, 0)),
            pl.BlockSpec((block_rows, width), lambda i: (i, 0)),
            pl.BlockSpec((block_rows, heads), lambda i: (i, 0)),
        ],
        out_specs=[
            pl.BlockSpec((block_rows, width), lambda i: (i, 0)),
            pl.BlockSpec((length, width), lambda i: (0, 0)),
            pl.BlockSpec((length, width), lambda i: (0, 0)),
        ],
        compiler_params=pltpu.CompilerParams(
            dimension_semantics=("arbitrary",), vmem_limit_bytes=56 * 1024 * 1024
        ),
        cost_estimate=pl.CostEstimate(
            flops=flops,
            transcendentals=rows * length * heads,
            bytes_accessed=2 * (3 * rows * width + 2 * length * width) + 4 * (rows + 2 * length) * width,
        ),
    )(queries, keys, values, grad_out, lse)


def gelu_tanh(values):
    return jax.nn.gelu(values, approximate=True)


def on_device(
    tokens, out_grad, noise_index, qkv_weight, out_weight, up_weight, down_weight, ada_weight
):
    clips = tokens.shape[0]
    patches = tokens.shape[2]
    model_width = tokens.shape[-1]
    local_width = qkv_weight.shape[2]
    rows_here = qkv_weight.shape[0]
    heads_here = local_width // HEAD_DIM
    scaling = HEAD_DIM ** (-0.5)
    groups = lax.axis_size("tensor")
    halves = lax.axis_size("frame")
    replicas = lax.axis_size("dp")

    with jax.named_scope("modulation"):
        levels_all = lax.all_gather(noise_index, ("dp", "frame"), axis=0, tiled=True)
        levels_all = levels_all.reshape(replicas * halves, clips, groups)
        condition_all = jax.nn.silu(level_embedding(levels_all, model_width)).astype(jnp.bfloat16)
        row_block = lax.axis_index("dp") * halves + lax.axis_index("frame")
        my_condition = lax.dynamic_slice_in_dim(
            condition_all, row_block * rows_here, rows_here, axis=3
        )
        partial_mod = jnp.einsum(
            "acgd,dkw->acgkw", my_condition, ada_weight, preferred_element_type=jnp.float32
        )
        summed_mod = jnp.sum(
            lax.all_to_all(partial_mod, ("dp", "frame"), 0, 0, tiled=True), axis=0
        )
        group_mod = lax.all_gather(summed_mod, "tensor", axis=3, tiled=True)
        group_mod = jnp.swapaxes(group_mod, 1, 2)[:, :, :, None, :]
        group_index = lax.axis_index("tensor")
        modulation = lax.dynamic_index_in_dim(group_mod, group_index, axis=2, keepdims=False)

    frame_index = lax.axis_index("frame")

    def order_by_half(mine, other):
        both = jnp.stack([mine, other])
        return jnp.where(frame_index == 0, both, both[::-1])

    def hidden_half(weights):
        half = weights[0].shape[1] // halves
        pieces = []
        for weight in weights:
            blocks = weight.reshape(rows_here, halves, half)
            mine = jnp.take(blocks, frame_index, axis=1)
            sent = jnp.take(blocks, 1 - frame_index, axis=1)
            received = lax.ppermute(sent, "frame", [(0, 1), (1, 0)])
            pieces.append(order_by_half(mine, received).reshape(halves * rows_here, half))
        joined = jnp.concatenate(pieces, axis=0)
        gathered = lax.all_gather(joined, "tensor", axis=0, tiled=True)
        gathered = lax.all_gather(gathered, "dp", axis=0, tiled=True)
        gathered = gathered.reshape(replicas, groups, len(weights), halves * rows_here, half)
        return tuple(gathered[:, :, k] for k in range(len(weights)))

    def hidden_half_back(totals):
        half = totals[0].shape[-1]
        blocks = jnp.concatenate(totals, axis=2).astype(jnp.bfloat16)
        blocks = blocks.reshape(replicas * groups, len(totals) * halves * rows_here, half)
        summed = lax.psum_scatter(blocks, "dp", scatter_dimension=0, tiled=True)
        summed = lax.psum_scatter(summed, "tensor", scatter_dimension=0, tiled=True)
        summed = summed.reshape(len(totals), halves, rows_here, half)
        mine = jnp.take(summed, frame_index, axis=1).astype(jnp.float32)
        sent = jnp.take(summed, 1 - frame_index, axis=1)
        received = lax.ppermute(sent, "frame", [(0, 1), (1, 0)]).astype(jnp.float32)
        both = jnp.stack([mine, received], axis=1)
        ordered = jnp.where(frame_index == 0, both, both[:, ::-1])
        return tuple(
            jnp.swapaxes(ordered[k], 0, 1).reshape(rows_here, halves * half)
            for k in range(len(totals))
        )

    with jax.named_scope("weights"):
        joint_weight, mixer_weight = (
            lax.all_gather(w, ("dp", "frame"), axis=0, tiled=True)
            for w in (qkv_weight, out_weight)
        )
        upward_weight, downward_weight = hidden_half((up_weight, down_weight))

    residual = tokens[:, 0].astype(jnp.float32)
    upstream = out_grad[:, 0].astype(jnp.float32)
    with jax.named_scope("group_inputs"):
        group_tokens = lax.all_gather(tokens[:, 0], "tensor", axis=1, tiled=True)
        group_upstream = None
    def gather_halves(values):
        if halves != 2:
            return lax.all_gather(values, "frame", axis=1, tiled=True)
        other = lax.ppermute(values, "frame", [(0, 1), (1, 0)])
        return jnp.concatenate([values, other], axis=1)

    def scatter_halves(values):
        if halves != 2:
            return lax.psum_scatter(
                values.astype(jnp.bfloat16), "frame", scatter_dimension=1, tiled=True
            ).astype(jnp.float32)
        count = values.shape[1] // 2
        mine = values[:, :count]
        other = lax.ppermute(values[:, count:].astype(jnp.bfloat16), "frame", [(0, 1), (1, 0)])
        return mine.astype(jnp.bfloat16).astype(jnp.float32) + other.astype(jnp.float32)

    def clip_pass(residual, upstream, modulation, group_tokens, group_upstream, group_mod):
        clips = residual.shape[0]
        patches = residual.shape[1]
        shift1, scale1, gate1 = modulation[:, 0], modulation[:, 1], modulation[:, 2]
        shift2, scale2, gate2 = modulation[:, 3], modulation[:, 4], modulation[:, 5]
        def gather_tokens(values):
            return lax.all_gather(values, "tensor", axis=1, tiled=True)

        def scatter_tokens(values):
            parts = values.astype(jnp.bfloat16).reshape(
                values.shape[0], groups, -1, values.shape[-1]
            )
            received = lax.all_to_all(parts, "tensor", 1, 1, tiled=True)
            return jnp.sum(received.astype(jnp.float32), axis=1)

        with jax.named_scope("forward"):
            normed_one, inverse_one = normalize(residual)
            group_normed, _ = normalize(
                group_tokens.astype(jnp.float32).reshape(clips, groups, patches, model_width)
            )
            flat_one = (
                (group_normed * (1.0 + group_mod[:, 1]) + group_mod[:, 0])
                .astype(jnp.bfloat16)
                .reshape(clips, groups * patches, model_width)
            )
            token_count = flat_one.shape[1]
            projected = jnp.einsum(
                "crd,dkh->crkh", flat_one, joint_weight, preferred_element_type=jnp.float32
            ).astype(jnp.bfloat16)
            queries = projected[:, :, 0]
            keys_all = gather_halves(projected[:, :, 1])
            values_all = gather_halves(projected[:, :, 2])
            attended, log_totals = attention_forward(queries[0], keys_all[0], values_all[0])
            attended = attended[None]
            partial_one = jnp.einsum(
                "crh,oh->cro", attended, mixer_weight, preferred_element_type=jnp.float32
            )
            branch_one = scatter_tokens(partial_one)
            middle = residual + gate1 * branch_one
            normed_two, inverse_two = normalize(middle)
            entering_two = (normed_two * (1.0 + scale2) + shift2).astype(jnp.bfloat16)
            flat_two = gather_halves(entering_two)
            blocked_two = flat_two.reshape(clips, -1, replicas, halves * rows_here)
            up_values = jnp.einsum(
                "crad,atdj->crtj", blocked_two, upward_weight, preferred_element_type=jnp.float32
            )
            hidden = gelu_tanh(up_values).astype(jnp.bfloat16)
            partial_two = jnp.einsum(
                "crtj,atdj->crad", hidden, downward_weight, preferred_element_type=jnp.float32
            ).reshape(clips, -1, model_width)
            branch_two = scatter_halves(partial_two)
            output = (middle + gate2 * branch_two).astype(jnp.bfloat16)

        with jax.named_scope("backward_ffn"):
            grad_gate_two = jnp.sum(upstream * branch_two, axis=1)
            grad_two_all = gather_halves((gate2 * upstream).astype(jnp.bfloat16))
            blocked_grad = grad_two_all.reshape(clips, -1, replicas, halves * rows_here)
            grad_hidden = jnp.einsum(
                "crad,atdj->crtj", blocked_grad, downward_weight, preferred_element_type=jnp.float32
            )
            down_total = jnp.einsum(
                "crad,crtj->atdj", blocked_grad, hidden, preferred_element_type=jnp.float32
            )
            _, gelu_pullback = jax.vjp(gelu_tanh, up_values)
            grad_up = gelu_pullback(grad_hidden)[0].astype(jnp.bfloat16)
            up_total = jnp.einsum(
                "crad,crtj->atdj", blocked_two, grad_up, preferred_element_type=jnp.float32
            )
            partial_back_two = jnp.einsum(
                "crtj,atdj->crad", grad_up, upward_weight, preferred_element_type=jnp.float32
            ).reshape(clips, -1, model_width)
            grad_entering_two = scatter_halves(partial_back_two)
            grad_shift_two = jnp.sum(grad_entering_two, axis=1)
            grad_scale_two = jnp.sum(grad_entering_two * normed_two, axis=1)
            grad_middle = upstream + norm_back(
                grad_entering_two * (1.0 + scale2), normed_two, inverse_two
            )
            grad_gate_one = jnp.sum(grad_middle * branch_one, axis=1)

        with jax.named_scope("backward_attention"):
            grad_branch_one = (gate1 * grad_middle).astype(jnp.bfloat16)
            grad_one_all = gather_tokens(grad_branch_one)
            grad_attended = jnp.einsum(
                "cro,oh->crh", grad_one_all, mixer_weight, preferred_element_type=jnp.float32
            ).astype(jnp.bfloat16)
            mixer_total = jnp.einsum(
                "cro,crh->oh", grad_one_all, attended, preferred_element_type=jnp.float32
            )
            query_grads, key_grads, value_grads = attention_backward(
                queries[0], keys_all[0], values_all[0], grad_attended[0], log_totals
            )
            query_grads = query_grads[None]
            key_grads = key_grads[None]
            value_grads = value_grads[None]
            key_own, value_own = (
                scatter_halves(grads.reshape(clips, -1, local_width))
                for grads in (key_grads, value_grads)
            )
            grad_projected = jnp.stack([query_grads, key_own, value_own], axis=2).astype(
                jnp.bfloat16
            )
            joint_total = jnp.einsum(
                "crd,crkh->dkh", flat_one, grad_projected, preferred_element_type=jnp.float32
            )
            partial_back_one = jnp.einsum(
                "crkh,dkh->crd", grad_projected, joint_weight, preferred_element_type=jnp.float32
            )
            grad_entering_one = scatter_tokens(partial_back_one)
            grad_shift_one = jnp.sum(grad_entering_one, axis=1)
            grad_scale_one = jnp.sum(grad_entering_one * normed_one, axis=1)
            grad_input = grad_middle + norm_back(
                grad_entering_one * (1.0 + scale1), normed_one, inverse_one
            )


        grad_modulation = jnp.stack(
            [grad_shift_one, grad_scale_one, grad_gate_one, grad_shift_two, grad_scale_two, grad_gate_two],
            axis=1,
        )
        totals = (joint_total, mixer_total, up_total, down_total)
        return output, grad_input.astype(jnp.bfloat16), grad_modulation, totals

    pieces = [
        clip_pass(
            residual[i : i + 1],
            upstream[i : i + 1],
            modulation[i : i + 1],
            group_tokens[i : i + 1],
            None,
            group_mod[i : i + 1],
        )
        for i in range(clips)
    ]
    output = jnp.concatenate([p[0] for p in pieces], axis=0)
    grad_input_low = jnp.concatenate([p[1] for p in pieces], axis=0)
    grad_modulation = jnp.concatenate([p[2] for p in pieces], axis=0)
    joint_total, mixer_total, up_total, down_total = (
        sum(p[3][k] for p in pieces[1:]) + pieces[0][3][k] for k in range(4)
    )
    with jax.named_scope("ada_grad"):
        grad_columns = lax.all_to_all(
            grad_modulation.reshape(clips, 1, 6, model_width), "tensor", 3, 1, tiled=True
        )
        grad_all = lax.all_gather(grad_columns, ("dp", "frame"), axis=0, tiled=True)
        grad_all = grad_all.reshape(replicas * halves, clips, groups, 6, local_width)
        adaptive_total = jnp.einsum(
            "acgd,acgkw->dkw",
            my_condition.astype(jnp.float32),
            grad_all,
            precision=highest,
        )

    with jax.named_scope("weight_grads"):
        attention_totals = jnp.concatenate(
            [joint_total.reshape(model_width, 3 * local_width), mixer_total], axis=1
        )
        attention_sums = lax.psum_scatter(
            attention_totals.astype(jnp.bfloat16), ("dp", "frame"), scatter_dimension=0, tiled=True
        ).astype(jnp.float32)
        joint_sum = attention_sums[:, : 3 * local_width].reshape(rows_here, 3, local_width)
        mixer_sum = attention_sums[:, 3 * local_width :]
        up_sum, down_sum = hidden_half_back((up_total, down_total))
        summed = (joint_sum, mixer_sum, up_sum, down_sum)
    result = output[:, None]
    input_grad = grad_input_low[:, None]
    return (result, input_grad, summed[0], summed[1], summed[2], summed[3], adaptive_total)


def solution(mesh):
    return jax.shard_map(
        on_device,
        mesh=mesh,
        in_specs=(
            P("dp", ("frame", "tensor"), None, None),
            P("dp", ("frame", "tensor"), None, None),
            P("dp", "frame"),
            P(("dp", "frame"), None, "tensor"),
            P(("dp", "frame"), "tensor"),
            P(("dp", "frame"), "tensor"),
            P(("dp", "frame"), "tensor"),
            P(("dp", "frame"), None, "tensor"),
        ),
        out_specs=(
            P("dp", ("frame", "tensor"), None, None),
            P("dp", ("frame", "tensor"), None, None),
            P(("dp", "frame"), None, "tensor"),
            P(("dp", "frame"), "tensor"),
            P(("dp", "frame"), "tensor"),
            P(("dp", "frame"), "tensor"),
            P(("dp", "frame"), None, "tensor"),
        ),
        check_vma=False,
    )
```

```python
import functools
import math

import jax
import jax.numpy as jnp
from jax import lax
from jax.experimental import pallas as pl
from jax.experimental.pallas import tpu as pltpu
from jax.sharding import PartitionSpec as P

HEAD_DIM = 64


epsilon = 1e-06
highest = lax.Precision.HIGHEST


def normalize(values):
    center = values - jnp.mean(values, axis=-1, keepdims=True)
    spread = jnp.mean(center * center, axis=-1, keepdims=True)
    inverse = lax.rsqrt(spread + epsilon)
    return (center * inverse, inverse)


def norm_back(upstream, normed, inverse):
    upstream_mean = jnp.mean(upstream, axis=-1, keepdims=True)
    product_mean = jnp.mean(upstream * normed, axis=-1, keepdims=True)
    return inverse * (upstream - upstream_mean - normed * product_mean)


def level_embedding(levels, model_width):
    halfway = model_width // 2
    frequency = jnp.exp(-math.log(10000.0) * jnp.arange(halfway, dtype=jnp.float32) / halfway)
    angles = levels.astype(jnp.float32)[..., None] * frequency
    return jnp.concatenate([jnp.cos(angles), jnp.sin(angles)], axis=-1)


def _nt(a, b):
    return lax.dot_general(a, b, (((1,), (1,)), ((), ())), preferred_element_type=jnp.float32)


def _tn(a, b):
    return lax.dot_general(a, b, (((0,), (0,)), ((), ())), preferred_element_type=jnp.float32)


def _forward_kernel(heads, scaling, q_ref, k_ref, v_ref, o_ref, lse_ref):
    for h in range(heads):
        cols = slice(h * HEAD_DIM, (h + 1) * HEAD_DIM)
        scores = _nt(q_ref[:, cols], k_ref[:, cols]) * scaling
        largest = jnp.max(scores, axis=1, keepdims=True)
        raised = jnp.exp(scores - largest)
        total = jnp.sum(raised, axis=1, keepdims=True)
        probs_low = (raised / total).astype(jnp.bfloat16)
        out = jnp.dot(probs_low, v_ref[:, cols], preferred_element_type=jnp.float32)
        o_ref[:, cols] = out.astype(o_ref.dtype)
        lse_ref[:, h : h + 1] = largest + jnp.log(total)


def _backward_kernel(heads, scaling, q_ref, k_ref, v_ref, g_ref, lse_ref, dq_ref, dk_ref, dv_ref):
    @pl.when(pl.program_id(0) == 0)
    def _():
        dk_ref[...] = jnp.zeros_like(dk_ref)
        dv_ref[...] = jnp.zeros_like(dv_ref)

    for h in range(heads):
        cols = slice(h * HEAD_DIM, (h + 1) * HEAD_DIM)
        q = q_ref[:, cols]
        g = g_ref[:, cols]
        scores = _nt(q, k_ref[:, cols]) * scaling
        probs = jnp.exp(scores - lse_ref[:, h : h + 1])
        grad_probs = _nt(g, v_ref[:, cols])
        dv_ref[:, cols] += _tn(probs.astype(jnp.bfloat16), g)
        row_terms = jnp.sum(probs * grad_probs, axis=1, keepdims=True)
        grad_scores = (probs * (grad_probs - row_terms)).astype(jnp.bfloat16)
        dq_ref[:, cols] = jnp.dot(grad_scores, k_ref[:, cols], preferred_element_type=jnp.float32) * scaling
        dk_ref[:, cols] += _tn(grad_scores, q) * scaling


def attention_forward(queries, keys, values, block_rows=256):
    rows, width = queries.shape
    length = keys.shape[0]
    heads = width // HEAD_DIM
    block_rows = min(block_rows, rows)
    flops = 4 * rows * length * width
    return pl.pallas_call(
        functools.partial(_forward_kernel, heads, HEAD_DIM ** (-0.5)),
        out_shape=(
            jax.ShapeDtypeStruct((rows, width), jnp.bfloat16),
            jax.ShapeDtypeStruct((rows, heads), jnp.float32),
        ),
        grid=(rows // block_rows,),
        in_specs=[
            pl.BlockSpec((block_rows, width), lambda i: (i, 0)),
            pl.BlockSpec((length, width), lambda i: (0, 0)),
            pl.BlockSpec((length, width), lambda i: (0, 0)),
        ],
        out_specs=[
            pl.BlockSpec((block_rows, width), lambda i: (i, 0)),
            pl.BlockSpec((block_rows, heads), lambda i: (i, 0)),
        ],
        compiler_params=pltpu.CompilerParams(
            dimension_semantics=("arbitrary",), vmem_limit_bytes=56 * 1024 * 1024
        ),
        cost_estimate=pl.CostEstimate(
            flops=flops,
            transcendentals=rows * length * heads,
            bytes_accessed=2 * (2 * rows * width + 2 * length * width),
        ),
    )(queries, keys, values)


def attention_backward(queries, keys, values, grad_out, lse, block_rows=256):
    rows, width = queries.shape
    length = keys.shape[0]
    heads = width // HEAD_DIM
    block_rows = min(block_rows, rows)
    flops = 10 * rows * length * width
    return pl.pallas_call(
        functools.partial(_backward_kernel, heads, HEAD_DIM ** (-0.5)),
        out_shape=(
            jax.ShapeDtypeStruct((rows, width), jnp.float32),
            jax.ShapeDtypeStruct((length, width), jnp.float32),
            jax.ShapeDtypeStruct((length, width), jnp.float32),
        ),
        grid=(rows // block_rows,),
        in_specs=[
            pl.BlockSpec((block_rows, width), lambda i: (i, 0)),
            pl.BlockSpec((length, width), lambda i: (0, 0)),
            pl.BlockSpec((length, width), lambda i: (0, 0)),
            pl.BlockSpec((block_rows, width), lambda i: (i, 0)),
            pl.BlockSpec((block_rows, heads), lambda i: (i, 0)),
        ],
        out_specs=[
            pl.BlockSpec((block_rows, width), lambda i: (i, 0)),
            pl.BlockSpec((length, width), lambda i: (0, 0)),
            pl.BlockSpec((length, width), lambda i: (0, 0)),
        ],
        compiler_params=pltpu.CompilerParams(
            dimension_semantics=("arbitrary",), vmem_limit_bytes=56 * 1024 * 1024
        ),
        cost_estimate=pl.CostEstimate(
            flops=flops,
            transcendentals=rows * length * heads,
            bytes_accessed=2 * (3 * rows * width + 2 * length * width) + 4 * (rows + 2 * length) * width,
        ),
    )(queries, keys, values, grad_out, lse)


def gelu_tanh(values):
    return jax.nn.gelu(values, approximate=True)


def on_device(
    tokens, out_grad, noise_index, qkv_weight, out_weight, up_weight, down_weight, ada_weight
):
    clips = tokens.shape[0]
    patches = tokens.shape[2]
    model_width = tokens.shape[-1]
    local_width = qkv_weight.shape[2]
    rows_here = qkv_weight.shape[0]
    heads_here = local_width // HEAD_DIM
    scaling = HEAD_DIM ** (-0.5)
    groups = lax.axis_size("tensor")
    halves = lax.axis_size("frame")
    replicas = lax.axis_size("dp")

    with jax.named_scope("modulation"):
        levels_all = lax.all_gather(noise_index, ("dp", "frame"), axis=0, tiled=True)
        levels_all = levels_all.reshape(replicas * halves, clips, groups)
        condition_all = jax.nn.silu(level_embedding(levels_all, model_width)).astype(jnp.bfloat16)
        row_block = lax.axis_index("dp") * halves + lax.axis_index("frame")
        my_condition = lax.dynamic_slice_in_dim(
            condition_all, row_block * rows_here, rows_here, axis=3
        )
        partial_mod = jnp.einsum(
            "acgd,dkw->acgkw", my_condition, ada_weight, preferred_element_type=jnp.float32
        )
        summed_mod = jnp.sum(
            lax.all_to_all(partial_mod, ("dp", "frame"), 0, 0, tiled=True), axis=0
        )
        group_mod = lax.all_gather(summed_mod, "tensor", axis=3, tiled=True)
        group_mod = jnp.swapaxes(group_mod, 1, 2)[:, :, :, None, :]
        group_index = lax.axis_index("tensor")
        modulation = lax.dynamic_index_in_dim(group_mod, group_index, axis=2, keepdims=False)

    frame_index = lax.axis_index("frame")

    def order_by_half(mine, other):
        both = jnp.stack([mine, other])
        return jnp.where(frame_index == 0, both, both[::-1])

    def hidden_half(weights):
        half = weights[0].shape[1] // halves
        pieces = []
        for weight in weights:
            blocks = weight.reshape(rows_here, halves, half)
            mine = jnp.take(blocks, frame_index, axis=1)
            sent = jnp.take(blocks, 1 - frame_index, axis=1)
            received = lax.ppermute(sent, "frame", [(0, 1), (1, 0)])
            pieces.append(order_by_half(mine, received).reshape(halves * rows_here, half))
        joined = jnp.concatenate(pieces, axis=0)
        gathered = lax.all_gather(joined, "tensor", axis=0, tiled=True)
        gathered = lax.all_gather(gathered, "dp", axis=0, tiled=True)
        gathered = gathered.reshape(replicas, groups, len(weights), halves * rows_here, half)
        return tuple(gathered[:, :, k] for k in range(len(weights)))

    def hidden_half_back(totals):
        half = totals[0].shape[-1]
        blocks = jnp.concatenate(totals, axis=2).astype(jnp.bfloat16)
        blocks = blocks.reshape(replicas * groups, len(totals) * halves * rows_here, half)
        summed = lax.psum_scatter(blocks, "dp", scatter_dimension=0, tiled=True)
        summed = lax.psum_scatter(summed, "tensor", scatter_dimension=0, tiled=True)
        summed = summed.reshape(len(totals), halves, rows_here, half)
        mine = jnp.take(summed, frame_index, axis=1).astype(jnp.float32)
        sent = jnp.take(summed, 1 - frame_index, axis=1)
        received = lax.ppermute(sent, "frame", [(0, 1), (1, 0)]).astype(jnp.float32)
        both = jnp.stack([mine, received], axis=1)
        ordered = jnp.where(frame_index == 0, both, both[:, ::-1])
        return tuple(
            jnp.swapaxes(ordered[k], 0, 1).reshape(rows_here, halves * half)
            for k in range(len(totals))
        )

    with jax.named_scope("weights"):
        joint_weight, mixer_weight = (
            lax.all_gather(w, ("dp", "frame"), axis=0, tiled=True)
            for w in (qkv_weight, out_weight)
        )
        upward_weight, downward_weight = hidden_half((up_weight, down_weight))

    residual = tokens[:, 0].astype(jnp.float32)
    upstream = out_grad[:, 0].astype(jnp.float32)
    with jax.named_scope("group_inputs"):
        group_tokens = jnp.concatenate(
            [
                lax.all_gather(tokens[i : i + 1, 0], "tensor", axis=1, tiled=True)
                for i in range(clips)
            ],
            axis=0,
        )
        group_upstream = None
    def gather_halves(values):
        if halves != 2:
            return lax.all_gather(values, "frame", axis=1, tiled=True)
        other = lax.ppermute(values, "frame", [(0, 1), (1, 0)])
        return jnp.concatenate([values, other], axis=1)

    def scatter_halves(values):
        if halves != 2:
            return lax.psum_scatter(
                values.astype(jnp.bfloat16), "frame", scatter_dimension=1, tiled=True
            ).astype(jnp.float32)
        count = values.shape[1] // 2
        mine = values[:, :count]
        other = lax.ppermute(values[:, count:].astype(jnp.bfloat16), "frame", [(0, 1), (1, 0)])
        return mine.astype(jnp.bfloat16).astype(jnp.float32) + other.astype(jnp.float32)

    def clip_pass(residual, upstream, modulation, group_tokens, group_upstream, group_mod):
        clips = residual.shape[0]
        patches = residual.shape[1]
        shift1, scale1, gate1 = modulation[:, 0], modulation[:, 1], modulation[:, 2]
        shift2, scale2, gate2 = modulation[:, 3], modulation[:, 4], modulation[:, 5]
        def gather_tokens(values):
            return lax.all_gather(values, "tensor", axis=1, tiled=True)

        def scatter_tokens(values):
            parts = values.astype(jnp.bfloat16).reshape(
                values.shape[0], groups, -1, values.shape[-1]
            )
            received = lax.all_to_all(parts, "tensor", 1, 1, tiled=True)
            return jnp.sum(received.astype(jnp.float32), axis=1)

        with jax.named_scope("forward"):
            normed_one, inverse_one = normalize(residual)
            group_normed, _ = normalize(
                group_tokens.astype(jnp.float32).reshape(clips, groups, patches, model_width)
            )
            flat_one = (
                (group_normed * (1.0 + group_mod[:, 1]) + group_mod[:, 0])
                .astype(jnp.bfloat16)
                .reshape(clips, groups * patches, model_width)
            )
            token_count = flat_one.shape[1]
            projected = jnp.einsum(
                "crd,dkh->crkh", flat_one, joint_weight, preferred_element_type=jnp.float32
            ).astype(jnp.bfloat16)
            queries = projected[:, :, 0]
            keys_all = gather_halves(projected[:, :, 1])
            values_all = gather_halves(projected[:, :, 2])
            attended, log_totals = attention_forward(queries[0], keys_all[0], values_all[0])
            attended = attended[None]
            partial_one = jnp.einsum(
                "crh,oh->cro", attended, mixer_weight, preferred_element_type=jnp.float32
            )
            branch_one = scatter_tokens(partial_one)
            middle = residual + gate1 * branch_one
            normed_two, inverse_two = normalize(middle)
            entering_two = (normed_two * (1.0 + scale2) + shift2).astype(jnp.bfloat16)
            flat_two = gather_halves(entering_two)
            blocked_two = flat_two.reshape(clips, -1, replicas, halves * rows_here)
            up_values = jnp.einsum(
                "crad,atdj->crtj", blocked_two, upward_weight, preferred_element_type=jnp.float32
            )
            hidden = gelu_tanh(up_values).astype(jnp.bfloat16)
            partial_two = jnp.einsum(
                "crtj,atdj->crad", hidden, downward_weight, preferred_element_type=jnp.float32
            ).reshape(clips, -1, model_width)
            branch_two = scatter_halves(partial_two)
            output = (middle + gate2 * branch_two).astype(jnp.bfloat16)

        with jax.named_scope("backward_ffn"):
            grad_gate_two = jnp.sum(upstream * branch_two, axis=1)
            grad_two_all = gather_halves((gate2 * upstream).astype(jnp.bfloat16))
            blocked_grad = grad_two_all.reshape(clips, -1, replicas, halves * rows_here)
            grad_hidden = jnp.einsum(
                "crad,atdj->crtj", blocked_grad, downward_weight, preferred_element_type=jnp.float32
            )
            down_total = jnp.einsum(
                "crad,crtj->atdj", blocked_grad, hidden, preferred_element_type=jnp.float32
            )
            _, gelu_pullback = jax.vjp(gelu_tanh, up_values)
            grad_up = gelu_pullback(grad_hidden)[0].astype(jnp.bfloat16)
            up_total = jnp.einsum(
                "crad,crtj->atdj", blocked_two, grad_up, preferred_element_type=jnp.float32
            )
            partial_back_two = jnp.einsum(
                "crtj,atdj->crad", grad_up, upward_weight, preferred_element_type=jnp.float32
            ).reshape(clips, -1, model_width)
            grad_entering_two = scatter_halves(partial_back_two)
            grad_shift_two = jnp.sum(grad_entering_two, axis=1)
            grad_scale_two = jnp.sum(grad_entering_two * normed_two, axis=1)
            grad_middle = upstream + norm_back(
                grad_entering_two * (1.0 + scale2), normed_two, inverse_two
            )
            grad_gate_one = jnp.sum(grad_middle * branch_one, axis=1)

        with jax.named_scope("backward_attention"):
            grad_branch_one = (gate1 * grad_middle).astype(jnp.bfloat16)
            grad_one_all = gather_tokens(grad_branch_one)
            grad_attended = jnp.einsum(
                "cro,oh->crh", grad_one_all, mixer_weight, preferred_element_type=jnp.float32
            ).astype(jnp.bfloat16)
            mixer_total = jnp.einsum(
                "cro,crh->oh", grad_one_all, attended, preferred_element_type=jnp.float32
            )
            query_grads, key_grads, value_grads = attention_backward(
                queries[0], keys_all[0], values_all[0], grad_attended[0], log_totals
            )
            query_grads = query_grads[None]
            key_grads = key_grads[None]
            value_grads = value_grads[None]
            key_own, value_own = (
                scatter_halves(grads.reshape(clips, -1, local_width))
                for grads in (key_grads, value_grads)
            )
            grad_projected = jnp.stack([query_grads, key_own, value_own], axis=2).astype(
                jnp.bfloat16
            )
            joint_total = jnp.einsum(
                "crd,crkh->dkh", flat_one, grad_projected, preferred_element_type=jnp.float32
            )
            partial_back_one = jnp.einsum(
                "crkh,dkh->crd", grad_projected, joint_weight, preferred_element_type=jnp.float32
            )
            grad_entering_one = scatter_tokens(partial_back_one)
            grad_shift_one = jnp.sum(grad_entering_one, axis=1)
            grad_scale_one = jnp.sum(grad_entering_one * normed_one, axis=1)
            grad_input = grad_middle + norm_back(
                grad_entering_one * (1.0 + scale1), normed_one, inverse_one
            )


        grad_modulation = jnp.stack(
            [grad_shift_one, grad_scale_one, grad_gate_one, grad_shift_two, grad_scale_two, grad_gate_two],
            axis=1,
        )
        totals = (joint_total, mixer_total, up_total, down_total)
        return output, grad_input.astype(jnp.bfloat16), grad_modulation, totals

    pieces = [
        clip_pass(
            residual[i : i + 1],
            upstream[i : i + 1],
            modulation[i : i + 1],
            group_tokens[i : i + 1],
            None,
            group_mod[i : i + 1],
        )
        for i in range(clips)
    ]
    output = jnp.concatenate([p[0] for p in pieces], axis=0)
    grad_input_low = jnp.concatenate([p[1] for p in pieces], axis=0)
    grad_modulation = jnp.concatenate([p[2] for p in pieces], axis=0)
    joint_total, mixer_total, up_total, down_total = (
        sum(p[3][k] for p in pieces[1:]) + pieces[0][3][k] for k in range(4)
    )
    with jax.named_scope("ada_grad"):
        grad_columns = lax.all_to_all(
            grad_modulation.reshape(clips, 1, 6, model_width), "tensor", 3, 1, tiled=True
        )
        grad_all = lax.all_gather(grad_columns, ("dp", "frame"), axis=0, tiled=True)
        grad_all = grad_all.reshape(replicas * halves, clips, groups, 6, local_width)
        adaptive_total = jnp.einsum(
            "acgd,acgkw->dkw",
            my_condition.astype(jnp.float32),
            grad_all,
            precision=highest,
        )

    with jax.named_scope("weight_grads"):
        joint_sum, mixer_sum = (
            lax.psum_scatter(
                total.astype(jnp.bfloat16), ("dp", "frame"), scatter_dimension=0, tiled=True
            ).astype(jnp.float32)
            for total in (joint_total, mixer_total)
        )
        up_sum, down_sum = hidden_half_back((up_total, down_total))
        summed = (joint_sum, mixer_sum, up_sum, down_sum)
    result = output[:, None]
    input_grad = grad_input_low[:, None]
    return (result, input_grad, summed[0], summed[1], summed[2], summed[3], adaptive_total)


def solution(mesh):
    return jax.shard_map(
        on_device,
        mesh=mesh,
        in_specs=(
            P("dp", ("frame", "tensor"), None, None),
            P("dp", ("frame", "tensor"), None, None),
            P("dp", "frame"),
            P(("dp", "frame"), None, "tensor"),
            P(("dp", "frame"), "tensor"),
            P(("dp", "frame"), "tensor"),
            P(("dp", "frame"), "tensor"),
            P(("dp", "frame"), None, "tensor"),
        ),
        out_specs=(
            P("dp", ("frame", "tensor"), None, None),
            P("dp", ("frame", "tensor"), None, None),
            P(("dp", "frame"), None, "tensor"),
            P(("dp", "frame"), "tensor"),
            P(("dp", "frame"), "tensor"),
            P(("dp", "frame"), "tensor"),
            P(("dp", "frame"), None, "tensor"),
        ),
        check_vma=False,
    )
```

```python
import functools
import math

import jax
import jax.numpy as jnp
from jax import lax
from jax.experimental import pallas as pl
from jax.experimental.pallas import tpu as pltpu
from jax.sharding import PartitionSpec as P

HEAD_DIM = 64


epsilon = 1e-06
highest = lax.Precision.HIGHEST


def normalize(values):
    center = values - jnp.mean(values, axis=-1, keepdims=True)
    spread = jnp.mean(center * center, axis=-1, keepdims=True)
    inverse = lax.rsqrt(spread + epsilon)
    return (center * inverse, inverse)


def norm_back(upstream, normed, inverse):
    upstream_mean = jnp.mean(upstream, axis=-1, keepdims=True)
    product_mean = jnp.mean(upstream * normed, axis=-1, keepdims=True)
    return inverse * (upstream - upstream_mean - normed * product_mean)


def level_embedding(levels, model_width):
    halfway = model_width // 2
    frequency = jnp.exp(-math.log(10000.0) * jnp.arange(halfway, dtype=jnp.float32) / halfway)
    angles = levels.astype(jnp.float32)[..., None] * frequency
    return jnp.concatenate([jnp.cos(angles), jnp.sin(angles)], axis=-1)


def _nt(a, b):
    return lax.dot_general(a, b, (((1,), (1,)), ((), ())), preferred_element_type=jnp.float32)


def _tn(a, b):
    return lax.dot_general(a, b, (((0,), (0,)), ((), ())), preferred_element_type=jnp.float32)


def _forward_kernel(heads, scaling, q_ref, k_ref, v_ref, o_ref, lse_ref):
    for h in range(heads):
        cols = slice(h * HEAD_DIM, (h + 1) * HEAD_DIM)
        scores = _nt(q_ref[:, cols], k_ref[:, cols]) * scaling
        largest = jnp.max(scores, axis=1, keepdims=True)
        raised = jnp.exp(scores - largest)
        total = jnp.sum(raised, axis=1, keepdims=True)
        probs_low = (raised / total).astype(jnp.bfloat16)
        out = jnp.dot(probs_low, v_ref[:, cols], preferred_element_type=jnp.float32)
        o_ref[:, cols] = out.astype(o_ref.dtype)
        lse_ref[:, h : h + 1] = largest + jnp.log(total)


def _backward_kernel(heads, scaling, q_ref, k_ref, v_ref, g_ref, lse_ref, dq_ref, dk_ref, dv_ref):
    @pl.when(pl.program_id(0) == 0)
    def _():
        dk_ref[...] = jnp.zeros_like(dk_ref)
        dv_ref[...] = jnp.zeros_like(dv_ref)

    for h in range(heads):
        cols = slice(h * HEAD_DIM, (h + 1) * HEAD_DIM)
        q = q_ref[:, cols]
        g = g_ref[:, cols]
        scores = _nt(q, k_ref[:, cols]) * scaling
        probs = jnp.exp(scores - lse_ref[:, h : h + 1])
        grad_probs = _nt(g, v_ref[:, cols])
        dv_ref[:, cols] += _tn(probs.astype(jnp.bfloat16), g)
        row_terms = jnp.sum(probs * grad_probs, axis=1, keepdims=True)
        grad_scores = (probs * (grad_probs - row_terms)).astype(jnp.bfloat16)
        dq_ref[:, cols] = jnp.dot(grad_scores, k_ref[:, cols], preferred_element_type=jnp.float32) * scaling
        dk_ref[:, cols] += _tn(grad_scores, q) * scaling


def attention_forward(queries, keys, values, block_rows=256):
    rows, width = queries.shape
    length = keys.shape[0]
    heads = width // HEAD_DIM
    block_rows = min(block_rows, rows)
    flops = 4 * rows * length * width
    return pl.pallas_call(
        functools.partial(_forward_kernel, heads, HEAD_DIM ** (-0.5)),
        out_shape=(
            jax.ShapeDtypeStruct((rows, width), jnp.bfloat16),
            jax.ShapeDtypeStruct((rows, heads), jnp.float32),
        ),
        grid=(rows // block_rows,),
        in_specs=[
            pl.BlockSpec((block_rows, width), lambda i: (i, 0)),
            pl.BlockSpec((length, width), lambda i: (0, 0)),
            pl.BlockSpec((length, width), lambda i: (0, 0)),
        ],
        out_specs=[
            pl.BlockSpec((block_rows, width), lambda i: (i, 0)),
            pl.BlockSpec((block_rows, heads), lambda i: (i, 0)),
        ],
        compiler_params=pltpu.CompilerParams(
            dimension_semantics=("arbitrary",), vmem_limit_bytes=56 * 1024 * 1024
        ),
        cost_estimate=pl.CostEstimate(
            flops=flops,
            transcendentals=rows * length * heads,
            bytes_accessed=2 * (2 * rows * width + 2 * length * width),
        ),
    )(queries, keys, values)


def attention_backward(queries, keys, values, grad_out, lse, block_rows=256):
    rows, width = queries.shape
    length = keys.shape[0]
    heads = width // HEAD_DIM
    block_rows = min(block_rows, rows)
    flops = 10 * rows * length * width
    return pl.pallas_call(
        functools.partial(_backward_kernel, heads, HEAD_DIM ** (-0.5)),
        out_shape=(
            jax.ShapeDtypeStruct((rows, width), jnp.float32),
            jax.ShapeDtypeStruct((length, width), jnp.float32),
            jax.ShapeDtypeStruct((length, width), jnp.float32),
        ),
        grid=(rows // block_rows,),
        in_specs=[
            pl.BlockSpec((block_rows, width), lambda i: (i, 0)),
            pl.BlockSpec((length, width), lambda i: (0, 0)),
            pl.BlockSpec((length, width), lambda i: (0, 0)),
            pl.BlockSpec((block_rows, width), lambda i: (i, 0)),
            pl.BlockSpec((block_rows, heads), lambda i: (i, 0)),
        ],
        out_specs=[
            pl.BlockSpec((block_rows, width), lambda i: (i, 0)),
            pl.BlockSpec((length, width), lambda i: (0, 0)),
            pl.BlockSpec((length, width), lambda i: (0, 0)),
        ],
        compiler_params=pltpu.CompilerParams(
            dimension_semantics=("arbitrary",), vmem_limit_bytes=56 * 1024 * 1024
        ),
        cost_estimate=pl.CostEstimate(
            flops=flops,
            transcendentals=rows * length * heads,
            bytes_accessed=2 * (3 * rows * width + 2 * length * width) + 4 * (rows + 2 * length) * width,
        ),
    )(queries, keys, values, grad_out, lse)


def gelu_tanh(values):
    return jax.nn.gelu(values, approximate=True)


def on_device(
    tokens, out_grad, noise_index, qkv_weight, out_weight, up_weight, down_weight, ada_weight
):
    clips = tokens.shape[0]
    patches = tokens.shape[2]
    model_width = tokens.shape[-1]
    local_width = qkv_weight.shape[2]
    rows_here = qkv_weight.shape[0]
    heads_here = local_width // HEAD_DIM
    scaling = HEAD_DIM ** (-0.5)
    groups = lax.axis_size("tensor")
    halves = lax.axis_size("frame")
    replicas = lax.axis_size("dp")

    with jax.named_scope("modulation"):
        levels_all = lax.all_gather(noise_index, ("dp", "frame"), axis=0, tiled=True)
        levels_all = levels_all.reshape(replicas * halves, clips, groups)
        condition_all = jax.nn.silu(level_embedding(levels_all, model_width)).astype(jnp.bfloat16)
        row_block = lax.axis_index("dp") * halves + lax.axis_index("frame")
        my_condition = lax.dynamic_slice_in_dim(
            condition_all, row_block * rows_here, rows_here, axis=3
        )
        partial_mod = jnp.einsum(
            "acgd,dkw->acgkw", my_condition, ada_weight, preferred_element_type=jnp.float32
        )
        summed_mod = jnp.sum(
            lax.all_to_all(partial_mod, ("dp", "frame"), 0, 0, tiled=True), axis=0
        )
        group_mod = lax.all_gather(summed_mod, "tensor", axis=3, tiled=True)
        group_mod = jnp.swapaxes(group_mod, 1, 2)[:, :, :, None, :]
        group_index = lax.axis_index("tensor")
        modulation = lax.dynamic_index_in_dim(group_mod, group_index, axis=2, keepdims=False)

    frame_index = lax.axis_index("frame")

    def order_by_half(mine, other):
        both = jnp.stack([mine, other])
        return jnp.where(frame_index == 0, both, both[::-1])

    def hidden_half(weights):
        half = weights[0].shape[1] // halves
        pieces = []
        for weight in weights:
            blocks = weight.reshape(rows_here, halves, half)
            mine = jnp.take(blocks, frame_index, axis=1)
            sent = jnp.take(blocks, 1 - frame_index, axis=1)
            received = lax.ppermute(sent, "frame", [(0, 1), (1, 0)])
            pieces.append(order_by_half(mine, received).reshape(halves * rows_here, half))
        joined = jnp.concatenate(pieces, axis=0)
        gathered = lax.all_gather(joined, "tensor", axis=0, tiled=True)
        gathered = lax.all_gather(gathered, "dp", axis=0, tiled=True)
        gathered = gathered.reshape(replicas, groups, len(weights), halves * rows_here, half)
        return tuple(gathered[:, :, k] for k in range(len(weights)))

    def hidden_half_back(totals):
        half = totals[0].shape[-1]
        blocks = jnp.concatenate(totals, axis=2).astype(jnp.bfloat16)
        blocks = blocks.reshape(replicas * groups, len(totals) * halves * rows_here, half)
        summed = lax.psum_scatter(blocks, "dp", scatter_dimension=0, tiled=True)
        summed = lax.psum_scatter(summed, "tensor", scatter_dimension=0, tiled=True)
        summed = summed.reshape(len(totals), halves, rows_here, half)
        mine = jnp.take(summed, frame_index, axis=1).astype(jnp.float32)
        sent = jnp.take(summed, 1 - frame_index, axis=1)
        received = lax.ppermute(sent, "frame", [(0, 1), (1, 0)]).astype(jnp.float32)
        both = jnp.stack([mine, received], axis=1)
        ordered = jnp.where(frame_index == 0, both, both[:, ::-1])
        return tuple(
            jnp.swapaxes(ordered[k], 0, 1).reshape(rows_here, halves * half)
            for k in range(len(totals))
        )

    with jax.named_scope("weights"):
        joint_weight, mixer_weight = (
            lax.all_gather(w, ("dp", "frame"), axis=0, tiled=True)
            for w in (qkv_weight, out_weight)
        )
        upward_weight, downward_weight = hidden_half((up_weight, down_weight))

    residual = tokens[:, 0].astype(jnp.float32)
    upstream = out_grad[:, 0].astype(jnp.float32)
    with jax.named_scope("group_inputs"):
        group_tokens = jnp.concatenate(
            [
                lax.all_gather(tokens[i : i + 1, 0], "tensor", axis=1, tiled=True)
                for i in range(clips)
            ],
            axis=0,
        )
        group_upstream = None
    def gather_halves(values):
        if halves != 2:
            return lax.all_gather(values, "frame", axis=1, tiled=True)
        other = lax.ppermute(values, "frame", [(0, 1), (1, 0)])
        return jnp.concatenate([values, other], axis=1)

    def scatter_halves(values):
        if halves != 2:
            return lax.psum_scatter(
                values.astype(jnp.bfloat16), "frame", scatter_dimension=1, tiled=True
            ).astype(jnp.float32)
        count = values.shape[1] // 2
        mine = values[:, :count]
        other = lax.ppermute(values[:, count:].astype(jnp.bfloat16), "frame", [(0, 1), (1, 0)])
        return mine.astype(jnp.bfloat16).astype(jnp.float32) + other.astype(jnp.float32)

    def clip_pass(residual, upstream, modulation, group_tokens, group_upstream, group_mod):
        clips = residual.shape[0]
        patches = residual.shape[1]
        shift1, scale1, gate1 = modulation[:, 0], modulation[:, 1], modulation[:, 2]
        shift2, scale2, gate2 = modulation[:, 3], modulation[:, 4], modulation[:, 5]
        def gather_tokens(values):
            return lax.all_gather(values, "tensor", axis=1, tiled=True)

        def scatter_tokens(values):
            parts = values.astype(jnp.bfloat16).reshape(
                values.shape[0], groups, -1, values.shape[-1]
            )
            received = lax.all_to_all(parts, "tensor", 1, 1, tiled=True)
            return jnp.sum(received.astype(jnp.float32), axis=1)

        with jax.named_scope("forward"):
            normed_one, inverse_one = normalize(residual)
            group_normed, _ = normalize(
                group_tokens.astype(jnp.float32).reshape(clips, groups, patches, model_width)
            )
            flat_one = (
                (group_normed * (1.0 + group_mod[:, 1]) + group_mod[:, 0])
                .astype(jnp.bfloat16)
                .reshape(clips, groups * patches, model_width)
            )
            token_count = flat_one.shape[1]
            projected = jnp.einsum(
                "crd,dkh->crkh", flat_one, joint_weight, preferred_element_type=jnp.float32
            ).astype(jnp.bfloat16)
            queries = projected[:, :, 0]
            keys_all = gather_halves(projected[:, :, 1])
            values_all = gather_halves(projected[:, :, 2])
            attended, log_totals = attention_forward(queries[0], keys_all[0], values_all[0])
            attended = attended[None]
            partial_one = jnp.einsum(
                "crh,oh->cro", attended, mixer_weight, preferred_element_type=jnp.float32
            )
            branch_one = scatter_tokens(partial_one)
            middle = residual + gate1 * branch_one
            normed_two, inverse_two = normalize(middle)
            entering_two = (normed_two * (1.0 + scale2) + shift2).astype(jnp.bfloat16)
            flat_two = gather_halves(entering_two)
            blocked_two = flat_two.reshape(clips, -1, replicas, halves * rows_here)
            up_values = jnp.einsum(
                "crad,atdj->crtj", blocked_two, upward_weight, preferred_element_type=jnp.float32
            )
            hidden = gelu_tanh(up_values).astype(jnp.bfloat16)
            partial_two = jnp.einsum(
                "crtj,atdj->crad", hidden, downward_weight, preferred_element_type=jnp.float32
            ).reshape(clips, -1, model_width)
            branch_two = scatter_halves(partial_two)
            output = (middle + gate2 * branch_two).astype(jnp.bfloat16)

        with jax.named_scope("backward_ffn"):
            grad_gate_two = jnp.sum(upstream * branch_two, axis=1)
            grad_two_all = gather_halves((gate2 * upstream).astype(jnp.bfloat16))
            blocked_grad = grad_two_all.reshape(clips, -1, replicas, halves * rows_here)
            grad_hidden = jnp.einsum(
                "crad,atdj->crtj", blocked_grad, downward_weight, preferred_element_type=jnp.float32
            )
            down_total = jnp.einsum(
                "crad,crtj->atdj", blocked_grad, hidden, preferred_element_type=jnp.float32
            )
            _, gelu_pullback = jax.vjp(gelu_tanh, up_values)
            grad_up = gelu_pullback(grad_hidden)[0].astype(jnp.bfloat16)
            up_total = jnp.einsum(
                "crad,crtj->atdj", blocked_two, grad_up, preferred_element_type=jnp.float32
            )
            partial_back_two = jnp.einsum(
                "crtj,atdj->crad", grad_up, upward_weight, preferred_element_type=jnp.float32
            ).reshape(clips, -1, model_width)
            grad_entering_two = scatter_halves(partial_back_two)
            grad_shift_two = jnp.sum(grad_entering_two, axis=1)
            grad_scale_two = jnp.sum(grad_entering_two * normed_two, axis=1)
            grad_middle = upstream + norm_back(
                grad_entering_two * (1.0 + scale2), normed_two, inverse_two
            )
            grad_gate_one = jnp.sum(grad_middle * branch_one, axis=1)

        with jax.named_scope("backward_attention"):
            grad_branch_one = (gate1 * grad_middle).astype(jnp.bfloat16)
            grad_one_all = gather_tokens(grad_branch_one)
            grad_attended = jnp.einsum(
                "cro,oh->crh", grad_one_all, mixer_weight, preferred_element_type=jnp.float32
            ).astype(jnp.bfloat16)
            mixer_total = jnp.einsum(
                "cro,crh->oh", grad_one_all, attended, preferred_element_type=jnp.float32
            )
            query_grads, key_grads, value_grads = attention_backward(
                queries[0], keys_all[0], values_all[0], grad_attended[0], log_totals
            )
            query_grads = query_grads[None]
            key_grads = key_grads[None]
            value_grads = value_grads[None]
            key_own, value_own = (
                scatter_halves(grads.reshape(clips, -1, local_width))
                for grads in (key_grads, value_grads)
            )
            grad_projected = jnp.stack([query_grads, key_own, value_own], axis=2).astype(
                jnp.bfloat16
            )
            joint_total = jnp.einsum(
                "crd,crkh->dkh", flat_one, grad_projected, preferred_element_type=jnp.float32
            )
            partial_back_one = jnp.einsum(
                "crkh,dkh->crd", grad_projected, joint_weight, preferred_element_type=jnp.float32
            )
            grad_entering_one = scatter_tokens(partial_back_one)
            grad_shift_one = jnp.sum(grad_entering_one, axis=1)
            grad_scale_one = jnp.sum(grad_entering_one * normed_one, axis=1)
            grad_input = grad_middle + norm_back(
                grad_entering_one * (1.0 + scale1), normed_one, inverse_one
            )


        grad_modulation = jnp.stack(
            [grad_shift_one, grad_scale_one, grad_gate_one, grad_shift_two, grad_scale_two, grad_gate_two],
            axis=1,
        )
        totals = (joint_total, mixer_total, up_total, down_total)
        return output, grad_input.astype(jnp.bfloat16), grad_modulation, totals, grad_one_all

    pieces = [
        clip_pass(
            residual[i : i + 1],
            upstream[i : i + 1],
            modulation[i : i + 1],
            group_tokens[i : i + 1],
            None,
            group_mod[i : i + 1],
        )
        for i in range(clips)
    ]
    output = jnp.concatenate([p[0] for p in pieces], axis=0)
    grad_input_low = jnp.concatenate([p[1] for p in pieces], axis=0)
    grad_modulation = jnp.concatenate([p[2] for p in pieces], axis=0)
    joint_total, mixer_total, up_total, down_total = (
        sum(p[3][k] for p in pieces[1:]) + pieces[0][3][k] for k in range(4)
    )
    with jax.named_scope("ada_grad"):
        grad_columns = lax.all_to_all(
            grad_modulation.reshape(clips, 1, 6, model_width), "tensor", 3, 1, tiled=True
        )
        grad_all = lax.all_gather(grad_columns, ("dp", "frame"), axis=0, tiled=True)
        grad_all = grad_all.reshape(replicas * halves, clips, groups, 6, local_width)
        adaptive_total = jnp.einsum(
            "acgd,acgkw->dkw",
            my_condition.astype(jnp.float32),
            grad_all,
            precision=highest,
        )

    with jax.named_scope("weight_grads"):
        up_total, down_total, _ = lax.optimization_barrier((up_total, down_total, pieces[-1][4]))
        up_sum, down_sum = hidden_half_back((up_total, down_total))
        joint_total, mixer_total, up_sum, down_sum = lax.optimization_barrier(
            (joint_total, mixer_total, up_sum, down_sum)
        )
        joint_sum, mixer_sum = (
            lax.psum_scatter(
                total.astype(jnp.bfloat16), ("dp", "frame"), scatter_dimension=0, tiled=True
            ).astype(jnp.float32)
            for total in (joint_total, mixer_total)
        )
        summed = (joint_sum, mixer_sum, up_sum, down_sum)
    result = output[:, None]
    input_grad = grad_input_low[:, None]
    return (result, input_grad, summed[0], summed[1], summed[2], summed[3], adaptive_total)


def solution(mesh):
    return jax.shard_map(
        on_device,
        mesh=mesh,
        in_specs=(
            P("dp", ("frame", "tensor"), None, None),
            P("dp", ("frame", "tensor"), None, None),
            P("dp", "frame"),
            P(("dp", "frame"), None, "tensor"),
            P(("dp", "frame"), "tensor"),
            P(("dp", "frame"), "tensor"),
            P(("dp", "frame"), "tensor"),
            P(("dp", "frame"), None, "tensor"),
        ),
        out_specs=(
            P("dp", ("frame", "tensor"), None, None),
            P("dp", ("frame", "tensor"), None, None),
            P(("dp", "frame"), None, "tensor"),
            P(("dp", "frame"), "tensor"),
            P(("dp", "frame"), "tensor"),
            P(("dp", "frame"), "tensor"),
            P(("dp", "frame"), None, "tensor"),
        ),
        check_vma=False,
    )
```

```python
import functools
import math

import jax
import jax.numpy as jnp
from jax import lax
from jax.experimental import pallas as pl
from jax.experimental.pallas import tpu as pltpu
from jax.sharding import PartitionSpec as P

HEAD_DIM = 64


epsilon = 1e-06
highest = lax.Precision.HIGHEST


def normalize(values):
    center = values - jnp.mean(values, axis=-1, keepdims=True)
    spread = jnp.mean(center * center, axis=-1, keepdims=True)
    inverse = lax.rsqrt(spread + epsilon)
    return (center * inverse, inverse)


def norm_back(upstream, normed, inverse):
    upstream_mean = jnp.mean(upstream, axis=-1, keepdims=True)
    product_mean = jnp.mean(upstream * normed, axis=-1, keepdims=True)
    return inverse * (upstream - upstream_mean - normed * product_mean)


def level_embedding(levels, model_width):
    halfway = model_width // 2
    frequency = jnp.exp(-math.log(10000.0) * jnp.arange(halfway, dtype=jnp.float32) / halfway)
    angles = levels.astype(jnp.float32)[..., None] * frequency
    return jnp.concatenate([jnp.cos(angles), jnp.sin(angles)], axis=-1)


def _nt(a, b):
    return lax.dot_general(a, b, (((1,), (1,)), ((), ())), preferred_element_type=jnp.float32)


def _tn(a, b):
    return lax.dot_general(a, b, (((0,), (0,)), ((), ())), preferred_element_type=jnp.float32)


def _forward_kernel(heads, scaling, q_ref, k_ref, v_ref, o_ref, lse_ref):
    for h in range(heads):
        cols = slice(h * HEAD_DIM, (h + 1) * HEAD_DIM)
        scores = _nt(q_ref[:, cols], k_ref[:, cols]) * scaling
        largest = jnp.max(scores, axis=1, keepdims=True)
        raised = jnp.exp(scores - largest)
        total = jnp.sum(raised, axis=1, keepdims=True)
        probs_low = (raised / total).astype(jnp.bfloat16)
        out = jnp.dot(probs_low, v_ref[:, cols], preferred_element_type=jnp.float32)
        o_ref[:, cols] = out.astype(o_ref.dtype)
        lse_ref[:, h : h + 1] = largest + jnp.log(total)


def _backward_kernel(heads, scaling, q_ref, k_ref, v_ref, g_ref, lse_ref, dq_ref, dk_ref, dv_ref):
    @pl.when(pl.program_id(0) == 0)
    def _():
        dk_ref[...] = jnp.zeros_like(dk_ref)
        dv_ref[...] = jnp.zeros_like(dv_ref)

    for h in range(heads):
        cols = slice(h * HEAD_DIM, (h + 1) * HEAD_DIM)
        q = q_ref[:, cols]
        g = g_ref[:, cols]
        scores = _nt(q, k_ref[:, cols]) * scaling
        probs = jnp.exp(scores - lse_ref[:, h : h + 1])
        grad_probs = _nt(g, v_ref[:, cols])
        dv_ref[:, cols] += _tn(probs.astype(jnp.bfloat16), g)
        row_terms = jnp.sum(probs * grad_probs, axis=1, keepdims=True)
        grad_scores = (probs * (grad_probs - row_terms)).astype(jnp.bfloat16)
        dq_ref[:, cols] = jnp.dot(grad_scores, k_ref[:, cols], preferred_element_type=jnp.float32) * scaling
        dk_ref[:, cols] += _tn(grad_scores, q) * scaling


def attention_forward(queries, keys, values, block_rows=None):
    rows, width = queries.shape
    length = keys.shape[0]
    heads = width // HEAD_DIM
    if block_rows is None:
        block_rows = 512 if length <= 2048 else 256
    block_rows = min(block_rows, rows)
    flops = 4 * rows * length * width
    return pl.pallas_call(
        functools.partial(_forward_kernel, heads, HEAD_DIM ** (-0.5)),
        out_shape=(
            jax.ShapeDtypeStruct((rows, width), jnp.bfloat16),
            jax.ShapeDtypeStruct((rows, heads), jnp.float32),
        ),
        grid=(rows // block_rows,),
        in_specs=[
            pl.BlockSpec((block_rows, width), lambda i: (i, 0)),
            pl.BlockSpec((length, width), lambda i: (0, 0)),
            pl.BlockSpec((length, width), lambda i: (0, 0)),
        ],
        out_specs=[
            pl.BlockSpec((block_rows, width), lambda i: (i, 0)),
            pl.BlockSpec((block_rows, heads), lambda i: (i, 0)),
        ],
        compiler_params=pltpu.CompilerParams(
            dimension_semantics=("arbitrary",), vmem_limit_bytes=56 * 1024 * 1024
        ),
        cost_estimate=pl.CostEstimate(
            flops=flops,
            transcendentals=rows * length * heads,
            bytes_accessed=2 * (2 * rows * width + 2 * length * width),
        ),
    )(queries, keys, values)


def attention_backward(queries, keys, values, grad_out, lse, block_rows=None):
    rows, width = queries.shape
    length = keys.shape[0]
    heads = width // HEAD_DIM
    if block_rows is None:
        block_rows = 512 if length <= 2048 else 256
    block_rows = min(block_rows, rows)
    flops = 10 * rows * length * width
    return pl.pallas_call(
        functools.partial(_backward_kernel, heads, HEAD_DIM ** (-0.5)),
        out_shape=(
            jax.ShapeDtypeStruct((rows, width), jnp.float32),
            jax.ShapeDtypeStruct((length, width), jnp.float32),
            jax.ShapeDtypeStruct((length, width), jnp.float32),
        ),
        grid=(rows // block_rows,),
        in_specs=[
            pl.BlockSpec((block_rows, width), lambda i: (i, 0)),
            pl.BlockSpec((length, width), lambda i: (0, 0)),
            pl.BlockSpec((length, width), lambda i: (0, 0)),
            pl.BlockSpec((block_rows, width), lambda i: (i, 0)),
            pl.BlockSpec((block_rows, heads), lambda i: (i, 0)),
        ],
        out_specs=[
            pl.BlockSpec((block_rows, width), lambda i: (i, 0)),
            pl.BlockSpec((length, width), lambda i: (0, 0)),
            pl.BlockSpec((length, width), lambda i: (0, 0)),
        ],
        compiler_params=pltpu.CompilerParams(
            dimension_semantics=("arbitrary",), vmem_limit_bytes=56 * 1024 * 1024
        ),
        cost_estimate=pl.CostEstimate(
            flops=flops,
            transcendentals=rows * length * heads,
            bytes_accessed=2 * (3 * rows * width + 2 * length * width) + 4 * (rows + 2 * length) * width,
        ),
    )(queries, keys, values, grad_out, lse)


def gelu_tanh(values):
    return jax.nn.gelu(values, approximate=True)


def on_device(
    tokens, out_grad, noise_index, qkv_weight, out_weight, up_weight, down_weight, ada_weight
):
    clips = tokens.shape[0]
    patches = tokens.shape[2]
    model_width = tokens.shape[-1]
    local_width = qkv_weight.shape[2]
    rows_here = qkv_weight.shape[0]
    heads_here = local_width // HEAD_DIM
    scaling = HEAD_DIM ** (-0.5)
    groups = lax.axis_size("tensor")
    halves = lax.axis_size("frame")
    replicas = lax.axis_size("dp")

    with jax.named_scope("modulation"):
        levels_all = lax.all_gather(noise_index, ("dp", "frame"), axis=0, tiled=True)
        levels_all = levels_all.reshape(replicas * halves, clips, groups)
        condition_all = jax.nn.silu(level_embedding(levels_all, model_width)).astype(jnp.bfloat16)
        row_block = lax.axis_index("dp") * halves + lax.axis_index("frame")
        my_condition = lax.dynamic_slice_in_dim(
            condition_all, row_block * rows_here, rows_here, axis=3
        )
        partial_mod = jnp.einsum(
            "acgd,dkw->acgkw", my_condition, ada_weight, preferred_element_type=jnp.float32
        )
        summed_mod = jnp.sum(
            lax.all_to_all(partial_mod, ("dp", "frame"), 0, 0, tiled=True), axis=0
        )
        group_mod = lax.all_gather(summed_mod, "tensor", axis=3, tiled=True)
        group_mod = jnp.swapaxes(group_mod, 1, 2)[:, :, :, None, :]
        group_index = lax.axis_index("tensor")
        modulation = lax.dynamic_index_in_dim(group_mod, group_index, axis=2, keepdims=False)

    frame_index = lax.axis_index("frame")

    def order_by_half(mine, other):
        both = jnp.stack([mine, other])
        return jnp.where(frame_index == 0, both, both[::-1])

    def hidden_half(weights):
        half = weights[0].shape[1] // halves
        pieces = []
        for weight in weights:
            blocks = weight.reshape(rows_here, halves, half)
            mine = jnp.take(blocks, frame_index, axis=1)
            sent = jnp.take(blocks, 1 - frame_index, axis=1)
            received = lax.ppermute(sent, "frame", [(0, 1), (1, 0)])
            pieces.append(order_by_half(mine, received).reshape(halves * rows_here, half))
        joined = jnp.concatenate(pieces, axis=0)
        gathered = lax.all_gather(joined, "tensor", axis=0, tiled=True)
        gathered = lax.all_gather(gathered, "dp", axis=0, tiled=True)
        gathered = gathered.reshape(replicas, groups, len(weights), halves * rows_here, half)
        return tuple(gathered[:, :, k] for k in range(len(weights)))

    def hidden_half_back(totals):
        half = totals[0].shape[-1]
        blocks = jnp.concatenate(totals, axis=2).astype(jnp.bfloat16)
        blocks = blocks.reshape(replicas * groups, len(totals) * halves * rows_here, half)
        summed = lax.psum_scatter(blocks, "dp", scatter_dimension=0, tiled=True)
        summed = lax.psum_scatter(summed, "tensor", scatter_dimension=0, tiled=True)
        summed = summed.reshape(len(totals), halves, rows_here, half)
        mine = jnp.take(summed, frame_index, axis=1).astype(jnp.float32)
        sent = jnp.take(summed, 1 - frame_index, axis=1)
        received = lax.ppermute(sent, "frame", [(0, 1), (1, 0)]).astype(jnp.float32)
        both = jnp.stack([mine, received], axis=1)
        ordered = jnp.where(frame_index == 0, both, both[:, ::-1])
        return tuple(
            jnp.swapaxes(ordered[k], 0, 1).reshape(rows_here, halves * half)
            for k in range(len(totals))
        )

    with jax.named_scope("weights"):
        joint_weight, mixer_weight = (
            lax.all_gather(w, ("dp", "frame"), axis=0, tiled=True)
            for w in (qkv_weight, out_weight)
        )
        upward_weight, downward_weight = hidden_half((up_weight, down_weight))

    residual = tokens[:, 0].astype(jnp.float32)
    upstream = out_grad[:, 0].astype(jnp.float32)
    with jax.named_scope("group_inputs"):
        group_tokens = jnp.concatenate(
            [
                lax.all_gather(tokens[i : i + 1, 0], "tensor", axis=1, tiled=True)
                for i in range(clips)
            ],
            axis=0,
        )
        group_upstream = None
    def gather_halves(values):
        if halves != 2:
            return lax.all_gather(values, "frame", axis=1, tiled=True)
        other = lax.ppermute(values, "frame", [(0, 1), (1, 0)])
        return jnp.concatenate([values, other], axis=1)

    def scatter_halves(values):
        if halves != 2:
            return lax.psum_scatter(
                values.astype(jnp.bfloat16), "frame", scatter_dimension=1, tiled=True
            ).astype(jnp.float32)
        count = values.shape[1] // 2
        mine = values[:, :count]
        other = lax.ppermute(values[:, count:].astype(jnp.bfloat16), "frame", [(0, 1), (1, 0)])
        return mine.astype(jnp.bfloat16).astype(jnp.float32) + other.astype(jnp.float32)

    def clip_pass(residual, upstream, modulation, group_tokens, group_upstream, group_mod):
        clips = residual.shape[0]
        patches = residual.shape[1]
        shift1, scale1, gate1 = modulation[:, 0], modulation[:, 1], modulation[:, 2]
        shift2, scale2, gate2 = modulation[:, 3], modulation[:, 4], modulation[:, 5]
        def gather_tokens(values):
            return lax.all_gather(values, "tensor", axis=1, tiled=True)

        def scatter_tokens(values):
            parts = values.astype(jnp.bfloat16).reshape(
                values.shape[0], groups, -1, values.shape[-1]
            )
            received = lax.all_to_all(parts, "tensor", 1, 1, tiled=True)
            return jnp.sum(received.astype(jnp.float32), axis=1)

        with jax.named_scope("forward"):
            normed_one, inverse_one = normalize(residual)
            group_normed, _ = normalize(
                group_tokens.astype(jnp.float32).reshape(clips, groups, patches, model_width)
            )
            flat_one = (
                (group_normed * (1.0 + group_mod[:, 1]) + group_mod[:, 0])
                .astype(jnp.bfloat16)
                .reshape(clips, groups * patches, model_width)
            )
            token_count = flat_one.shape[1]
            projected = jnp.einsum(
                "crd,dkh->crkh", flat_one, joint_weight, preferred_element_type=jnp.float32
            ).astype(jnp.bfloat16)
            queries = projected[:, :, 0]
            keys_all = gather_halves(projected[:, :, 1])
            values_all = gather_halves(projected[:, :, 2])
            attended, log_totals = attention_forward(queries[0], keys_all[0], values_all[0])
            attended = attended[None]
            partial_one = jnp.einsum(
                "crh,oh->cro", attended, mixer_weight, preferred_element_type=jnp.float32
            )
            branch_one = scatter_tokens(partial_one)
            middle = residual + gate1 * branch_one
            normed_two, inverse_two = normalize(middle)
            entering_two = (normed_two * (1.0 + scale2) + shift2).astype(jnp.bfloat16)
            flat_two = gather_halves(entering_two)
            blocked_two = flat_two.reshape(clips, -1, replicas, halves * rows_here)
            up_values = jnp.einsum(
                "crad,atdj->crtj", blocked_two, upward_weight, preferred_element_type=jnp.float32
            )
            hidden = gelu_tanh(up_values).astype(jnp.bfloat16)
            partial_two = jnp.einsum(
                "crtj,atdj->crad", hidden, downward_weight, preferred_element_type=jnp.float32
            ).reshape(clips, -1, model_width)
            branch_two = scatter_halves(partial_two)
            output = (middle + gate2 * branch_two).astype(jnp.bfloat16)

        with jax.named_scope("backward_ffn"):
            grad_gate_two = jnp.sum(upstream * branch_two, axis=1)
            grad_two_all = gather_halves((gate2 * upstream).astype(jnp.bfloat16))
            blocked_grad = grad_two_all.reshape(clips, -1, replicas, halves * rows_here)
            grad_hidden = jnp.einsum(
                "crad,atdj->crtj", blocked_grad, downward_weight, preferred_element_type=jnp.float32
            )
            down_total = jnp.einsum(
                "crad,crtj->atdj", blocked_grad, hidden, preferred_element_type=jnp.float32
            )
            _, gelu_pullback = jax.vjp(gelu_tanh, up_values)
            grad_up = gelu_pullback(grad_hidden)[0].astype(jnp.bfloat16)
            up_total = jnp.einsum(
                "crad,crtj->atdj", blocked_two, grad_up, preferred_element_type=jnp.float32
            )
            partial_back_two = jnp.einsum(
                "crtj,atdj->crad", grad_up, upward_weight, preferred_element_type=jnp.float32
            ).reshape(clips, -1, model_width)
            grad_entering_two = scatter_halves(partial_back_two)
            grad_shift_two = jnp.sum(grad_entering_two, axis=1)
            grad_scale_two = jnp.sum(grad_entering_two * normed_two, axis=1)
            grad_middle = upstream + norm_back(
                grad_entering_two * (1.0 + scale2), normed_two, inverse_two
            )
            grad_gate_one = jnp.sum(grad_middle * branch_one, axis=1)

        with jax.named_scope("backward_attention"):
            grad_branch_one = (gate1 * grad_middle).astype(jnp.bfloat16)
            grad_one_all = gather_tokens(grad_branch_one)
            grad_attended = jnp.einsum(
                "cro,oh->crh", grad_one_all, mixer_weight, preferred_element_type=jnp.float32
            ).astype(jnp.bfloat16)
            mixer_total = jnp.einsum(
                "cro,crh->oh", grad_one_all, attended, preferred_element_type=jnp.float32
            )
            query_grads, key_grads, value_grads = attention_backward(
                queries[0], keys_all[0], values_all[0], grad_attended[0], log_totals
            )
            query_grads = query_grads[None]
            key_grads = key_grads[None]
            value_grads = value_grads[None]
            key_own, value_own = (
                scatter_halves(grads.reshape(clips, -1, local_width))
                for grads in (key_grads, value_grads)
            )
            grad_projected = jnp.stack([query_grads, key_own, value_own], axis=2).astype(
                jnp.bfloat16
            )
            joint_total = jnp.einsum(
                "crd,crkh->dkh", flat_one, grad_projected, preferred_element_type=jnp.float32
            )
            partial_back_one = jnp.einsum(
                "crkh,dkh->crd", grad_projected, joint_weight, preferred_element_type=jnp.float32
            )
            grad_entering_one = scatter_tokens(partial_back_one)
            grad_shift_one = jnp.sum(grad_entering_one, axis=1)
            grad_scale_one = jnp.sum(grad_entering_one * normed_one, axis=1)
            grad_input = grad_middle + norm_back(
                grad_entering_one * (1.0 + scale1), normed_one, inverse_one
            )


        grad_modulation = jnp.stack(
            [grad_shift_one, grad_scale_one, grad_gate_one, grad_shift_two, grad_scale_two, grad_gate_two],
            axis=1,
        )
        totals = (joint_total, mixer_total, up_total, down_total)
        return output, grad_input.astype(jnp.bfloat16), grad_modulation, totals

    pieces = [
        clip_pass(
            residual[i : i + 1],
            upstream[i : i + 1],
            modulation[i : i + 1],
            group_tokens[i : i + 1],
            None,
            group_mod[i : i + 1],
        )
        for i in range(clips)
    ]
    output = jnp.concatenate([p[0] for p in pieces], axis=0)
    grad_input_low = jnp.concatenate([p[1] for p in pieces], axis=0)
    grad_modulation = jnp.concatenate([p[2] for p in pieces], axis=0)
    joint_total, mixer_total, up_total, down_total = (
        sum(p[3][k] for p in pieces[1:]) + pieces[0][3][k] for k in range(4)
    )
    with jax.named_scope("ada_grad"):
        grad_columns = lax.all_to_all(
            grad_modulation.reshape(clips, 1, 6, model_width), "tensor", 3, 1, tiled=True
        )
        grad_all = lax.all_gather(grad_columns, ("dp", "frame"), axis=0, tiled=True)
        grad_all = grad_all.reshape(replicas * halves, clips, groups, 6, local_width)
        adaptive_total = jnp.einsum(
            "acgd,acgkw->dkw",
            my_condition.astype(jnp.float32),
            grad_all,
            precision=highest,
        )

    with jax.named_scope("weight_grads"):
        joint_sum, mixer_sum = (
            lax.psum_scatter(
                total.astype(jnp.bfloat16), ("dp", "frame"), scatter_dimension=0, tiled=True
            ).astype(jnp.float32)
            for total in (joint_total, mixer_total)
        )
        up_sum, down_sum = hidden_half_back((up_total, down_total))
        summed = (joint_sum, mixer_sum, up_sum, down_sum)
    result = output[:, None]
    input_grad = grad_input_low[:, None]
    return (result, input_grad, summed[0], summed[1], summed[2], summed[3], adaptive_total)


def solution(mesh):
    return jax.shard_map(
        on_device,
        mesh=mesh,
        in_specs=(
            P("dp", ("frame", "tensor"), None, None),
            P("dp", ("frame", "tensor"), None, None),
            P("dp", "frame"),
            P(("dp", "frame"), None, "tensor"),
            P(("dp", "frame"), "tensor"),
            P(("dp", "frame"), "tensor"),
            P(("dp", "frame"), "tensor"),
            P(("dp", "frame"), None, "tensor"),
        ),
        out_specs=(
            P("dp", ("frame", "tensor"), None, None),
            P("dp", ("frame", "tensor"), None, None),
            P(("dp", "frame"), None, "tensor"),
            P(("dp", "frame"), "tensor"),
            P(("dp", "frame"), "tensor"),
            P(("dp", "frame"), "tensor"),
            P(("dp", "frame"), None, "tensor"),
        ),
        check_vma=False,
    )
```

```python
import functools
import math

import jax
import jax.numpy as jnp
from jax import lax
from jax.experimental import pallas as pl
from jax.experimental.pallas import tpu as pltpu
from jax.sharding import PartitionSpec as P

HEAD_DIM = 64


epsilon = 1e-06
highest = lax.Precision.HIGHEST


def normalize(values):
    center = values - jnp.mean(values, axis=-1, keepdims=True)
    spread = jnp.mean(center * center, axis=-1, keepdims=True)
    inverse = lax.rsqrt(spread + epsilon)
    return (center * inverse, inverse)


def norm_back(upstream, normed, inverse):
    upstream_mean = jnp.mean(upstream, axis=-1, keepdims=True)
    product_mean = jnp.mean(upstream * normed, axis=-1, keepdims=True)
    return inverse * (upstream - upstream_mean - normed * product_mean)


def level_embedding(levels, model_width):
    halfway = model_width // 2
    frequency = jnp.exp(-math.log(10000.0) * jnp.arange(halfway, dtype=jnp.float32) / halfway)
    angles = levels.astype(jnp.float32)[..., None] * frequency
    return jnp.concatenate([jnp.cos(angles), jnp.sin(angles)], axis=-1)


def _nt(a, b):
    return lax.dot_general(a, b, (((1,), (1,)), ((), ())), preferred_element_type=jnp.float32)


def _tn(a, b):
    return lax.dot_general(a, b, (((0,), (0,)), ((), ())), preferred_element_type=jnp.float32)


def _forward_kernel(heads, scaling, q_ref, k_ref, v_ref, o_ref, lse_ref):
    for h in range(heads):
        cols = slice(h * HEAD_DIM, (h + 1) * HEAD_DIM)
        scores = _nt(q_ref[:, cols], k_ref[:, cols]) * scaling
        largest = jnp.max(scores, axis=1, keepdims=True)
        raised = jnp.exp(scores - largest)
        total = jnp.sum(raised, axis=1, keepdims=True)
        probs_low = (raised / total).astype(jnp.bfloat16)
        out = jnp.dot(probs_low, v_ref[:, cols], preferred_element_type=jnp.float32)
        o_ref[:, cols] = out.astype(o_ref.dtype)
        lse_ref[:, h : h + 1] = largest + jnp.log(total)


def _backward_kernel(heads, scaling, q_ref, k_ref, v_ref, g_ref, lse_ref, dq_ref, dk_ref, dv_ref):
    @pl.when(pl.program_id(0) == 0)
    def _():
        dk_ref[...] = jnp.zeros_like(dk_ref)
        dv_ref[...] = jnp.zeros_like(dv_ref)

    for h in range(heads):
        cols = slice(h * HEAD_DIM, (h + 1) * HEAD_DIM)
        q = q_ref[:, cols]
        g = g_ref[:, cols]
        scores = _nt(q, k_ref[:, cols]) * scaling
        probs = jnp.exp(scores - lse_ref[:, h : h + 1])
        grad_probs = _nt(g, v_ref[:, cols])
        dv_ref[:, cols] += _tn(probs.astype(jnp.bfloat16), g)
        row_terms = jnp.sum(probs * grad_probs, axis=1, keepdims=True)
        grad_scores = (probs * (grad_probs - row_terms)).astype(jnp.bfloat16)
        dq_ref[:, cols] = jnp.dot(grad_scores, k_ref[:, cols], preferred_element_type=jnp.float32) * scaling
        dk_ref[:, cols] += _tn(grad_scores, q) * scaling


def attention_forward(queries, keys, values, block_rows=256):
    rows, width = queries.shape
    length = keys.shape[0]
    heads = width // HEAD_DIM
    block_rows = min(block_rows, rows)
    flops = 4 * rows * length * width
    return pl.pallas_call(
        functools.partial(_forward_kernel, heads, HEAD_DIM ** (-0.5)),
        out_shape=(
            jax.ShapeDtypeStruct((rows, width), jnp.bfloat16),
            jax.ShapeDtypeStruct((rows, heads), jnp.float32),
        ),
        grid=(rows // block_rows,),
        in_specs=[
            pl.BlockSpec((block_rows, width), lambda i: (i, 0)),
            pl.BlockSpec((length, width), lambda i: (0, 0)),
            pl.BlockSpec((length, width), lambda i: (0, 0)),
        ],
        out_specs=[
            pl.BlockSpec((block_rows, width), lambda i: (i, 0)),
            pl.BlockSpec((block_rows, heads), lambda i: (i, 0)),
        ],
        compiler_params=pltpu.CompilerParams(
            dimension_semantics=("arbitrary",), vmem_limit_bytes=56 * 1024 * 1024
        ),
        cost_estimate=pl.CostEstimate(
            flops=flops,
            transcendentals=rows * length * heads,
            bytes_accessed=2 * (2 * rows * width + 2 * length * width),
        ),
    )(queries, keys, values)


def attention_backward(queries, keys, values, grad_out, lse, block_rows=256):
    rows, width = queries.shape
    length = keys.shape[0]
    heads = width // HEAD_DIM
    block_rows = min(block_rows, rows)
    flops = 10 * rows * length * width
    return pl.pallas_call(
        functools.partial(_backward_kernel, heads, HEAD_DIM ** (-0.5)),
        out_shape=(
            jax.ShapeDtypeStruct((rows, width), jnp.float32),
            jax.ShapeDtypeStruct((length, width), jnp.float32),
            jax.ShapeDtypeStruct((length, width), jnp.float32),
        ),
        grid=(rows // block_rows,),
        in_specs=[
            pl.BlockSpec((block_rows, width), lambda i: (i, 0)),
            pl.BlockSpec((length, width), lambda i: (0, 0)),
            pl.BlockSpec((length, width), lambda i: (0, 0)),
            pl.BlockSpec((block_rows, width), lambda i: (i, 0)),
            pl.BlockSpec((block_rows, heads), lambda i: (i, 0)),
        ],
        out_specs=[
            pl.BlockSpec((block_rows, width), lambda i: (i, 0)),
            pl.BlockSpec((length, width), lambda i: (0, 0)),
            pl.BlockSpec((length, width), lambda i: (0, 0)),
        ],
        compiler_params=pltpu.CompilerParams(
            dimension_semantics=("arbitrary",), vmem_limit_bytes=56 * 1024 * 1024
        ),
        cost_estimate=pl.CostEstimate(
            flops=flops,
            transcendentals=rows * length * heads,
            bytes_accessed=2 * (3 * rows * width + 2 * length * width) + 4 * (rows + 2 * length) * width,
        ),
    )(queries, keys, values, grad_out, lse)


def gelu_tanh(values):
    return jax.nn.gelu(values, approximate=True)


def on_device(
    tokens, out_grad, noise_index, qkv_weight, out_weight, up_weight, down_weight, ada_weight
):
    clips = tokens.shape[0]
    patches = tokens.shape[2]
    model_width = tokens.shape[-1]
    local_width = qkv_weight.shape[2]
    rows_here = qkv_weight.shape[0]
    heads_here = local_width // HEAD_DIM
    scaling = HEAD_DIM ** (-0.5)
    groups = lax.axis_size("tensor")
    halves = lax.axis_size("frame")
    replicas = lax.axis_size("dp")

    with jax.named_scope("modulation"):
        levels_all = lax.all_gather(noise_index, ("dp", "frame"), axis=0, tiled=True)
        levels_all = levels_all.reshape(replicas * halves, clips, groups)
        condition_all = jax.nn.silu(level_embedding(levels_all, model_width)).astype(jnp.bfloat16)
        row_block = lax.axis_index("dp") * halves + lax.axis_index("frame")
        my_condition = lax.dynamic_slice_in_dim(
            condition_all, row_block * rows_here, rows_here, axis=3
        )
        partial_mod = jnp.einsum(
            "acgd,dkw->acgkw", my_condition, ada_weight, preferred_element_type=jnp.float32
        )
        summed_mod = jnp.sum(
            lax.all_to_all(partial_mod, ("dp", "frame"), 0, 0, tiled=True), axis=0
        )
        group_mod = lax.all_gather(summed_mod, "tensor", axis=3, tiled=True)
        group_mod = jnp.swapaxes(group_mod, 1, 2)[:, :, :, None, :]
        group_index = lax.axis_index("tensor")
        modulation = lax.dynamic_index_in_dim(group_mod, group_index, axis=2, keepdims=False)

    frame_index = lax.axis_index("frame")

    def order_by_half(mine, other):
        both = jnp.stack([mine, other])
        return jnp.where(frame_index == 0, both, both[::-1])

    def hidden_half(weights):
        half = weights[0].shape[1] // halves
        pieces = []
        for weight in weights:
            blocks = weight.reshape(rows_here, halves, half)
            mine = jnp.take(blocks, frame_index, axis=1)
            sent = jnp.take(blocks, 1 - frame_index, axis=1)
            received = lax.ppermute(sent, "frame", [(0, 1), (1, 0)])
            pieces.append(order_by_half(mine, received).reshape(halves * rows_here, half))
        joined = jnp.concatenate(pieces, axis=0)
        gathered = lax.all_gather(joined, "tensor", axis=0, tiled=True)
        gathered = lax.all_gather(gathered, "dp", axis=0, tiled=True)
        gathered = gathered.reshape(replicas, groups, len(weights), halves * rows_here, half)
        return tuple(gathered[:, :, k] for k in range(len(weights)))

    def hidden_half_back(totals):
        half = totals[0].shape[-1]
        blocks = jnp.concatenate(totals, axis=2).astype(jnp.bfloat16)
        blocks = blocks.reshape(replicas * groups, len(totals) * halves * rows_here, half)
        summed = lax.psum_scatter(blocks, "dp", scatter_dimension=0, tiled=True)
        summed = lax.psum_scatter(summed, "tensor", scatter_dimension=0, tiled=True)
        summed = summed.reshape(len(totals), halves, rows_here, half)
        mine = jnp.take(summed, frame_index, axis=1).astype(jnp.float32)
        sent = jnp.take(summed, 1 - frame_index, axis=1)
        received = lax.ppermute(sent, "frame", [(0, 1), (1, 0)]).astype(jnp.float32)
        both = jnp.stack([mine, received], axis=1)
        ordered = jnp.where(frame_index == 0, both, both[:, ::-1])
        return tuple(
            jnp.swapaxes(ordered[k], 0, 1).reshape(rows_here, halves * half)
            for k in range(len(totals))
        )

    with jax.named_scope("weights"):
        joint_weight, mixer_weight = (
            lax.all_gather(w, ("dp", "frame"), axis=0, tiled=True)
            for w in (qkv_weight, out_weight)
        )
        ffn_cache = {}

    residual = tokens[:, 0].astype(jnp.float32)
    upstream = out_grad[:, 0].astype(jnp.float32)
    with jax.named_scope("group_inputs"):
        group_tokens = jnp.concatenate(
            [
                lax.all_gather(tokens[i : i + 1, 0], "tensor", axis=1, tiled=True)
                for i in range(clips)
            ],
            axis=0,
        )
        group_upstream = None
    def gather_halves(values):
        if halves != 2:
            return lax.all_gather(values, "frame", axis=1, tiled=True)
        other = lax.ppermute(values, "frame", [(0, 1), (1, 0)])
        return jnp.concatenate([values, other], axis=1)

    def scatter_halves(values):
        if halves != 2:
            return lax.psum_scatter(
                values.astype(jnp.bfloat16), "frame", scatter_dimension=1, tiled=True
            ).astype(jnp.float32)
        count = values.shape[1] // 2
        mine = values[:, :count]
        other = lax.ppermute(values[:, count:].astype(jnp.bfloat16), "frame", [(0, 1), (1, 0)])
        return mine.astype(jnp.bfloat16).astype(jnp.float32) + other.astype(jnp.float32)

    def clip_pass(residual, upstream, modulation, group_tokens, group_upstream, group_mod):
        clips = residual.shape[0]
        patches = residual.shape[1]
        shift1, scale1, gate1 = modulation[:, 0], modulation[:, 1], modulation[:, 2]
        shift2, scale2, gate2 = modulation[:, 3], modulation[:, 4], modulation[:, 5]
        def gather_tokens(values):
            return lax.all_gather(values, "tensor", axis=1, tiled=True)

        def scatter_tokens(values):
            parts = values.astype(jnp.bfloat16).reshape(
                values.shape[0], groups, -1, values.shape[-1]
            )
            received = lax.all_to_all(parts, "tensor", 1, 1, tiled=True)
            return jnp.sum(received.astype(jnp.float32), axis=1)

        with jax.named_scope("forward"):
            normed_one, inverse_one = normalize(residual)
            group_normed, _ = normalize(
                group_tokens.astype(jnp.float32).reshape(clips, groups, patches, model_width)
            )
            flat_one = (
                (group_normed * (1.0 + group_mod[:, 1]) + group_mod[:, 0])
                .astype(jnp.bfloat16)
                .reshape(clips, groups * patches, model_width)
            )
            token_count = flat_one.shape[1]
            projected = jnp.einsum(
                "crd,dkh->crkh", flat_one, joint_weight, preferred_element_type=jnp.float32
            ).astype(jnp.bfloat16)
            queries = projected[:, :, 0]
            keys_all = gather_halves(projected[:, :, 1])
            values_all = gather_halves(projected[:, :, 2])
            attended, log_totals = attention_forward(queries[0], keys_all[0], values_all[0])
            attended = attended[None]
            if not ffn_cache:
                up_in, down_in, attended = lax.optimization_barrier((up_weight, down_weight, attended))
                ffn_cache["weights"] = hidden_half((up_in, down_in))
            upward_weight, downward_weight = ffn_cache["weights"]
            partial_one = jnp.einsum(
                "crh,oh->cro", attended, mixer_weight, preferred_element_type=jnp.float32
            )
            branch_one = scatter_tokens(partial_one)
            middle = residual + gate1 * branch_one
            normed_two, inverse_two = normalize(middle)
            entering_two = (normed_two * (1.0 + scale2) + shift2).astype(jnp.bfloat16)
            flat_two = gather_halves(entering_two)
            blocked_two = flat_two.reshape(clips, -1, replicas, halves * rows_here)
            up_values = jnp.einsum(
                "crad,atdj->crtj", blocked_two, upward_weight, preferred_element_type=jnp.float32
            )
            hidden = gelu_tanh(up_values).astype(jnp.bfloat16)
            partial_two = jnp.einsum(
                "crtj,atdj->crad", hidden, downward_weight, preferred_element_type=jnp.float32
            ).reshape(clips, -1, model_width)
            branch_two = scatter_halves(partial_two)
            output = (middle + gate2 * branch_two).astype(jnp.bfloat16)

        with jax.named_scope("backward_ffn"):
            grad_gate_two = jnp.sum(upstream * branch_two, axis=1)
            grad_two_all = gather_halves((gate2 * upstream).astype(jnp.bfloat16))
            blocked_grad = grad_two_all.reshape(clips, -1, replicas, halves * rows_here)
            grad_hidden = jnp.einsum(
                "crad,atdj->crtj", blocked_grad, downward_weight, preferred_element_type=jnp.float32
            )
            down_total = jnp.einsum(
                "crad,crtj->atdj", blocked_grad, hidden, preferred_element_type=jnp.float32
            )
            _, gelu_pullback = jax.vjp(gelu_tanh, up_values)
            grad_up = gelu_pullback(grad_hidden)[0].astype(jnp.bfloat16)
            up_total = jnp.einsum(
                "crad,crtj->atdj", blocked_two, grad_up, preferred_element_type=jnp.float32
            )
            partial_back_two = jnp.einsum(
                "crtj,atdj->crad", grad_up, upward_weight, preferred_element_type=jnp.float32
            ).reshape(clips, -1, model_width)
            grad_entering_two = scatter_halves(partial_back_two)
            grad_shift_two = jnp.sum(grad_entering_two, axis=1)
            grad_scale_two = jnp.sum(grad_entering_two * normed_two, axis=1)
            grad_middle = upstream + norm_back(
                grad_entering_two * (1.0 + scale2), normed_two, inverse_two
            )
            grad_gate_one = jnp.sum(grad_middle * branch_one, axis=1)

        with jax.named_scope("backward_attention"):
            grad_branch_one = (gate1 * grad_middle).astype(jnp.bfloat16)
            grad_one_all = gather_tokens(grad_branch_one)
            grad_attended = jnp.einsum(
                "cro,oh->crh", grad_one_all, mixer_weight, preferred_element_type=jnp.float32
            ).astype(jnp.bfloat16)
            mixer_total = jnp.einsum(
                "cro,crh->oh", grad_one_all, attended, preferred_element_type=jnp.float32
            )
            query_grads, key_grads, value_grads = attention_backward(
                queries[0], keys_all[0], values_all[0], grad_attended[0], log_totals
            )
            query_grads = query_grads[None]
            key_grads = key_grads[None]
            value_grads = value_grads[None]
            key_own, value_own = (
                scatter_halves(grads.reshape(clips, -1, local_width))
                for grads in (key_grads, value_grads)
            )
            grad_projected = jnp.stack([query_grads, key_own, value_own], axis=2).astype(
                jnp.bfloat16
            )
            joint_total = jnp.einsum(
                "crd,crkh->dkh", flat_one, grad_projected, preferred_element_type=jnp.float32
            )
            partial_back_one = jnp.einsum(
                "crkh,dkh->crd", grad_projected, joint_weight, preferred_element_type=jnp.float32
            )
            grad_entering_one = scatter_tokens(partial_back_one)
            grad_shift_one = jnp.sum(grad_entering_one, axis=1)
            grad_scale_one = jnp.sum(grad_entering_one * normed_one, axis=1)
            grad_input = grad_middle + norm_back(
                grad_entering_one * (1.0 + scale1), normed_one, inverse_one
            )


        grad_modulation = jnp.stack(
            [grad_shift_one, grad_scale_one, grad_gate_one, grad_shift_two, grad_scale_two, grad_gate_two],
            axis=1,
        )
        totals = (joint_total, mixer_total, up_total, down_total)
        return output, grad_input.astype(jnp.bfloat16), grad_modulation, totals

    pieces = [
        clip_pass(
            residual[i : i + 1],
            upstream[i : i + 1],
            modulation[i : i + 1],
            group_tokens[i : i + 1],
            None,
            group_mod[i : i + 1],
        )
        for i in range(clips)
    ]
    output = jnp.concatenate([p[0] for p in pieces], axis=0)
    grad_input_low = jnp.concatenate([p[1] for p in pieces], axis=0)
    grad_modulation = jnp.concatenate([p[2] for p in pieces], axis=0)
    joint_total, mixer_total, up_total, down_total = (
        sum(p[3][k] for p in pieces[1:]) + pieces[0][3][k] for k in range(4)
    )
    with jax.named_scope("ada_grad"):
        grad_columns = lax.all_to_all(
            grad_modulation.reshape(clips, 1, 6, model_width), "tensor", 3, 1, tiled=True
        )
        grad_all = lax.all_gather(grad_columns, ("dp", "frame"), axis=0, tiled=True)
        grad_all = grad_all.reshape(replicas * halves, clips, groups, 6, local_width)
        adaptive_total = jnp.einsum(
            "acgd,acgkw->dkw",
            my_condition.astype(jnp.float32),
            grad_all,
            precision=highest,
        )

    with jax.named_scope("weight_grads"):
        joint_sum, mixer_sum = (
            lax.psum_scatter(
                total.astype(jnp.bfloat16), ("dp", "frame"), scatter_dimension=0, tiled=True
            ).astype(jnp.float32)
            for total in (joint_total, mixer_total)
        )
        up_sum, down_sum = hidden_half_back((up_total, down_total))
        summed = (joint_sum, mixer_sum, up_sum, down_sum)
    result = output[:, None]
    input_grad = grad_input_low[:, None]
    return (result, input_grad, summed[0], summed[1], summed[2], summed[3], adaptive_total)


def solution(mesh):
    return jax.shard_map(
        on_device,
        mesh=mesh,
        in_specs=(
            P("dp", ("frame", "tensor"), None, None),
            P("dp", ("frame", "tensor"), None, None),
            P("dp", "frame"),
            P(("dp", "frame"), None, "tensor"),
            P(("dp", "frame"), "tensor"),
            P(("dp", "frame"), "tensor"),
            P(("dp", "frame"), "tensor"),
            P(("dp", "frame"), None, "tensor"),
        ),
        out_specs=(
            P("dp", ("frame", "tensor"), None, None),
            P("dp", ("frame", "tensor"), None, None),
            P(("dp", "frame"), None, "tensor"),
            P(("dp", "frame"), "tensor"),
            P(("dp", "frame"), "tensor"),
            P(("dp", "frame"), "tensor"),
            P(("dp", "frame"), None, "tensor"),
        ),
        check_vma=False,
    )
```

```python
import functools
import math

import jax
import jax.numpy as jnp
from jax import lax
from jax.experimental import pallas as pl
from jax.experimental.pallas import tpu as pltpu
from jax.sharding import PartitionSpec as P


HEAD_DIM = 64


epsilon = 1e-06
highest = lax.Precision.HIGHEST


def normalize(values):
    center = values - jnp.mean(values, axis=-1, keepdims=True)
    spread = jnp.mean(center * center, axis=-1, keepdims=True)
    inverse = lax.rsqrt(spread + epsilon)
    return (center * inverse, inverse)


def norm_back(upstream, normed, inverse):
    upstream_mean = jnp.mean(upstream, axis=-1, keepdims=True)
    product_mean = jnp.mean(upstream * normed, axis=-1, keepdims=True)
    return inverse * (upstream - upstream_mean - normed * product_mean)


def level_embedding(levels, model_width):
    halfway = model_width // 2
    frequency = jnp.exp(-math.log(10000.0) * jnp.arange(halfway, dtype=jnp.float32) / halfway)
    angles = levels.astype(jnp.float32)[..., None] * frequency
    return jnp.concatenate([jnp.cos(angles), jnp.sin(angles)], axis=-1)


def _nt(a, b):
    return lax.dot_general(a, b, (((1,), (1,)), ((), ())), preferred_element_type=jnp.float32)


def _tn(a, b):
    return lax.dot_general(a, b, (((0,), (0,)), ((), ())), preferred_element_type=jnp.float32)


def _forward_kernel(heads, scaling, q_ref, k_ref, v_ref, o_ref, lse_ref):
    for h in range(heads):
        cols = slice(h * HEAD_DIM, (h + 1) * HEAD_DIM)
        scores = _nt(q_ref[:, cols], k_ref[:, cols]) * scaling
        largest = jnp.max(scores, axis=1, keepdims=True)
        raised = jnp.exp(scores - largest)
        total = jnp.sum(raised, axis=1, keepdims=True)
        probs_low = (raised / total).astype(jnp.bfloat16)
        out = jnp.dot(probs_low, v_ref[:, cols], preferred_element_type=jnp.float32)
        o_ref[:, cols] = out.astype(o_ref.dtype)
        lse_ref[:, h : h + 1] = largest + jnp.log(total)


def _backward_kernel(heads, scaling, q_ref, k_ref, v_ref, g_ref, lse_ref, dq_ref, dk_ref, dv_ref):
    @pl.when(pl.program_id(0) == 0)
    def _():
        dk_ref[...] = jnp.zeros_like(dk_ref)
        dv_ref[...] = jnp.zeros_like(dv_ref)

    for h in range(heads):
        cols = slice(h * HEAD_DIM, (h + 1) * HEAD_DIM)
        q = q_ref[:, cols]
        g = g_ref[:, cols]
        scores = _nt(q, k_ref[:, cols]) * scaling
        probs = jnp.exp(scores - lse_ref[:, h : h + 1])
        grad_probs = _nt(g, v_ref[:, cols])
        dv_ref[:, cols] += _tn(probs.astype(jnp.bfloat16), g)
        row_terms = jnp.sum(probs * grad_probs, axis=1, keepdims=True)
        grad_scores = (probs * (grad_probs - row_terms)).astype(jnp.bfloat16)
        dq_ref[:, cols] = jnp.dot(grad_scores, k_ref[:, cols], preferred_element_type=jnp.float32) * scaling
        dk_ref[:, cols] += _tn(grad_scores, q) * scaling


def attention_forward(queries, keys, values, block_rows=256):
    rows, width = queries.shape
    length = keys.shape[0]
    heads = width // HEAD_DIM
    block_rows = min(block_rows, rows)
    flops = 4 * rows * length * width
    return pl.pallas_call(
        functools.partial(_forward_kernel, heads, HEAD_DIM ** (-0.5)),
        out_shape=(
            jax.ShapeDtypeStruct((rows, width), jnp.bfloat16),
            jax.ShapeDtypeStruct((rows, heads), jnp.float32),
        ),
        grid=(rows // block_rows,),
        in_specs=[
            pl.BlockSpec((block_rows, width), lambda i: (i, 0)),
            pl.BlockSpec((length, width), lambda i: (0, 0)),
            pl.BlockSpec((length, width), lambda i: (0, 0)),
        ],
        out_specs=[
            pl.BlockSpec((block_rows, width), lambda i: (i, 0)),
            pl.BlockSpec((block_rows, heads), lambda i: (i, 0)),
        ],
        compiler_params=pltpu.CompilerParams(
            dimension_semantics=("arbitrary",), vmem_limit_bytes=56 * 1024 * 1024
        ),
        cost_estimate=pl.CostEstimate(
            flops=flops,
            transcendentals=rows * length * heads,
            bytes_accessed=2 * (2 * rows * width + 2 * length * width),
        ),
    )(queries, keys, values)


def attention_backward(queries, keys, values, grad_out, lse, block_rows=256):
    rows, width = queries.shape
    length = keys.shape[0]
    heads = width // HEAD_DIM
    block_rows = min(block_rows, rows)
    flops = 10 * rows * length * width
    return pl.pallas_call(
        functools.partial(_backward_kernel, heads, HEAD_DIM ** (-0.5)),
        out_shape=(
            jax.ShapeDtypeStruct((rows, width), jnp.float32),
            jax.ShapeDtypeStruct((length, width), jnp.float32),
            jax.ShapeDtypeStruct((length, width), jnp.float32),
        ),
        grid=(rows // block_rows,),
        in_specs=[
            pl.BlockSpec((block_rows, width), lambda i: (i, 0)),
            pl.BlockSpec((length, width), lambda i: (0, 0)),
            pl.BlockSpec((length, width), lambda i: (0, 0)),
            pl.BlockSpec((block_rows, width), lambda i: (i, 0)),
            pl.BlockSpec((block_rows, heads), lambda i: (i, 0)),
        ],
        out_specs=[
            pl.BlockSpec((block_rows, width), lambda i: (i, 0)),
            pl.BlockSpec((length, width), lambda i: (0, 0)),
            pl.BlockSpec((length, width), lambda i: (0, 0)),
        ],
        compiler_params=pltpu.CompilerParams(
            dimension_semantics=("arbitrary",), vmem_limit_bytes=56 * 1024 * 1024
        ),
        cost_estimate=pl.CostEstimate(
            flops=flops,
            transcendentals=rows * length * heads,
            bytes_accessed=2 * (3 * rows * width + 2 * length * width) + 4 * (rows + 2 * length) * width,
        ),
    )(queries, keys, values, grad_out, lse)


def gelu_tanh(values):
    return jax.nn.gelu(values, approximate=True)


def block_body(
    tokens, out_grad, noise_index, qkv_weight, out_weight, up_weight, down_weight, ada_weight
):
    clips = tokens.shape[0]
    model_width = tokens.shape[-1]
    local_width = qkv_weight.shape[2]
    rows_here = qkv_weight.shape[0]
    groups = lax.axis_size("tensor")
    halves = lax.axis_size("frame")
    replicas = lax.axis_size("dp")

    levels_all = lax.all_gather(noise_index, ("dp", "frame"), axis=0, tiled=True)
    levels_all = levels_all.reshape(replicas * halves, clips, groups)
    condition_all = jax.nn.silu(level_embedding(levels_all, model_width)).astype(jnp.bfloat16)
    row_block = lax.axis_index("dp") * halves + lax.axis_index("frame")
    my_condition = lax.dynamic_slice_in_dim(condition_all, row_block * rows_here, rows_here, axis=3)
    partial_mod = jnp.einsum(
        "acgd,dkw->acgkw", my_condition, ada_weight, preferred_element_type=jnp.float32
    )
    summed_mod = jnp.sum(
        lax.all_to_all(partial_mod, ("dp", "frame"), 0, 0, tiled=True), axis=0
    )
    group_mod = lax.all_gather(summed_mod, "tensor", axis=3, tiled=True)
    group_mod = jnp.swapaxes(group_mod, 1, 2)[:, :, :, None, :]
    group_index = lax.axis_index("tensor")
    modulation = lax.dynamic_index_in_dim(group_mod, group_index, axis=2, keepdims=False)

    frame_index = lax.axis_index("frame")

    def order_by_half(mine, other):
        both = jnp.stack([mine, other])
        return jnp.where(frame_index == 0, both, both[::-1])

    def hidden_half(weights):
        half = weights[0].shape[1] // halves
        pieces = []
        for weight in weights:
            blocks = weight.reshape(rows_here, halves, half)
            mine = jnp.take(blocks, frame_index, axis=1)
            sent = jnp.take(blocks, 1 - frame_index, axis=1)
            received = lax.ppermute(sent, "frame", [(0, 1), (1, 0)])
            pieces.append(order_by_half(mine, received).reshape(halves * rows_here, half))
        joined = jnp.concatenate(pieces, axis=0)
        gathered = lax.all_gather(joined, "tensor", axis=0, tiled=True)
        gathered = lax.all_gather(gathered, "dp", axis=0, tiled=True)
        gathered = gathered.reshape(replicas, groups, len(weights), halves * rows_here, half)
        return tuple(gathered[:, :, k] for k in range(len(weights)))

    def hidden_half_back(totals):
        half = totals[0].shape[-1]
        blocks = jnp.concatenate(totals, axis=2).astype(jnp.bfloat16)
        blocks = blocks.reshape(replicas * groups, len(totals) * halves * rows_here, half)
        summed = lax.psum_scatter(blocks, "dp", scatter_dimension=0, tiled=True)
        summed = lax.psum_scatter(summed, "tensor", scatter_dimension=0, tiled=True)
        summed = summed.reshape(len(totals), halves, rows_here, half)
        mine = jnp.take(summed, frame_index, axis=1).astype(jnp.float32)
        sent = jnp.take(summed, 1 - frame_index, axis=1)
        received = lax.ppermute(sent, "frame", [(0, 1), (1, 0)]).astype(jnp.float32)
        both = jnp.stack([mine, received], axis=1)
        ordered = jnp.where(frame_index == 0, both, both[:, ::-1])
        return tuple(
            jnp.swapaxes(ordered[k], 0, 1).reshape(rows_here, halves * half)
            for k in range(len(totals))
        )

    joint_weight, mixer_weight = (
        lax.all_gather(w, ("dp", "frame"), axis=0, tiled=True)
        for w in (qkv_weight, out_weight)
    )
    upward_weight, downward_weight = hidden_half((up_weight, down_weight))

    residual = tokens[:, 0].astype(jnp.float32)
    upstream = out_grad[:, 0].astype(jnp.float32)
    gathered_tokens = []
    for i in range(clips):
        gathered_tokens.append(lax.all_gather(tokens[i : i + 1, 0], "tensor", axis=1, tiled=True))
    group_tokens = jnp.concatenate(gathered_tokens, axis=0)

    def gather_halves(values):
        if halves != 2:
            return lax.all_gather(values, "frame", axis=1, tiled=True)
        other = lax.ppermute(values, "frame", [(0, 1), (1, 0)])
        return jnp.concatenate([values, other], axis=1)

    def scatter_halves(values):
        if halves != 2:
            return lax.psum_scatter(
                values.astype(jnp.bfloat16), "frame", scatter_dimension=1, tiled=True
            ).astype(jnp.float32)
        count = values.shape[1] // 2
        mine = values[:, :count]
        other = lax.ppermute(values[:, count:].astype(jnp.bfloat16), "frame", [(0, 1), (1, 0)])
        return mine.astype(jnp.bfloat16).astype(jnp.float32) + other.astype(jnp.float32)

    def clip_pass(residual, upstream, modulation, group_tokens, group_mod):
        clips = residual.shape[0]
        patches = residual.shape[1]
        scale1, gate1 = modulation[:, 1], modulation[:, 2]
        shift2, scale2, gate2 = modulation[:, 3], modulation[:, 4], modulation[:, 5]

        def gather_tokens(values):
            return lax.all_gather(values, "tensor", axis=1, tiled=True)

        def scatter_tokens(values):
            parts = values.astype(jnp.bfloat16).reshape(
                values.shape[0], groups, -1, values.shape[-1]
            )
            received = lax.all_to_all(parts, "tensor", 1, 1, tiled=True)
            return jnp.sum(received.astype(jnp.float32), axis=1)

        normed_one, inverse_one = normalize(residual)
        group_normed, _ = normalize(
            group_tokens.astype(jnp.float32).reshape(clips, groups, patches, model_width)
        )
        flat_one = (
            (group_normed * (1.0 + group_mod[:, 1]) + group_mod[:, 0])
            .astype(jnp.bfloat16)
            .reshape(clips, groups * patches, model_width)
        )
        projected = jnp.einsum(
            "crd,dkh->crkh", flat_one, joint_weight, preferred_element_type=jnp.float32
        ).astype(jnp.bfloat16)
        queries = projected[:, :, 0]
        keys_all = gather_halves(projected[:, :, 1])
        values_all = gather_halves(projected[:, :, 2])
        attended, log_totals = attention_forward(queries[0], keys_all[0], values_all[0])
        attended = attended[None]
        partial_one = jnp.einsum(
            "crh,oh->cro", attended, mixer_weight, preferred_element_type=jnp.float32
        )
        branch_one = scatter_tokens(partial_one)
        middle = residual + gate1 * branch_one
        normed_two, inverse_two = normalize(middle)
        entering_two = (normed_two * (1.0 + scale2) + shift2).astype(jnp.bfloat16)
        flat_two = gather_halves(entering_two)
        blocked_two = flat_two.reshape(clips, -1, replicas, halves * rows_here)
        up_values = jnp.einsum(
            "crad,atdj->crtj", blocked_two, upward_weight, preferred_element_type=jnp.float32
        )
        hidden = gelu_tanh(up_values).astype(jnp.bfloat16)
        partial_two = jnp.einsum(
            "crtj,atdj->crad", hidden, downward_weight, preferred_element_type=jnp.float32
        ).reshape(clips, -1, model_width)
        branch_two = scatter_halves(partial_two)
        output = (middle + gate2 * branch_two).astype(jnp.bfloat16)

        grad_gate_two = jnp.sum(upstream * branch_two, axis=1)
        grad_two_all = gather_halves((gate2 * upstream).astype(jnp.bfloat16))
        blocked_grad = grad_two_all.reshape(clips, -1, replicas, halves * rows_here)
        grad_hidden = jnp.einsum(
            "crad,atdj->crtj", blocked_grad, downward_weight, preferred_element_type=jnp.float32
        )
        down_total = jnp.einsum(
            "crad,crtj->atdj", blocked_grad, hidden, preferred_element_type=jnp.float32
        )
        _, gelu_pullback = jax.vjp(gelu_tanh, up_values)
        grad_up = gelu_pullback(grad_hidden)[0].astype(jnp.bfloat16)
        up_total = jnp.einsum(
            "crad,crtj->atdj", blocked_two, grad_up, preferred_element_type=jnp.float32
        )
        partial_back_two = jnp.einsum(
            "crtj,atdj->crad", grad_up, upward_weight, preferred_element_type=jnp.float32
        ).reshape(clips, -1, model_width)
        grad_entering_two = scatter_halves(partial_back_two)
        grad_shift_two = jnp.sum(grad_entering_two, axis=1)
        grad_scale_two = jnp.sum(grad_entering_two * normed_two, axis=1)
        grad_middle = upstream + norm_back(
            grad_entering_two * (1.0 + scale2), normed_two, inverse_two
        )
        grad_gate_one = jnp.sum(grad_middle * branch_one, axis=1)

        grad_branch_one = (gate1 * grad_middle).astype(jnp.bfloat16)
        grad_one_all = gather_tokens(grad_branch_one)
        grad_attended = jnp.einsum(
            "cro,oh->crh", grad_one_all, mixer_weight, preferred_element_type=jnp.float32
        ).astype(jnp.bfloat16)
        mixer_total = jnp.einsum(
            "cro,crh->oh", grad_one_all, attended, preferred_element_type=jnp.float32
        )
        query_grads, key_grads, value_grads = attention_backward(
            queries[0], keys_all[0], values_all[0], grad_attended[0], log_totals
        )
        query_grads = query_grads[None]
        key_grads = key_grads[None]
        value_grads = value_grads[None]
        key_own, value_own = (
            scatter_halves(grads.reshape(clips, -1, local_width))
            for grads in (key_grads, value_grads)
        )
        grad_projected = jnp.stack([query_grads, key_own, value_own], axis=2).astype(jnp.bfloat16)
        joint_total = jnp.einsum(
            "crd,crkh->dkh", flat_one, grad_projected, preferred_element_type=jnp.float32
        )
        partial_back_one = jnp.einsum(
            "crkh,dkh->crd", grad_projected, joint_weight, preferred_element_type=jnp.float32
        )
        grad_entering_one = scatter_tokens(partial_back_one)
        grad_shift_one = jnp.sum(grad_entering_one, axis=1)
        grad_scale_one = jnp.sum(grad_entering_one * normed_one, axis=1)
        grad_input = grad_middle + norm_back(
            grad_entering_one * (1.0 + scale1), normed_one, inverse_one
        )


        grad_modulation = jnp.stack(
            [grad_shift_one, grad_scale_one, grad_gate_one, grad_shift_two, grad_scale_two, grad_gate_two],
            axis=1,
        )
        totals = (joint_total, mixer_total, up_total, down_total)
        return output, grad_input.astype(jnp.bfloat16), grad_modulation, totals

    pieces = []
    for i in range(clips):
        pieces.append(
            clip_pass(
                residual[i : i + 1],
                upstream[i : i + 1],
                modulation[i : i + 1],
                group_tokens[i : i + 1],
                group_mod[i : i + 1],
            )
        )
    output = jnp.concatenate([p[0] for p in pieces], axis=0)
    grad_input_low = jnp.concatenate([p[1] for p in pieces], axis=0)
    grad_modulation = jnp.concatenate([p[2] for p in pieces], axis=0)
    joint_total, mixer_total, up_total, down_total = (
        sum(p[3][k] for p in pieces[1:]) + pieces[0][3][k] for k in range(4)
    )
    grad_columns = lax.all_to_all(
        grad_modulation.reshape(clips, 1, 6, model_width), "tensor", 3, 1, tiled=True
    )
    grad_all = lax.all_gather(grad_columns, ("dp", "frame"), axis=0, tiled=True)
    grad_all = grad_all.reshape(replicas * halves, clips, groups, 6, local_width)
    adaptive_total = jnp.einsum(
        "acgd,acgkw->dkw",
        my_condition.astype(jnp.float32),
        grad_all,
        precision=highest,
    )

    joint_sum, mixer_sum = (
        lax.psum_scatter(
            total.astype(jnp.bfloat16), ("dp", "frame"), scatter_dimension=0, tiled=True
        ).astype(jnp.float32)
        for total in (joint_total, mixer_total)
    )
    up_sum, down_sum = hidden_half_back((up_total, down_total))
    summed = (joint_sum, mixer_sum, up_sum, down_sum)
    result = output[:, None]
    input_grad = grad_input_low[:, None]
    return (result, input_grad, summed[0], summed[1], summed[2], summed[3], adaptive_total)


def solution(mesh):
    return jax.shard_map(
        block_body,
        mesh=mesh,
        in_specs=(
            P("dp", ("frame", "tensor"), None, None),
            P("dp", ("frame", "tensor"), None, None),
            P("dp", "frame"),
            P(("dp", "frame"), None, "tensor"),
            P(("dp", "frame"), "tensor"),
            P(("dp", "frame"), "tensor"),
            P(("dp", "frame"), "tensor"),
            P(("dp", "frame"), None, "tensor"),
        ),
        out_specs=(
            P("dp", ("frame", "tensor"), None, None),
            P("dp", ("frame", "tensor"), None, None),
            P(("dp", "frame"), None, "tensor"),
            P(("dp", "frame"), "tensor"),
            P(("dp", "frame"), "tensor"),
            P(("dp", "frame"), "tensor"),
            P(("dp", "frame"), None, "tensor"),
        ),
        check_vma=False,
    )
```
